32 devices in a mesh: dp: 8 (over z, x), tensor: 4 (over y, core).
Axes of the slice: x: 2, y: 2, z: 4, core: 2. Of those that a mesh axis runs over, the one named last changes fastest.
Arguments:
- hidden_in: float32 [1024, 1536], P('dp'), may hold values from -6 to 6
- cotangent: float32 [1024, 1536], P('dp'), may hold values from -6 to 6
- segment_ids: int32 [8, 128], P('dp'), may hold values from 0 to 4, as said below
- positions: int32 [8, 128], P('dp'), may hold values from 0 to 2174, as said below
- w_query: bfloat16 [2, 1536, 1536], P(None, None, 'tensor'), may hold values from -0.15625 to 0.15625
- w_key: bfloat16 [2, 1536, 768], P(None, None, 'tensor'), may hold values from -0.15625 to 0.15625
- w_value: bfloat16 [2, 1536, 768], P(None, None, 'tensor'), may hold values from -0.15625 to 0.15625
- w_output: bfloat16 [2, 1536, 1536], P(None, 'tensor'), may hold values from -0.625 to 0.625
- w_gate: bfloat16 [2, 1536, 4096], P(None, None, 'tensor'), may hold values from -0.15625 to 0.15625
- w_up: bfloat16 [2, 1536, 4096], P(None, None, 'tensor'), may hold values from -0.15625 to 0.15625
- w_down: bfloat16 [2, 4096, 1536], P(None, 'tensor'), may hold values from -0.09375 to 0.09375
- attn_gain: float32 [2, 1536], replicated, may hold values from 0.1 to 1.9
- mlp_gain: float32 [2, 1536], replicated, may hold values from 0.1 to 1.9
Outputs:
- hidden_out: float32 [1024, 1536], P('dp')
- grad_input: float32 [1024, 1536], P('dp')
- grad_query: float32 [2, 1536, 1536], P(None, 'dp', 'tensor')
- grad_key: float32 [2, 1536, 768], P(None, 'dp', 'tensor')
- grad_value: float32 [2, 1536, 768], P(None, 'dp', 'tensor')
- grad_output: float32 [2, 1536, 1536], P(None, 'tensor', 'dp')
- grad_gate: float32 [2, 1536, 4096], P(None, 'dp', 'tensor')
- grad_up: float32 [2, 1536, 4096], P(None, 'dp', 'tensor')
- grad_down: float32 [2, 4096, 1536], P(None, 'tensor', 'dp')
- grad_attn_gain: float32 [2, 1536], P(None, 'dp')
- grad_mlp_gain: float32 [2, 1536], P(None, 'dp')
The draws below stay inside these ranges and needn't reach their ends.
Inputs may be any that keep to these rules, and one draw needn't show every extreme that they name: `segment_ids`: segment ids start at 0 in every packed sequence, never fall along it, and every packed sequence holds exactly 5 documents. Within one document, positions rise by one from token to token; the first document of every packed sequence starts at 0 and the last one ends at 2174.
All inputs are finite; a program needn't handle non-finite values.
Results may differ from the reference program's by a relative error of at most 0.025.
Values sent between devices are 32-bit elements; how exact they have to be, the bound alone decides.
A program may use at most 256 MiB of HBM per device.

```python
import jax
import jax.numpy as jnp
from jax import lax

D = 1536
HQ = 16
KV = 8
HD = 96
FF = 4096
LAYERS = 2
DOCS = 5
SEQ_LEN = 128
SEQS = 8
TOKENS = 1024


def document_starts(key):
    scores = jax.random.randint(jax.random.fold_in(key, 11), (SEQS, SEQ_LEN - 1), 0, 1048576)
    scores = scores * SEQ_LEN + jnp.arange(SEQ_LEN - 1, dtype=jnp.int32)[None, :]
    ranking = jnp.argsort(scores, axis=1, stable=True)
    chosen = (ranking[:, :DOCS - 1] + 1).astype(jnp.int32)
    row_index = jnp.broadcast_to(jnp.arange(SEQS, dtype=jnp.int32)[:, None], chosen.shape)
    boundary = jnp.zeros((SEQS, SEQ_LEN), dtype=jnp.bool_).at[row_index, chosen].set(True)
    return boundary.at[:, 0].set(True)


def draw_segment_ids(key, part):
    boundary = document_starts(key)
    return (jnp.cumsum(boundary.astype(jnp.int32), axis=1) - 1).astype(jnp.int32)


def draw_positions(key, part):
    boundary = document_starts(key)
    segments = jnp.cumsum(boundary.astype(jnp.int32), axis=1) - 1
    token_order = jnp.broadcast_to(jnp.arange(SEQ_LEN, dtype=jnp.int32)[None, :], (SEQS, SEQ_LEN))
    starts = lax.cummax(jnp.where(boundary, token_order, 0), axis=1)
    offsets = jax.random.randint(jax.random.fold_in(key, 23), (SEQS, SEQ_LEN), 0, 2048)
    first_offset = jnp.take_along_axis(offsets, starts, axis=1)
    first_offset = jnp.where(segments == 0, 0, first_offset)
    first_offset = jnp.where(segments == DOCS - 1, 2047 + starts, first_offset)
    return (token_order - starts + first_offset).astype(jnp.int32)


def raised(result, key, source, target, blocks, factor):
    def block_of(dim):
        return (jnp.arange(result.shape[dim]) // (result.shape[dim] // blocks)).reshape((-1,) + (1,) * (result.ndim - 1 - dim))

    near = jax.random.permutation(key, blocks)[block_of(target)]
    far = (block_of(target) + blocks // 2) % blocks
    return jnp.where((block_of(source) == near) | (block_of(source) == far), factor * result, result)


def steps_of(key, shape, split, low, top_value):
    factor_of = 1.0
    for axis_at, shards_of in split:
        draws = jax.random.uniform(jax.random.fold_in(jax.random.fold_in(key, 6), axis_at), (shards_of,), jnp.float32, low / len(split), top_value / len(split))
        factor_of = factor_of * jnp.repeat(jnp.exp(draws), shape[axis_at] // shards_of).reshape((-1,) + (1,) * (len(shape) - 1 - axis_at))
    return factor_of


def noise(key, extent, deviation, bound, split=(), held_as=jnp.bfloat16):
    values = jax.random.normal(key, extent, jnp.float32) * deviation
    if len(split) > 0:
        values = steps_of(key, extent, split, -0.22, 0.18) * values
    return jnp.clip(values, min=-bound, max=bound).astype(held_as)


def heavy_noise(rng, extent, spread, bound, split, heavy, held_as=jnp.bfloat16):
    values = spread * jax.random.normal(rng, extent, jnp.float32)
    if split:
        values = values * steps_of(rng, extent, split, -0.22, 0.18)
    return jnp.clip(raised(values, jax.random.fold_in(rng, 3), *heavy), -bound, bound).astype(held_as)


def setup_inputs(seed: int = 0) -> dict:
    key_of = jax.random.split(jax.random.key(seed), 14)
    return {
        "hidden_in": noise(key_of[0], (TOKENS, D), 1.0, 6.0, ((0, 8),), jnp.float32),
        "cotangent": heavy_noise(key_of[1], (TOKENS, D), 1.0, 6.0, ((0, 8),), (0, 1, 8, 2.0), jnp.float32),
        "segment_ids": draw_segment_ids(jax.random.fold_in(key_of[13], 71), 0),
        "positions": draw_positions(jax.random.fold_in(key_of[13], 71), 0),
        "w_query": noise(key_of[4], (LAYERS, D, HQ * HD), D ** -0.5, 0.15625, ((2, 4),)),
        "w_key": noise(key_of[5], (LAYERS, D, KV * HD), D ** -0.5, 0.15625, ((2, 4),)),
        "w_value": noise(key_of[6], (LAYERS, D, KV * HD), D ** -0.5, 0.15625, ((2, 4),)),
        "w_output": noise(key_of[7], (LAYERS, HQ * HD, D), (D // 16) ** -0.5, 0.625, ((1, 4),)),
        "w_gate": noise(key_of[8], (LAYERS, D, FF), D ** -0.5, 0.15625, ((2, 4),)),
        "w_up": noise(key_of[9], (LAYERS, D, FF), D ** -0.5, 0.15625, ((2, 4),)),
        "w_down": noise(key_of[10], (LAYERS, FF, D), FF ** -0.5, 0.09375, ((1, 4),)),
        "attn_gain": jnp.clip(1.0 + 0.18 * jax.random.normal(key_of[11], (LAYERS, D), jnp.float32), 0.1, 1.9),
        "mlp_gain": jnp.clip(1.0 + 0.18 * jax.random.normal(key_of[12], (LAYERS, D), jnp.float32), 0.1, 1.9),
    }


epsilon = 1e-05
rope_base = 100000.0
masked_score = -1e+30

def inverse_rms(values):
    return lax.rsqrt(lax.optimization_barrier(jnp.mean(values * values, axis=-1, keepdims=True)) + epsilon)

def rotary_tables(places):
    half_dim = HD // 2
    frequencies = rope_base ** (-(jnp.arange(half_dim).astype(jnp.float32) * 2.0 / HD))
    angles = places.astype(jnp.float32)[:, None] * frequencies[None, :]
    return (jnp.cos(angles), jnp.sin(angles))

def rotate(tensor, cosine, sine, direction):
    half_dim = tensor.shape[-1] // 2
    first_half = tensor[..., :half_dim]
    second_half = tensor[..., half_dim:]
    cos_part = cosine[:, None, :]
    sin_part = sine[:, None, :]
    return jnp.concatenate([first_half * cos_part - direction * second_half * sin_part, second_half * cos_part + direction * first_half * sin_part], axis=-1)

def attention_scores(queries, key_rows, allowed):
    scores = jnp.einsum('qkgd,skd->kgqs', queries.astype(jnp.float32), key_rows.astype(jnp.float32)) * HD ** (-0.5)
    return jnp.where(allowed[None, None], scores, masked_score)

def attention_forward(queries, key_rows, value_rows, allowed):
    scores = attention_scores(queries, key_rows, allowed)
    row_max = lax.optimization_barrier(jnp.max(scores, axis=-1, keepdims=True))
    exponent = jnp.exp(scores - row_max)
    row_total = lax.optimization_barrier(jnp.sum(exponent, axis=-1, keepdims=True))
    probabilities = (exponent / row_total).astype(jnp.bfloat16)
    logsum = row_max + jnp.log(row_total)
    mixed_rows = jnp.einsum('kgqs,skd->qkgd', probabilities.astype(jnp.float32), value_rows.astype(jnp.float32))
    return (mixed_rows.astype(jnp.bfloat16), logsum)

def attention_backward(queries, key_rows, value_rows, mixed_rows, logsum, grad_mixed, allowed):
    scores = attention_scores(queries, key_rows, allowed)
    again_probs = jnp.exp(scores - logsum)
    probs_low = again_probs.astype(jnp.bfloat16)
    grad_values = jnp.einsum('kgqs,qkgd->skd', probs_low.astype(jnp.float32), grad_mixed.astype(jnp.float32))
    grad_probs = jnp.einsum('qkgd,skd->kgqs', grad_mixed.astype(jnp.float32), value_rows.astype(jnp.float32))
    row_dot = lax.optimization_barrier(jnp.sum(grad_mixed.astype(jnp.float32) * mixed_rows.astype(jnp.float32), axis=-1))
    row_dot = jnp.transpose(row_dot, (1, 2, 0))[..., None]
    grad_scores = (again_probs * (grad_probs - row_dot) * HD ** (-0.5)).astype(jnp.bfloat16)
    grad_queries = jnp.einsum('kgqs,skd->qkgd', grad_scores.astype(jnp.float32), key_rows.astype(jnp.float32))
    grad_keys = jnp.einsum('kgqs,qkgd->skd', grad_scores.astype(jnp.float32), queries.astype(jnp.float32))
    return (grad_queries, grad_keys, grad_values)

def norm_backward(grad_normed, values, inverse, gain_row):
    normalized = values * inverse
    grad_gain = lax.optimization_barrier(jnp.sum(grad_normed * normalized, axis=0))
    scaled = grad_normed * gain_row
    grad_values = inverse * (scaled - normalized * lax.optimization_barrier(jnp.mean(scaled * normalized, axis=-1, keepdims=True)))
    return (grad_gain, grad_values)

def layer_forward(hidden, allowed, cosine, sine, weights):
    w_query, w_key, w_value, w_output, w_gate, w_up, w_down, attn_gain, mlp_gain = weights
    length = hidden.shape[0]
    query_heads = w_query.shape[1] // HD
    kv_heads = w_key.shape[1] // HD
    group_size = query_heads // kv_heads
    inverse_one = inverse_rms(hidden)
    normed = (hidden * inverse_one * attn_gain).astype(jnp.bfloat16)
    queries = jnp.dot(normed, w_query, preferred_element_type=jnp.float32).reshape(length, query_heads, HD)
    queries = rotate(queries, cosine, sine, 1.0).astype(jnp.bfloat16).reshape(length, kv_heads, group_size, HD)
    key_rows = jnp.dot(normed, w_key, preferred_element_type=jnp.float32).reshape(length, kv_heads, HD)
    key_rows = rotate(key_rows, cosine, sine, 1.0).astype(jnp.bfloat16)
    value_rows = jnp.dot(normed, w_value, preferred_element_type=jnp.float32).astype(jnp.bfloat16).reshape(length, kv_heads, HD)
    mixed_rows, logsum = attention_forward(queries, key_rows, value_rows, allowed)
    mixed_flat = mixed_rows.reshape(length, query_heads * HD)
    attended = hidden + jnp.dot(mixed_flat, w_output, preferred_element_type=jnp.float32)
    inverse_two = inverse_rms(attended)
    normed_two = (attended * inverse_two * mlp_gain).astype(jnp.bfloat16)
    gate_pre = jnp.dot(normed_two, w_gate, preferred_element_type=jnp.float32)
    up_pre = jnp.dot(normed_two, w_up, preferred_element_type=jnp.float32)
    activated = (jax.nn.silu(gate_pre) * up_pre).astype(jnp.bfloat16)
    output = attended + jnp.dot(activated, w_down, preferred_element_type=jnp.float32)
    kept_state = (hidden, inverse_one, normed, queries, key_rows, value_rows, mixed_rows, logsum, attended, inverse_two, normed_two, gate_pre, up_pre, activated)
    return (output, kept_state)

def layer_backward(upstream, kept_state, allowed, cosine, sine, weights):
    w_query, w_key, w_value, w_output, w_gate, w_up, w_down, attn_gain, mlp_gain = weights
    hidden, inverse_one, normed, queries, key_rows, value_rows, mixed_rows, logsum, attended, inverse_two, normed_two, gate_pre, up_pre, activated = kept_state
    length = hidden.shape[0]
    query_heads = w_query.shape[1] // HD
    kv_heads = w_key.shape[1] // HD
    group_size = query_heads // kv_heads
    g_low = upstream.astype(jnp.bfloat16)
    grad_down = jnp.dot(activated.T, g_low, preferred_element_type=jnp.float32)
    grad_act = jnp.dot(g_low, w_down.T, preferred_element_type=jnp.float32)
    sigmoid_gate = jax.nn.sigmoid(gate_pre)
    grad_gate_low = (grad_act * up_pre * sigmoid_gate * (1.0 + gate_pre * (1.0 - sigmoid_gate))).astype(jnp.bfloat16)
    grad_up_low = (grad_act * gate_pre * sigmoid_gate).astype(jnp.bfloat16)
    grad_gate = jnp.dot(normed_two.T, grad_gate_low, preferred_element_type=jnp.float32)
    grad_up = jnp.dot(normed_two.T, grad_up_low, preferred_element_type=jnp.float32)
    grad_normed_two = jnp.dot(grad_gate_low, w_gate.T, preferred_element_type=jnp.float32) + jnp.dot(grad_up_low, w_up.T, preferred_element_type=jnp.float32)
    grad_mlp_gain, grad_norm_two = norm_backward(grad_normed_two, attended, inverse_two, mlp_gain)
    grad_attended = upstream + grad_norm_two
    grad_att_low = grad_attended.astype(jnp.bfloat16)
    mixed_flat = mixed_rows.reshape(length, query_heads * HD)
    grad_output = jnp.dot(mixed_flat.T, grad_att_low, preferred_element_type=jnp.float32)
    grad_mixed = jnp.dot(grad_att_low, w_output.T, preferred_element_type=jnp.float32).astype(jnp.bfloat16)
    grad_mixed = grad_mixed.reshape(length, kv_heads, group_size, HD)
    grad_queries, grad_keys, grad_values = attention_backward(queries, key_rows, value_rows, mixed_rows, logsum, grad_mixed, allowed)
    grad_query_low = rotate(grad_queries.reshape(length, query_heads, HD), cosine, sine, -1.0).astype(jnp.bfloat16).reshape(length, query_heads * HD)
    grad_key_low = rotate(grad_keys, cosine, sine, -1.0).astype(jnp.bfloat16).reshape(length, kv_heads * HD)
    grad_value_low = grad_values.astype(jnp.bfloat16).reshape(length, kv_heads * HD)
    grad_query = jnp.dot(normed.T, grad_query_low, preferred_element_type=jnp.float32)
    grad_key = jnp.dot(normed.T, grad_key_low, preferred_element_type=jnp.float32)
    grad_value = jnp.dot(normed.T, grad_value_low, preferred_element_type=jnp.float32)
    grad_normed = jnp.dot(grad_query_low, w_query.T, preferred_element_type=jnp.float32) + jnp.dot(grad_key_low, w_key.T, preferred_element_type=jnp.float32) + jnp.dot(grad_value_low, w_value.T, preferred_element_type=jnp.float32)
    grad_attn_gain, grad_norm_one = norm_backward(grad_normed, hidden, inverse_one, attn_gain)
    grad_hidden = grad_attended + grad_norm_one
    return (grad_hidden, (grad_query, grad_key, grad_value, grad_output, grad_gate, grad_up, grad_down, grad_attn_gain, grad_mlp_gain))

def reference(hidden_in, cotangent, segment_ids, positions, w_query, w_key, w_value, w_output, w_gate, w_up, w_down, attn_gain, mlp_gain):
    weights_all = (w_query, w_key, w_value, w_output, w_gate, w_up, w_down, attn_gain, mlp_gain)

    def per_sequence(totals, sequence_data):
        hidden, grad_top, segments, places = sequence_data
        cosine, sine = rotary_tables(places)
        token_order = jnp.arange(SEQ_LEN)
        allowed = (segments[:, None] == segments[None, :]) & (token_order[None, :] <= token_order[:, None])
        layer_weights = [tuple((weight[which_layer] for weight in weights_all)) for which_layer in range(LAYERS)]
        kept_list = []
        for which_layer in range(LAYERS):
            hidden, kept_state = layer_forward(hidden, allowed, cosine, sine, layer_weights[which_layer])
            kept_list.append(kept_state)
        upstream = grad_top
        grad_layers = [None] * LAYERS
        for which_layer in reversed(range(LAYERS)):
            upstream, grad_layers[which_layer] = layer_backward(upstream, kept_list[which_layer], allowed, cosine, sine, layer_weights[which_layer])
        stacked = tuple((jnp.stack([grad_layers[which_layer][member] for which_layer in range(LAYERS)]) for member in range(9)))
        totals = tuple((total_part + new_part for total_part, new_part in zip(totals, stacked)))
        return (totals, (hidden, upstream))
    initial = tuple((jnp.zeros(weight.shape, jnp.float32) for weight in weights_all))
    sequence_data = (hidden_in.reshape(SEQS, SEQ_LEN, D), cotangent.reshape(SEQS, SEQ_LEN, D), segment_ids, positions)
    totals, (outputs, grads_in) = lax.scan(per_sequence, initial, sequence_data)
    return (outputs.reshape(TOKENS, D), grads_in.reshape(TOKENS, D), totals[0], totals[1], totals[2], totals[3], totals[4], totals[5], totals[6], totals[7], totals[8])
```

```python
import functools

import jax
import jax.numpy as jnp
from jax import lax
from jax.experimental import pallas as pl
from jax.experimental.pallas import tpu as pltpu
from jax.sharding import PartitionSpec as P

HD = 96
LAYERS = 2
CHUNKS = 4
MESH = pl.DeviceIdType.MESH


epsilon = 1e-05
rope_base = 100000.0
masked_score = -1e30


def reduce_kernel(part, base, out, from_core, half, from_y, send, recv):
    dp = lax.axis_index("dp")
    tensor = lax.axis_index("tensor")
    core = tensor % 2
    core_peer = (dp, tensor + 1 - 2 * core)
    y_peer = (dp, lax.rem(tensor + 2, 4))
    rows = part.shape[0] // CHUNKS
    width = part.shape[1] // 2
    mine = pl.ds(pl.multiple_of(core * width, 128), width)
    other = pl.ds(pl.multiple_of((1 - core) * width, 128), width)

    barrier = pltpu.get_barrier_semaphore()
    for peer in (core_peer, y_peer):
        pl.semaphore_signal(barrier, inc=1, device_id=peer, device_id_type=MESH)
    pl.semaphore_wait(barrier, 2)

    def copy(stage, k, src, dst, peer):
        return pltpu.make_async_remote_copy(
            src_ref=src,
            dst_ref=dst,
            send_sem=send.at[stage, k],
            recv_sem=recv.at[stage, k],
            device_id=peer,
            device_id_type=MESH,
        )

    rows_of = [pl.ds(k * rows, rows) for k in range(CHUNKS)]
    first = [
        copy(0, k, part.at[rows_of[k], other], from_core.at[rows_of[k]], core_peer)
        for k in range(CHUNKS)
    ]
    second = [
        copy(1, k, half.at[rows_of[k]], from_y.at[rows_of[k]], y_peer) for k in range(CHUNKS)
    ]
    third = [
        copy(2, k, out.at[rows_of[k], mine], out.at[rows_of[k], mine], core_peer)
        for k in range(CHUNKS)
    ]
    for k in range(CHUNKS):
        first[k].start()
    for k in range(CHUNKS):
        first[k].wait_recv()
        half[rows_of[k], :] = part[rows_of[k], mine] + from_core[rows_of[k], :]
        second[k].start()
    for k in range(CHUNKS):
        second[k].wait_recv()
        out[rows_of[k], mine] = base[rows_of[k], mine] + (
            half[rows_of[k], :] + from_y[rows_of[k], :]
        )
        third[k].start()
    for k in range(CHUNKS):
        third[k].wait_recv()
    for k in range(CHUNKS):
        first[k].wait_send()
        second[k].wait_send()
        third[k].wait_send()


def tensor_sum(part, base):
    length, width = part.shape
    vmem = pl.BlockSpec(memory_space=pltpu.VMEM)
    return pl.pallas_call(
        reduce_kernel,
        out_shape=jax.ShapeDtypeStruct((length, width), jnp.float32),
        in_specs=[vmem, vmem],
        out_specs=vmem,
        scratch_shapes=[
            pltpu.VMEM((length, width // 2), jnp.float32),
            pltpu.VMEM((length, width // 2), jnp.float32),
            pltpu.VMEM((length, width // 2), jnp.float32),
            pltpu.SemaphoreType.DMA((3, CHUNKS)),
            pltpu.SemaphoreType.DMA((3, CHUNKS)),
        ],
        compiler_params=pltpu.CompilerParams(collective_id=0, has_side_effects=True),
        name="tensor_sum",
    )(part, base)


def gather_kernel(n, own_full, shared_full, sliced_full, *refs):
    own_n, shared_n, sliced_n = len(own_full), len(shared_full), len(sliced_full)
    ins = refs[: own_n + shared_n + sliced_n]
    outs = refs[own_n + shared_n + sliced_n : 2 * (own_n + shared_n + sliced_n)]
    send, recv, send_x, recv_x, send_c, recv_c, send_a, recv_a, local = refs[
        2 * (own_n + shared_n + sliced_n) :
    ]
    dp = lax.axis_index("dp")
    tensor = lax.axis_index("tensor")
    core = tensor % 2
    side = dp % 2
    group = dp // 2
    groups = n // 2
    core_peer = (dp, tensor + 1 - 2 * core)
    x_peer = (dp + 1 - 2 * side, tensor)

    barrier = pltpu.get_barrier_semaphore()
    for peer in [core_peer] + [(lax.rem(dp + k, n), tensor) for k in range(1, n)]:
        pl.semaphore_signal(barrier, inc=1, device_id=peer, device_id_type=MESH)
    pl.semaphore_wait(barrier, n)

    def remote(src, dst, s, r, peer):
        return pltpu.make_async_remote_copy(
            src_ref=src, dst_ref=dst, send_sem=s, recv_sem=r, device_id=peer, device_id_type=MESH
        )

    locals_ = []
    for a, (src, dst) in enumerate(zip(ins, outs)):
        if a < own_n + shared_n:
            length = src.shape[0]
            there = dst.at[pl.ds(pl.multiple_of(dp * length, 8), length)]
            locals_.append(pltpu.make_async_copy(src, there, local.at[a]))
        else:
            locals_.append(pltpu.make_async_copy(src.at[dp], dst.at[dp], local.at[a]))
        locals_[-1].start()

    def block(a, ref, index, whole):
        length = ins[a].shape[0]
        rows = pl.ds(pl.multiple_of(index * length, 8), length)
        if a < own_n:
            return ref.at[:, :] if whole else ref.at[rows]
        width = ins[a].shape[1] // 2
        columns = pl.ds(pl.multiple_of(core * width, 128), width)
        return ref.at[:, columns] if whole else ref.at[rows, columns]

    pending = []
    arrays = range(own_n + shared_n)
    direct = {}
    for a in arrays:
        for k in range(1, groups):
            peer = (lax.rem(group + k, groups) * 2 + side, tensor)
            c = remote(
                block(a, ins[a], 0, True),
                block(a, outs[a], dp, False),
                send.at[a, k],
                recv.at[a, k],
                peer,
            )
            c.start()
            direct[a, k] = c
        c = remote(
            block(a, ins[a], 0, True),
            block(a, outs[a], dp, False),
            send_x.at[a, 0],
            recv_x.at[a, 0],
            x_peer,
        )
        c.start()
        direct[a, 0] = c
    exchange = []
    for b in range(sliced_n):
        a = own_n + shared_n + b
        for k in range(1, n):
            to = lax.rem(dp + k, n)
            c = remote(
                ins[a].at[to], outs[a].at[dp], send_a.at[b, k], recv_a.at[b, k], (to, tensor)
            )
            c.start()
            exchange.append(c)
    crossed = {}
    for a in arrays:
        for k in range(1, groups):
            direct[a, k].wait_recv()
            source = lax.rem(group + groups - k, groups) * 2 + side
            c = remote(
                block(a, outs[a], source, False),
                block(a, outs[a], source, False),
                send_x.at[a, k],
                recv_x.at[a, k],
                x_peer,
            )
            c.start()
            crossed[a, k] = c
            if a >= own_n:
                c = remote(
                    block(a, outs[a], source, False),
                    block(a, outs[a], source, False),
                    send_c.at[a - own_n, k],
                    recv_c.at[a - own_n, k],
                    core_peer,
                )
                c.start()
                pending.append(c)
    for a in arrays:
        for k in range(groups):
            (direct[a, 0] if k == 0 else crossed[a, k]).wait_recv()
            if a >= own_n:
                source = lax.rem(group + groups - k, groups) * 2 + 1 - side
                c = remote(
                    block(a, outs[a], source, False),
                    block(a, outs[a], source, False),
                    send_c.at[a - own_n, groups + k],
                    recv_c.at[a - own_n, groups + k],
                    core_peer,
                )
                c.start()
                pending.append(c)
    for c in exchange:
        c.wait()
    for c in pending:
        c.wait()
    for c in list(direct.values()) + list(crossed.values()):
        c.wait_send()
    for c in locals_:
        c.wait()


def gather(n, own, shared, sliced):
    arrays = list(own) + list(shared) + list(sliced)
    out_shape = [
        jax.ShapeDtypeStruct((n * a.shape[0], a.shape[1]), jnp.float32)
        for a in list(own) + list(shared)
    ] + [jax.ShapeDtypeStruct(a.shape, jnp.float32) for a in sliced]
    anywhere = pl.BlockSpec(memory_space=pl.ANY)
    whole = len(own) + len(shared)
    dma = pltpu.SemaphoreType.DMA
    return pl.pallas_call(
        functools.partial(gather_kernel, n, tuple(own), tuple(shared), tuple(sliced)),
        out_shape=out_shape,
        in_specs=[anywhere] * len(arrays),
        out_specs=[anywhere] * len(arrays),
        scratch_shapes=[
            dma((whole, n // 2)),
            dma((whole, n // 2)),
            dma((whole, n // 2)),
            dma((whole, n // 2)),
            dma((len(shared), n)),
            dma((len(shared), n)),
            dma((len(sliced), n)),
            dma((len(sliced), n)),
            dma((len(arrays),)),
        ],
        compiler_params=pltpu.CompilerParams(collective_id=1, has_side_effects=True),
        name="gather_tokens",
    )(*arrays)


def inverse_rms(values):
    return lax.rsqrt(jnp.mean(values * values, axis=-1, keepdims=True) + epsilon)


def rotary_tables(places):
    half_dim = HD // 2
    frequencies = rope_base ** (-(jnp.arange(half_dim).astype(jnp.float32) * 2.0 / HD))
    angles = places.astype(jnp.float32)[:, None] * frequencies[None, :]
    return (jnp.cos(angles), jnp.sin(angles))


def rotate(tensor, cosine, sine, direction):
    half_dim = tensor.shape[-1] // 2
    first_half = tensor[..., :half_dim]
    second_half = tensor[..., half_dim:]
    cos_part = cosine[:, None, :]
    sin_part = sine[:, None, :]
    return jnp.concatenate(
        [
            first_half * cos_part - direction * second_half * sin_part,
            second_half * cos_part + direction * first_half * sin_part,
        ],
        axis=-1,
    )


def attention_scores(queries, key_rows, allowed):
    scores = jnp.einsum(
        "qkgd,skd->kgqs", queries, key_rows, preferred_element_type=jnp.float32
    ) * HD ** (-0.5)
    return jnp.where(allowed[None, None], scores, masked_score)


def attention_forward(queries, key_rows, value_rows, allowed):
    scores = attention_scores(queries, key_rows, allowed)
    row_max = jnp.max(scores, axis=-1, keepdims=True)
    exponent = jnp.exp(scores - row_max)
    row_total = jnp.sum(exponent, axis=-1, keepdims=True)
    probabilities = (exponent / row_total).astype(jnp.bfloat16)
    logsum = row_max + jnp.log(row_total)
    mixed_rows = jnp.einsum(
        "kgqs,skd->qkgd", probabilities, value_rows, preferred_element_type=jnp.float32
    )
    return (mixed_rows.astype(jnp.bfloat16), logsum)


def attention_backward(queries, key_rows, value_rows, mixed_rows, logsum, grad_mixed, allowed):
    scores = attention_scores(queries, key_rows, allowed)
    again_probs = jnp.exp(scores - logsum)
    probs_low = again_probs.astype(jnp.bfloat16)
    grad_values = jnp.einsum(
        "kgqs,qkgd->skd", probs_low, grad_mixed, preferred_element_type=jnp.float32
    )
    grad_probs = jnp.einsum(
        "qkgd,skd->kgqs", grad_mixed, value_rows, preferred_element_type=jnp.float32
    )
    row_dot = jnp.sum(grad_mixed.astype(jnp.float32) * mixed_rows.astype(jnp.float32), axis=-1)
    row_dot = jnp.transpose(row_dot, (1, 2, 0))[..., None]
    grad_scores = (again_probs * (grad_probs - row_dot) * HD ** (-0.5)).astype(jnp.bfloat16)
    grad_queries = jnp.einsum(
        "kgqs,skd->qkgd", grad_scores, key_rows, preferred_element_type=jnp.float32
    )
    grad_keys = jnp.einsum(
        "kgqs,qkgd->skd", grad_scores, queries, preferred_element_type=jnp.float32
    )
    return (grad_queries, grad_keys, grad_values)


def norm_backward(grad_normed, values, inverse, gain_row):
    normalized = values * inverse
    grad_gain = jnp.sum(grad_normed * normalized, axis=0)
    scaled = grad_normed * gain_row
    grad_values = inverse * (
        scaled - normalized * jnp.mean(scaled * normalized, axis=-1, keepdims=True)
    )
    return (grad_gain, grad_values)


def layer_forward(hidden, allowed, cosine, sine, weights):
    w_query, w_key, w_value, w_output, w_gate, w_up, w_down, attn_gain, mlp_gain = weights
    length = hidden.shape[0]
    query_heads = w_query.shape[1] // HD
    kv_heads = w_key.shape[1] // HD
    group_size = query_heads // kv_heads
    inverse_one = inverse_rms(hidden)
    normed = (hidden * inverse_one * attn_gain).astype(jnp.bfloat16)
    queries = jnp.dot(normed, w_query, preferred_element_type=jnp.float32).reshape(
        length, query_heads, HD
    )
    queries = (
        rotate(queries, cosine, sine, 1.0)
        .astype(jnp.bfloat16)
        .reshape(length, kv_heads, group_size, HD)
    )
    key_rows = jnp.dot(normed, w_key, preferred_element_type=jnp.float32).reshape(
        length, kv_heads, HD
    )
    key_rows = rotate(key_rows, cosine, sine, 1.0).astype(jnp.bfloat16)
    value_rows = (
        jnp.dot(normed, w_value, preferred_element_type=jnp.float32)
        .astype(jnp.bfloat16)
        .reshape(length, kv_heads, HD)
    )
    mixed_rows, logsum = attention_forward(queries, key_rows, value_rows, allowed)
    mixed_flat = mixed_rows.reshape(length, query_heads * HD)
    attn_part = jnp.dot(mixed_flat, w_output, preferred_element_type=jnp.float32)
    attended = tensor_sum(attn_part, hidden)
    inverse_two = inverse_rms(attended)
    normed_two = (attended * inverse_two * mlp_gain).astype(jnp.bfloat16)
    gate_pre = jnp.dot(normed_two, w_gate, preferred_element_type=jnp.float32)
    up_pre = jnp.dot(normed_two, w_up, preferred_element_type=jnp.float32)
    activated = (jax.nn.silu(gate_pre) * up_pre).astype(jnp.bfloat16)
    mlp_part = jnp.dot(activated, w_down, preferred_element_type=jnp.float32)
    output = tensor_sum(mlp_part, attended)
    kept_state = (
        hidden,
        inverse_one,
        normed,
        queries,
        key_rows,
        value_rows,
        mixed_rows,
        logsum,
        attended,
        inverse_two,
        normed_two,
        gate_pre,
        up_pre,
    )
    return (output, kept_state)


def layer_backward(upstream, kept_state, allowed, cosine, sine, weights):
    w_query, w_key, w_value, w_output, w_gate, w_up, w_down, attn_gain, mlp_gain = weights
    (
        hidden,
        inverse_one,
        normed,
        queries,
        key_rows,
        value_rows,
        mixed_rows,
        logsum,
        attended,
        inverse_two,
        normed_two,
        gate_pre,
        up_pre,
    ) = kept_state
    length = hidden.shape[0]
    query_heads = w_query.shape[1] // HD
    kv_heads = w_key.shape[1] // HD
    group_size = query_heads // kv_heads
    zeros = jnp.zeros_like(hidden)
    g_low = upstream.astype(jnp.bfloat16)
    grad_act = jnp.dot(g_low, w_down.T, preferred_element_type=jnp.float32)
    grad_gate_low, grad_up_low, _ = mlp_grads(gate_pre, up_pre, grad_act)
    mlp_input_part = jnp.dot(grad_gate_low, w_gate.T, preferred_element_type=jnp.float32) + jnp.dot(
        grad_up_low, w_up.T, preferred_element_type=jnp.float32
    )
    grad_normed_two = tensor_sum(mlp_input_part, zeros)
    grad_mlp_gain, grad_norm_two = norm_backward(grad_normed_two, attended, inverse_two, mlp_gain)
    grad_attended = upstream + grad_norm_two
    grad_att_low = grad_attended.astype(jnp.bfloat16)
    grad_mixed = jnp.dot(grad_att_low, w_output.T, preferred_element_type=jnp.float32).astype(
        jnp.bfloat16
    )
    grad_mixed = grad_mixed.reshape(length, kv_heads, group_size, HD)
    grad_queries, grad_keys, grad_values = attention_backward(
        queries, key_rows, value_rows, mixed_rows, logsum, grad_mixed, allowed
    )
    grad_query_low = (
        rotate(grad_queries.reshape(length, query_heads, HD), cosine, sine, -1.0)
        .astype(jnp.bfloat16)
        .reshape(length, query_heads * HD)
    )
    grad_key_low = (
        rotate(grad_keys, cosine, sine, -1.0).astype(jnp.bfloat16).reshape(length, kv_heads * HD)
    )
    grad_value_low = grad_values.astype(jnp.bfloat16).reshape(length, kv_heads * HD)
    attn_input_part = (
        jnp.dot(grad_query_low, w_query.T, preferred_element_type=jnp.float32)
        + jnp.dot(grad_key_low, w_key.T, preferred_element_type=jnp.float32)
        + jnp.dot(grad_value_low, w_value.T, preferred_element_type=jnp.float32)
    )
    grad_normed = tensor_sum(attn_input_part, zeros)
    grad_attn_gain, grad_norm_one = norm_backward(grad_normed, hidden, inverse_one, attn_gain)
    grad_hidden = grad_attended + grad_norm_one
    sent = (
        jnp.concatenate(
            [mixed_rows.reshape(length, query_heads * HD), grad_query_low, grad_key_low, grad_value_low],
            axis=1,
        ).astype(jnp.float32),
        normed_two.astype(jnp.float32),
        g_low.astype(jnp.float32),
        normed.astype(jnp.float32),
        grad_att_low.astype(jnp.float32),
        grad_attn_gain,
        grad_mlp_gain,
    )
    return grad_hidden, sent


def mlp_grads(gate_pre, up_pre, grad_act):
    sigmoid_gate = jax.nn.sigmoid(gate_pre)
    grad_gate_low = (
        grad_act * up_pre * sigmoid_gate * (1.0 + gate_pre * (1.0 - sigmoid_gate))
    ).astype(jnp.bfloat16)
    grad_up_low = (grad_act * gate_pre * sigmoid_gate).astype(jnp.bfloat16)
    activated = (gate_pre * sigmoid_gate * up_pre).astype(jnp.bfloat16)
    return grad_gate_low, grad_up_low, activated


def over_tokens(left, right):
    return lax.dot_general(
        left, right, (((0,), (0,)), ((), ())), preferred_element_type=jnp.float32
    )


def shards(
    hidden_in,
    cotangent,
    segment_ids,
    positions,
    w_query,
    w_key,
    w_value,
    w_output,
    w_gate,
    w_up,
    w_down,
    attn_gain,
    mlp_gain,
):
    n = lax.axis_size("dp")
    dp = lax.axis_index("dp")
    weights_all = (w_query, w_key, w_value, w_output, w_gate, w_up, w_down, attn_gain, mlp_gain)
    length, width = hidden_in.shape
    piece = width // n
    cosine, sine = rotary_tables(positions[0])
    segments = segment_ids[0]
    token_order = jnp.arange(length)
    allowed = (segments[:, None] == segments[None, :]) & (
        token_order[None, :] <= token_order[:, None]
    )
    layer_weights = [
        tuple((weight[which_layer] for weight in weights_all)) for which_layer in range(LAYERS)
    ]
    kept_list = []
    hidden = hidden_in
    for which_layer in range(LAYERS):
        hidden, kept_state = layer_forward(
            hidden, allowed, cosine, sine, layer_weights[which_layer]
        )
        kept_list.append(kept_state)
    upstream = cotangent
    sent_layers = [None] * LAYERS
    for which_layer in reversed(range(LAYERS)):
        upstream, sent_layers[which_layer] = layer_backward(
            upstream, kept_list[which_layer], allowed, cosine, sine, layer_weights[which_layer]
        )

    def by_piece(rows):
        return jnp.transpose(rows.reshape(rows.shape[0], n, piece), (1, 0, 2))

    own, shared, sliced = [], [], []
    for sent in sent_layers:
        own.append(sent[0])
        shared.extend(sent[1:3])
        sliced.extend([by_piece(sent[3]), by_piece(sent[4])])
    gains = jnp.stack([sent[5] for sent in sent_layers] + [sent[6] for sent in sent_layers])
    gains = jnp.concatenate([gains, jnp.zeros_like(gains)], axis=0)
    sliced.append(by_piece(gains))
    gathered = gather(n, own, shared, sliced)
    whole = len(own) + len(shared)
    heads = w_query.shape[2]
    kv = w_key.shape[2]
    grads = [[] for _ in range(7)]
    for l in range(LAYERS):
        state = gathered[l].astype(jnp.bfloat16)
        normed_two = gathered[LAYERS + 2 * l].astype(jnp.bfloat16)
        g_low = gathered[LAYERS + 2 * l + 1].astype(jnp.bfloat16)
        normed = gathered[whole + 2 * l].reshape(n * length, piece).astype(jnp.bfloat16)
        grad_att = gathered[whole + 2 * l + 1].reshape(n * length, piece).astype(jnp.bfloat16)
        gate_pre = jnp.dot(normed_two, w_gate[l], preferred_element_type=jnp.float32)
        up_pre = jnp.dot(normed_two, w_up[l], preferred_element_type=jnp.float32)
        grad_act = jnp.dot(g_low, w_down[l].T, preferred_element_type=jnp.float32)
        grad_gate_low, grad_up_low, activated = mlp_grads(gate_pre, up_pre, grad_act)
        my_normed_two = lax.dynamic_slice_in_dim(normed_two, dp * piece, piece, 1)
        my_g = lax.dynamic_slice_in_dim(g_low, dp * piece, piece, 1)
        mixed = state[:, :heads]
        grad_qkv = over_tokens(normed, state[:, heads:])
        grads[0].append(grad_qkv[:, :heads])
        grads[1].append(grad_qkv[:, heads : heads + kv])
        grads[2].append(grad_qkv[:, heads + kv :])
        grads[3].append(over_tokens(mixed, grad_att))
        grads[4].append(over_tokens(my_normed_two, grad_gate_low))
        grads[5].append(over_tokens(my_normed_two, grad_up_low))
        grads[6].append(over_tokens(activated, my_g))
    gain_sums = jnp.sum(gathered[-1], axis=0)
    return (
        hidden,
        upstream,
        *[jnp.stack(g) for g in grads],
        gain_sums[:LAYERS],
        gain_sums[LAYERS : 2 * LAYERS],
    )


def solution(mesh):
    return jax.shard_map(
        shards,
        mesh=mesh,
        in_specs=(
            P("dp", None),
            P("dp", None),
            P("dp", None),
            P("dp", None),
            P(None, None, "tensor"),
            P(None, None, "tensor"),
            P(None, None, "tensor"),
            P(None, "tensor", None),
            P(None, None, "tensor"),
            P(None, None, "tensor"),
            P(None, "tensor", None),
            P(),
            P(),
        ),
        out_specs=(
            P("dp", None),
            P("dp", None),
            P(None, "dp", "tensor"),
            P(None, "dp", "tensor"),
            P(None, "dp", "tensor"),
            P(None, "tensor", "dp"),
            P(None, "dp", "tensor"),
            P(None, "dp", "tensor"),
            P(None, "tensor", "dp"),
            P(None, "dp"),
            P(None, "dp"),
        ),
        check_vma=False,
    )
```

```python
import functools

import jax
import jax.numpy as jnp
from jax import lax
from jax.experimental import pallas as pl
from jax.experimental.pallas import tpu as pltpu
from jax.sharding import PartitionSpec as P

HD = 96
LAYERS = 2
TILE = 256
ROWS = 16
MESH = pl.DeviceIdType.MESH


epsilon = 1e-05
rope_base = 100000.0
masked_score = -1e30
low = jnp.bfloat16
full = jnp.float32


def nn(a, b):
    return lax.dot_general(a, b, (((1,), (0,)), ((), ())), preferred_element_type=full)


def nt(a, b):
    return lax.dot_general(a, b, (((1,), (1,)), ((), ())), preferred_element_type=full)


def tn(a, b):
    return lax.dot_general(a, b, (((0,), (0,)), ((), ())), preferred_element_type=full)


def mlp_grads(gate_pre, up_pre, grad_act):
    sigmoid_gate = jax.nn.sigmoid(gate_pre)
    grad_gate_low = (
        grad_act * up_pre * sigmoid_gate * (1.0 + gate_pre * (1.0 - sigmoid_gate))
    ).astype(low)
    grad_up_low = (grad_act * gate_pre * sigmoid_gate).astype(low)
    activated = (gate_pre * sigmoid_gate * up_pre).astype(low)
    return grad_gate_low, grad_up_low, activated


def each(count, body):
    def step(i, carry):
        body(i)
        return carry

    lax.fori_loop(0, count, step, 0)


def columns(start, size):
    return pl.ds(pl.multiple_of(start, 128), size)


def layers_kernel(n, *refs):
    (
        hidden_in,
        cotangent,
        cosine,
        sine,
        allowed,
        attn_gain,
        mlp_gain,
        w_query,
        w_key,
        w_value,
        w_output,
        w_gate,
        w_up,
        w_down,
        hidden_out,
        grad_input,
        mixed_all,
        qkv_all,
        normed_two_all,
        g_all,
        normed_all,
        grad_att_all,
        gains_all,
        v_query,
        v_key,
        v_value,
        v_output,
        v_gate,
        v_up,
        v_down,
        stream,
        grads,
        upstream,
        normed_low,
        left_low,
        right_low,
        gate_pre,
        up_pre,
        query_t,
        key_t,
        value_t,
        mixed_t,
        logsum,
        mixed_out,
        qkv_out,
        normed_two_out,
        g_out,
        normed_out,
        grad_att_out,
        gains_out,
        gain_rows,
        wide,
        part,
        from_core,
        half,
        from_y,
        w_sem,
        sum_send,
        sum_recv,
        z_send,
        z_recv,
        x_send,
        x_recv,
        c_send,
        c_recv,
        a_send,
        a_recv,
        b_send,
        b_recv,
        local,
    ) = refs
    length, width = hidden_in.shape
    heads = w_query.shape[2] // HD
    kv_heads = w_key.shape[2] // HD
    share = heads // kv_heads
    hidden_units = w_gate.shape[2]
    piece = width // n
    side_width = width // 2
    chunks = side_width // TILE
    turn = HD // 2
    scale = HD ** (-0.5)

    dp = lax.axis_index("dp")
    tensor = lax.axis_index("tensor")
    core = tensor % 2
    side = dp % 2
    group = dp // 2
    groups = n // 2
    core_peer = (dp, tensor + 1 - 2 * core)
    y_peer = (dp, lax.rem(tensor + 2, 4))
    x_peer = (dp + 1 - 2 * side, tensor)

    stored = (w_query, w_key, w_value, w_output, w_gate, w_up, w_down)
    held = (v_query, v_key, v_value, v_output, v_gate, v_up, v_down)
    loads = {}
    for l in range(LAYERS):
        for i, (src, dst) in enumerate(zip(stored, held)):
            loads[l, i] = pltpu.make_async_copy(src.at[l], dst.at[l], w_sem.at[l, i])
            loads[l, i].start()

    barrier = pltpu.get_barrier_semaphore()
    greeted = [core_peer, y_peer] + [(lax.rem(dp + k, n), tensor) for k in range(1, n)]
    for peer in greeted:
        pl.semaphore_signal(barrier, inc=1, device_id=peer, device_id_type=MESH)
    pl.semaphore_wait(barrier, len(greeted))

    def remote(src, dst, s, r, peer):
        return pltpu.make_async_remote_copy(
            src_ref=src, dst_ref=dst, send_sem=s, recv_sem=r, device_id=peer, device_id_type=MESH
        )

    unsent = []
    unreceived = []

    ways = {}
    kinds = {
        "mixed": (0, mixed_out, mixed_all, False),
        "qkv": (1, qkv_out, qkv_all, False),
        "normed_two": (2, normed_two_out, normed_two_all, True),
        "g": (3, g_out, g_all, True),
    }

    def block(kind, l, index):
        _, _, everywhere, shared = kinds[kind]
        rows = pl.ds(pl.multiple_of(index * length, 8), length)
        if shared:
            return everywhere.at[l, rows, columns(core * side_width, side_width)]
        return everywhere.at[l, rows]

    def send_own(kind, l):
        a, own, everywhere, shared = kinds[kind]
        slot = a * LAYERS + l
        mine = own.at[l, :, columns(core * side_width, side_width)] if shared else own.at[l]
        for k in range(groups):
            if k == 0:
                c = remote(
                    mine, block(kind, l, dp), x_send.at[slot, 0], x_recv.at[slot, 0], x_peer
                )
            else:
                peer = (lax.rem(group + k, groups) * 2 + side, tensor)
                c = remote(
                    mine, block(kind, l, dp), z_send.at[slot, k], z_recv.at[slot, k], peer
                )
            c.start()
            ways[kind, l, "own", k] = c
            unsent.append(c)
        rows = pl.ds(pl.multiple_of(dp * length, 8), length)
        c = pltpu.make_async_copy(own.at[l], everywhere.at[l, rows], local.at[slot])
        c.start()
        unreceived.append(c.wait)

    def to_core(kind, l, index, k):
        a = kinds[kind][0]
        if kinds[kind][3]:
            slot = (a - 2) * LAYERS + l
            here = block(kind, l, index)
            c = remote(here, here, c_send.at[slot, k], c_recv.at[slot, k], core_peer)
            c.start()
            unsent.append(c)
            unreceived.append(c.wait_recv)

    def pass_on(kind, l):
        slot = kinds[kind][0] * LAYERS + l
        for k in range(1, groups):
            ways[kind, l, "own", k].wait_recv()
            source = lax.rem(group + groups - k, groups) * 2 + side
            here = block(kind, l, source)
            c = remote(here, here, x_send.at[slot, k], x_recv.at[slot, k], x_peer)
            c.start()
            ways[kind, l, "x", k] = c
            unsent.append(c)
            to_core(kind, l, source, k)

    def take_across(kind, l):
        for k in range(groups):
            ways[kind, l, "own" if k == 0 else "x", k].wait_recv()
            source = lax.rem(group + groups - k, groups) * 2 + 1 - side
            to_core(kind, l, source, groups + k)

    slices = {
        "normed": (0, normed_out, normed_all, True),
        "grad_att": (1, grad_att_out, grad_att_all, True),
        "gains": (2, gains_out, gains_all, False),
    }

    def sliced(kind, ref, l, index):
        if slices[kind][3]:
            rows = pl.ds(pl.multiple_of(core * (length // 2), 8), length // 2)
            return ref.at[l, index, rows]
        return ref.at[l, index]

    def send_slices(kind, l):
        b, own, everywhere, halves = slices[kind]
        slot = b * LAYERS + l
        for k in range(1, n):
            to = lax.rem(dp + k, n)
            c = remote(
                sliced(kind, own, l, to),
                sliced(kind, everywhere, l, dp),
                a_send.at[slot, k],
                a_recv.at[slot, k],
                (to, tensor),
            )
            c.start()
            ways[kind, l, k] = c
            unsent.append(c)
        c = pltpu.make_async_copy(
            own.at[l, dp], everywhere.at[l, dp], local.at[4 * LAYERS + slot]
        )
        c.start()
        unreceived.append(c.wait)

    def take_slices(kind, l):
        b, _, everywhere, halves = slices[kind]
        slot = b * LAYERS + l
        for k in range(1, n):
            ways[kind, l, k].wait_recv()
            if halves:
                source = lax.rem(dp + n - k, n)
                here = sliced(kind, everywhere, l, source)
                c = remote(here, here, b_send.at[slot, k], b_recv.at[slot, k], core_peer)
                c.start()
                unsent.append(c)
                unreceived.append(c.wait_recv)

    def cut(dst, l, src):
        for t in range(n):
            dst[l, t] = src[:, t * piece : (t + 1) * piece]

    def tensor_sum(j, tile, base, dest, meanwhile):
        def copy(stage, k, src, dst, peer):
            return remote(src, dst, sum_send.at[j, stage, k], sum_recv.at[j, stage, k], peer)

        def at(k):
            return pl.ds(pl.multiple_of(k * TILE, 128), TILE)

        def mine(k):
            return columns(core * side_width + k * TILE, TILE)

        def other(k):
            return columns((1 - core) * side_width + k * TILE, TILE)

        def first(k):
            return copy(0, k, part.at[:, at(k)], from_core.at[j, :, at(k)], core_peer)

        def second(k):
            return copy(1, k, half.at[:, at(k)], from_y.at[j, :, at(k)], y_peer)

        def third(k):
            return copy(2, k, dest.at[:, mine(k)], dest.at[:, mine(k)], core_peer)

        def begin(k):
            part[:, at(k)] = tile(other(k))
            first(k).start()

        def middle(k):
            own = tile(mine(k))
            first(k).wait_recv()
            half[:, at(k)] = own + from_core[j, :, at(k)]
            second(k).start()

        def finish(k):
            second(k).wait_recv()
            total = half[:, at(k)] + from_y[j, :, at(k)]
            if base is not None:
                total = base[:, mine(k)] + total
            dest[:, mine(k)] = total
            third(k).start()

        def settle(k):
            third(k).wait_recv()
            first(k).wait_send()
            second(k).wait_send()
            third(k).wait_send()

        each(chunks, begin)
        each(chunks, middle)
        meanwhile()
        each(chunks, finish)
        each(chunks, settle)

    def inverse_rms(values):
        return lax.rsqrt(jnp.mean(values * values, axis=-1, keepdims=True) + epsilon)

    def normalize(src, gain, l, out, out_wide):
        def rows_of(i):
            rows = pl.ds(pl.multiple_of(i * ROWS, ROWS), ROWS)
            values = src[rows, :]
            normed = (values * inverse_rms(values) * gain[l : l + 1, :]).astype(low)
            out[rows, :] = normed
            out_wide[rows, :] = normed.astype(full)

        each(length // ROWS, rows_of)

    def norm_backward(grad, values_ref, gain, l, row, before, out, out_low, out_wide):
        def rows_of(i, total):
            rows = pl.ds(pl.multiple_of(i * ROWS, ROWS), ROWS)
            values = values_ref[rows, :]
            grad_normed = grad[rows, :]
            inverse = inverse_rms(values)
            normalized = values * inverse
            term = grad_normed * normalized
            total = total + term[:8] + term[8:]
            scaled = grad_normed * gain[l : l + 1, :]
            back = inverse * (
                scaled - normalized * jnp.mean(scaled * normalized, axis=-1, keepdims=True)
            )
            after = before[rows, :] + back
            out[rows, :] = after
            if out_low is not None:
                after_low = after.astype(low)
                out_low[rows, :] = after_low
                out_wide[rows, :] = after_low.astype(full)
            return total

        total = lax.fori_loop(0, length // ROWS, rows_of, jnp.zeros((8, width), full))
        gain_rows[row : row + 1, :] = jnp.sum(total, axis=0, keepdims=True)

    def turned(values, direction):
        u, w = values[:turn], values[turn:]
        c, s = cosine[...], sine[...]
        return jnp.concatenate([u * c - direction * w * s, w * c + direction * u * s], axis=0)

    def head(ref, l, h):
        return ref[l, h * HD : (h + 1) * HD, :]

    def scores_t(l, h):
        raw = tn(head(key_t, l, h // share), head(query_t, l, h)) * scale
        return jnp.where(allowed[...] > 0.5, raw, masked_score)

    def attend(l):
        for i in range(3):
            loads[l, i].wait()
        source = normed_low[...]
        for ref, dst, count, rope in (
            (v_query, query_t, heads, True),
            (v_key, key_t, kv_heads, True),
            (v_value, value_t, kv_heads, False),
        ):
            projected = jnp.transpose(nn(source, ref[l]))
            for h in range(count):
                values = projected[h * HD : (h + 1) * HD]
                values = turned(values, 1.0) if rope else values
                dst[l, h * HD : (h + 1) * HD, :] = values.astype(low)
        for h in range(heads):
            scores = scores_t(l, h)
            row_max = jnp.max(scores, axis=0, keepdims=True)
            exponent = jnp.exp(scores - row_max)
            row_total = jnp.sum(exponent, axis=0, keepdims=True)
            probabilities = (exponent / row_total).astype(low)
            logsum[l, h : h + 1, :] = row_max + jnp.log(row_total)
            mixed = nn(head(value_t, l, h // share), probabilities)
            mixed_t[l, h * HD : (h + 1) * HD, :] = mixed.astype(low).astype(full)
        mixed = jnp.transpose(mixed_t[l])
        mixed_out[l] = mixed
        left_low[:, : heads * HD] = mixed.astype(low)

    def attention_back(l):
        grad_mixed_t = jnp.transpose(nt(normed_low[...], v_output[l]).astype(low).astype(full))
        for g in range(kv_heads):
            grad_value = jnp.zeros((HD, length), full)
            grad_key = jnp.zeros((HD, length), full)
            for h in range(g * share, (g + 1) * share):
                grad_mixed = grad_mixed_t[h * HD : (h + 1) * HD]
                grad_mixed_low = grad_mixed.astype(low)
                again = jnp.exp(scores_t(l, h) - logsum[l, h : h + 1, :])
                grad_value += nt(grad_mixed_low, again.astype(low))
                grad_probs = tn(head(value_t, l, g), grad_mixed_low)
                row_dot = jnp.sum(grad_mixed * head(mixed_t, l, h), axis=0, keepdims=True)
                grad_scores = (again * (grad_probs - row_dot) * scale).astype(low)
                grad_query = nn(head(key_t, l, g), grad_scores)
                grad_key += nt(head(query_t, l, h), grad_scores)
                wide[h * HD : (h + 1) * HD, :] = turned(grad_query, -1.0).astype(low).astype(full)
            at = (heads + g) * HD
            wide[at : at + HD, :] = turned(grad_key, -1.0).astype(low).astype(full)
            at = (heads + kv_heads + g) * HD
            wide[at : at + HD, :] = grad_value.astype(low).astype(full)
        rows = jnp.transpose(wide[...])
        qkv_out[l] = rows
        left_low[:, : rows.shape[1]] = rows.astype(low)

    step = hidden_units // 2
    nothing = lambda: None

    def attention_layer(l, meanwhile):
        normalize(stream.at[2 * l], attn_gain, l, normed_low, normed_two_out.at[l])
        cut(normed_out, l, normed_two_out.at[l])
        send_slices("normed", l)
        attend(l)
        send_own("mixed", l)
        loads[l, 3].wait()
        tensor_sum(
            2 * l,
            lambda at: nn(left_low[:, : heads * HD], v_output[l, :, at]),
            stream.at[2 * l],
            stream.at[2 * l + 1],
            meanwhile,
        )

    def mlp_layer(l, meanwhile):
        normalize(stream.at[2 * l + 1], mlp_gain, l, normed_low, normed_two_out.at[l])
        send_own("normed_two", l)
        loads[l, 4].wait()
        loads[l, 5].wait()

        def units(i):
            at = columns(i * TILE, TILE)
            source = normed_low[...]
            gate = nn(source, v_gate[l, :, at])
            up = nn(source, v_up[l, :, at])
            gate_pre[l, :, at] = gate
            up_pre[l, :, at] = up
            left_low[:, at] = (gate * jax.nn.sigmoid(gate) * up).astype(low)

        each(hidden_units // TILE, units)
        loads[l, 6].wait()
        tensor_sum(
            2 * l + 1,
            lambda at: nn(left_low[...], v_down[l, :, at]),
            stream.at[2 * l + 1],
            stream.at[2 * l + 2],
            meanwhile,
        )

    def mlp_back(l, meanwhile):
        def units(i):
            at = columns(i * TILE, TILE)
            grad_act = nt(normed_low[...], v_down[l, at, :])
            left, right, _ = mlp_grads(gate_pre[l, :, at], up_pre[l, :, at], grad_act)
            left_low[:, at] = left
            right_low[:, at] = right

        each(hidden_units // TILE, units)
        j = 2 * LAYERS + 2 * (LAYERS - 1 - l)
        tensor_sum(
            j,
            lambda at: nt(left_low[...], v_gate[l, at, :]) + nt(right_low[...], v_up[l, at, :]),
            None,
            grads.at[j - 2 * LAYERS],
            meanwhile,
        )
        norm_backward(
            grads.at[j - 2 * LAYERS],
            stream.at[2 * l + 1],
            mlp_gain,
            l,
            LAYERS + l,
            upstream,
            upstream,
            normed_low,
            part_wide,
        )
        cut(grad_att_out, l, part_wide)
        send_slices("grad_att", l)

    part_wide = grads.at[2 * LAYERS]

    def attention_layer_back(l, meanwhile):
        attention_back(l)
        send_own("qkv", l)
        j = 2 * LAYERS + 2 * (LAYERS - 1 - l) + 1
        q_end, k_end = heads * HD, (heads + kv_heads) * HD
        v_end = (heads + 2 * kv_heads) * HD
        tensor_sum(
            j,
            lambda at: nt(left_low[:, :q_end], v_query[l, at, :])
            + nt(left_low[:, q_end:k_end], v_key[l, at, :])
            + nt(left_low[:, k_end:v_end], v_value[l, at, :]),
            None,
            grads.at[j - 2 * LAYERS],
            meanwhile,
        )
        last = l == 0
        norm_backward(
            grads.at[j - 2 * LAYERS],
            stream.at[2 * l],
            attn_gain,
            l,
            l,
            upstream,
            grad_input if last else upstream,
            None if last else normed_low,
            None if last else g_out.at[l - 1],
        )
        if not last:
            send_own("g", l - 1)

    stream[0] = hidden_in[...]
    upstream[...] = cotangent[...]
    g_out[LAYERS - 1] = cotangent[...].astype(low).astype(full)
    send_own("g", LAYERS - 1)
    gain_rows[...] = jnp.zeros_like(gain_rows)

    def steps(*calls):
        def run():
            for call, kind, l in calls:
                call(kind, l)

        return run

    attention_layer(0, nothing)
    mlp_layer(0, steps((pass_on, "g", 1), (take_slices, "normed", 0)))
    attention_layer(1, steps((pass_on, "mixed", 0), (take_across, "g", 1)))
    mlp_layer(1, steps((take_across, "mixed", 0)))
    hidden_out[...] = stream[2 * LAYERS]
    normed_low[...] = g_out[LAYERS - 1].astype(low)
    mlp_back(1, steps((pass_on, "normed_two", 0), (take_slices, "normed", 1)))
    attention_layer_back(1, steps((pass_on, "mixed", 1), (take_across, "normed_two", 0)))
    mlp_back(0, steps((pass_on, "normed_two", 1), (take_across, "mixed", 1)))
    attention_layer_back(0, steps((pass_on, "qkv", 1), (take_slices, "grad_att", 1)))
    cut(gains_out, 0, gain_rows)
    send_slices("gains", 0)
    for call, kind, l in (
        (take_across, "normed_two", 1),
        (pass_on, "g", 0),
        (take_across, "qkv", 1),
        (pass_on, "qkv", 0),
        (take_across, "g", 0),
        (take_slices, "grad_att", 0),
        (take_across, "qkv", 0),
        (take_slices, "gains", 0),
    ):
        call(kind, l)
    for wait in unreceived:
        wait()
    for c in unsent:
        c.wait_send()


def layers(n, hidden_in, cotangent, cosine, sine, allowed, attn_gain, mlp_gain, weights):
    length, width = hidden_in.shape
    w_query, w_key, w_value, w_output, w_gate, w_up, w_down = weights
    q_width, kv_width, hidden_units = w_query.shape[2], w_key.shape[2], w_gate.shape[2]
    qkv_width = q_width + 2 * kv_width
    piece = width // n
    f32 = lambda *shape: jax.ShapeDtypeStruct(shape, full)
    out_shape = [
        f32(length, width),
        f32(length, width),
        f32(LAYERS, n * length, q_width),
        f32(LAYERS, n * length, qkv_width),
        f32(LAYERS, n * length, width),
        f32(LAYERS, n * length, width),
        f32(LAYERS, n, length, piece),
        f32(LAYERS, n, length, piece),
        f32(1, n, 8, piece),
    ]
    vmem = pl.BlockSpec(memory_space=pltpu.VMEM)
    anywhere = pl.BlockSpec(memory_space=pl.ANY)
    dma = pltpu.SemaphoreType.DMA
    keep = lambda dtype, *shape: pltpu.VMEM(shape, dtype)
    sums = 4 * LAYERS
    chunks = width // 2 // TILE
    return pl.pallas_call(
        functools.partial(layers_kernel, n),
        out_shape=out_shape,
        in_specs=[vmem] * 7 + [anywhere] * 7,
        out_specs=[vmem] * 2 + [anywhere] * 7,
        scratch_shapes=[keep(low, *w.shape) for w in weights]
        + [
            keep(full, 2 * LAYERS + 1, length, width),
            keep(full, 2 * LAYERS + 1, length, width),
            keep(full, length, width),
            keep(low, length, width),
            keep(low, length, hidden_units),
            keep(low, length, hidden_units),
            keep(full, LAYERS, length, hidden_units),
            keep(full, LAYERS, length, hidden_units),
            keep(low, LAYERS, q_width, length),
            keep(low, LAYERS, kv_width, length),
            keep(low, LAYERS, kv_width, length),
            keep(full, LAYERS, q_width, length),
            keep(full, LAYERS, 8, length),
            keep(full, LAYERS, length, q_width),
            keep(full, LAYERS, length, qkv_width),
            keep(full, LAYERS, length, width),
            keep(full, LAYERS, length, width),
            keep(full, LAYERS, n, length, piece),
            keep(full, LAYERS, n, length, piece),
            keep(full, 1, n, 8, piece),
            keep(full, 8, width),
            keep(full, qkv_width, length),
            keep(full, length, width // 2),
            keep(full, sums, length, width // 2),
            keep(full, length, width // 2),
            keep(full, sums, length, width // 2),
            dma((LAYERS, 7)),
            dma((sums, 3, chunks)),
            dma((sums, 3, chunks)),
            dma((4 * LAYERS, n // 2)),
            dma((4 * LAYERS, n // 2)),
            dma((4 * LAYERS, n // 2)),
            dma((4 * LAYERS, n // 2)),
            dma((2 * LAYERS, n)),
            dma((2 * LAYERS, n)),
            dma((3 * LAYERS, n)),
            dma((3 * LAYERS, n)),
            dma((2 * LAYERS, n)),
            dma((2 * LAYERS, n)),
            dma((7 * LAYERS,)),
        ],
        compiler_params=pltpu.CompilerParams(
            collective_id=0, has_side_effects=True, vmem_limit_bytes=66_000_000
        ),
        name="layers",
    )(hidden_in, cotangent, cosine, sine, allowed, attn_gain, mlp_gain, *weights)


def shards(
    hidden_in,
    cotangent,
    segment_ids,
    positions,
    w_query,
    w_key,
    w_value,
    w_output,
    w_gate,
    w_up,
    w_down,
    attn_gain,
    mlp_gain,
):
    n = lax.axis_size("dp")
    dp = lax.axis_index("dp")
    weights = (w_query, w_key, w_value, w_output, w_gate, w_up, w_down)
    length, width = hidden_in.shape
    piece = width // n
    half_dim = HD // 2
    frequencies = rope_base ** (-(jnp.arange(half_dim).astype(jnp.float32) * 2.0 / HD))
    angles = frequencies[:, None] * positions[0].astype(jnp.float32)[None, :]
    segments = segment_ids[0]
    token_order = jnp.arange(length)
    allowed = (segments[:, None] == segments[None, :]) & (
        token_order[:, None] <= token_order[None, :]
    )
    hidden, grad_input, mixed_all, qkv_all, normed_two_all, g_all, normed_all, grad_att_all, gains = (
        layers(
            n,
            hidden_in,
            cotangent,
            jnp.cos(angles),
            jnp.sin(angles),
            allowed.astype(jnp.float32),
            attn_gain,
            mlp_gain,
            weights,
        )
    )
    heads = w_query.shape[2]
    kv = w_key.shape[2]
    grads = [[] for _ in range(7)]
    for l in range(LAYERS):
        mixed = mixed_all[l].astype(low)
        qkv = qkv_all[l].astype(low)
        normed_two = normed_two_all[l].astype(low)
        g_low = g_all[l].astype(low)
        normed = normed_all[l].reshape(n * length, piece).astype(low)
        grad_att = grad_att_all[l].reshape(n * length, piece).astype(low)
        gate_pre = nn(normed_two, w_gate[l])
        up_pre = nn(normed_two, w_up[l])
        grad_act = nt(g_low, w_down[l])
        grad_gate_low, grad_up_low, activated = mlp_grads(gate_pre, up_pre, grad_act)
        my_normed_two = lax.dynamic_slice_in_dim(normed_two, dp * piece, piece, 1)
        my_g = lax.dynamic_slice_in_dim(g_low, dp * piece, piece, 1)
        grad_qkv = tn(normed, qkv)
        grads[0].append(grad_qkv[:, :heads])
        grads[1].append(grad_qkv[:, heads : heads + kv])
        grads[2].append(grad_qkv[:, heads + kv :])
        grads[3].append(tn(mixed, grad_att))
        grads[4].append(tn(my_normed_two, grad_gate_low))
        grads[5].append(tn(my_normed_two, grad_up_low))
        grads[6].append(tn(activated, my_g))
    gain_sums = jnp.sum(gains[0], axis=0)
    return (
        hidden,
        grad_input,
        *[jnp.stack(g) for g in grads],
        gain_sums[:LAYERS],
        gain_sums[LAYERS : 2 * LAYERS],
    )


def solution(mesh):
    return jax.shard_map(
        shards,
        mesh=mesh,
        in_specs=(
            P("dp", None),
            P("dp", None),
            P("dp", None),
            P("dp", None),
            P(None, None, "tensor"),
            P(None, None, "tensor"),
            P(None, None, "tensor"),
            P(None, "tensor", None),
            P(None, None, "tensor"),
            P(None, None, "tensor"),
            P(None, "tensor", None),
            P(),
            P(),
        ),
        out_specs=(
            P("dp", None),
            P("dp", None),
            P(None, "dp", "tensor"),
            P(None, "dp", "tensor"),
            P(None, "dp", "tensor"),
            P(None, "tensor", "dp"),
            P(None, "dp", "tensor"),
            P(None, "dp", "tensor"),
            P(None, "tensor", "dp"),
            P(None, "dp"),
            P(None, "dp"),
        ),
        check_vma=False,
    )
```

```python
import functools
import math

import jax
import jax.numpy as jnp
from jax import lax
from jax.experimental import pallas as pl
from jax.experimental.pallas import tpu as pltpu
from jax.sharding import PartitionSpec as P

HD = 96
LAYERS = 2
TILE = 256
ROWS = 16
TOKENS = 256
SHARED_Y = (("normed_two", 0), ("g", 0))
MESH = pl.DeviceIdType.MESH


epsilon = 1e-05
rope_base = 100000.0
masked_score = -1e30
low = jnp.bfloat16
full = jnp.float32


def nn(a, b):
    return lax.dot_general(a, b, (((1,), (0,)), ((), ())), preferred_element_type=full)


def nt(a, b):
    return lax.dot_general(a, b, (((1,), (1,)), ((), ())), preferred_element_type=full)


def tn(a, b):
    return lax.dot_general(a, b, (((0,), (0,)), ((), ())), preferred_element_type=full)


def mlp_grads(gate_pre, up_pre, grad_act):
    sigmoid_gate = jax.nn.sigmoid(gate_pre)
    grad_gate_low = (
        grad_act * up_pre * sigmoid_gate * (1.0 + gate_pre * (1.0 - sigmoid_gate))
    ).astype(low)
    grad_up_low = (grad_act * gate_pre * sigmoid_gate).astype(low)
    activated = (gate_pre * sigmoid_gate * up_pre).astype(low)
    return grad_gate_low, grad_up_low, activated


def each(count, body):
    def step(i, carry):
        body(i)
        return carry

    lax.fori_loop(0, count, step, 0)


def columns(start, size):
    return pl.ds(pl.multiple_of(start, 128), size)


def layers_kernel(n, *refs):
    (
        hidden_in,
        cotangent,
        cosine,
        sine,
        allowed,
        attn_gain,
        mlp_gain,
        w_query,
        w_key,
        w_value,
        w_output,
        w_gate,
        w_up,
        w_down,
        hidden_out,
        grad_input,
        grad_q,
        grad_k,
        grad_v,
        grad_o,
        grad_g,
        grad_u,
        grad_d,
        mixed_all,
        qkv_all,
        normed_two_all,
        g_all,
        normed_all,
        grad_att_all,
        gains_all,
        v_query,
        v_key,
        v_value,
        v_output,
        v_gate,
        v_up,
        v_down,
        stream,
        grads,
        upstream,
        normed_low,
        left_low,
        right_low,
        gate_pre,
        up_pre,
        query_t,
        key_t,
        value_t,
        mixed_t,
        logsum,
        mixed_out,
        qkv_out,
        normed_two_out,
        g_out,
        slices_out,
        gains_out,
        gain_rows,
        wide,
        part,
        from_core,
        half,
        from_y,
        token_a,
        token_b,
        low_a,
        low_b,
        cut_a,
        cut_b,
        sum_g,
        sum_u,
        sum_d,
        state_qkv,
        state_mixed,
        state_a,
        state_b,
        sum_q,
        sum_k,
        sum_v,
        sum_o,
        w_sem,
        sum_send,
        sum_recv,
        z_send,
        z_recv,
        x_send,
        x_recv,
        c_send,
        c_recv,
        a_send,
        a_recv,
        b_send,
        b_recv,
        y_send,
        y_recv,
        d_send,
        d_recv,
        local,
        edge,
        fetch,
    ) = refs
    length, width = hidden_in.shape
    heads = w_query.shape[2] // HD
    kv_heads = w_key.shape[1] // HD
    share = heads // kv_heads
    hidden_units = w_gate.shape[2]
    piece = width // n
    side_width = width // 2
    chunks = side_width // TILE
    turn = HD // 2
    scale = HD ** (-0.5)

    dp = lax.axis_index("dp")
    tensor = lax.axis_index("tensor")
    core = tensor % 2
    side = dp % 2
    group = dp // 2
    groups = n // 2
    core_peer = (dp, tensor + 1 - 2 * core)
    y_peer = (dp, lax.rem(tensor + 2, 4))
    x_peer = (dp + 1 - 2 * side, tensor)

    stored = (w_query, w_key, w_value, w_output, w_gate, w_up, w_down)
    held = (v_query, v_key, v_value, v_output, v_gate, v_up, v_down)
    loads = {}
    for l in range(LAYERS):
        for i, (src, dst) in enumerate(zip(stored, held)):
            loads[l, i] = pltpu.make_async_copy(src.at[l], dst.at[l], w_sem.at[l, i])
            loads[l, i].start()

    arriving = [
        pltpu.make_async_copy(hidden_in, stream.at[0], edge.at[0]),
        pltpu.make_async_copy(cotangent, upstream, edge.at[1]),
    ]
    for c in arriving:
        c.start()

    barrier = pltpu.get_barrier_semaphore()
    greeted = [core_peer, y_peer] + [(lax.rem(dp + k, n), tensor) for k in range(1, n)]
    for peer in greeted:
        pl.semaphore_signal(barrier, inc=1, device_id=peer, device_id_type=MESH)
    pl.semaphore_wait(barrier, len(greeted))

    def remote(src, dst, s, r, peer):
        return pltpu.make_async_remote_copy(
            src_ref=src, dst_ref=dst, send_sem=s, recv_sem=r, device_id=peer, device_id_type=MESH
        )

    unsent = []
    missing = {}
    leaving = {}

    ways = {}
    kinds = {
        "mixed": (0, mixed_out, mixed_all, False),
        "qkv": (1, qkv_out, qkv_all, False),
        "normed_two": (2, normed_two_out, normed_two_all, True),
        "g": (3, g_out, g_all, True),
    }

    quarter_width = width // 4

    def block(kind, l, index, owner=None):
        _, _, everywhere, shared = kinds[kind]
        rows = pl.ds(pl.multiple_of(index * length, 8), length)
        if (kind, l) in SHARED_Y:
            at = tensor if owner is None else owner
            return everywhere.at[l, rows, columns(at * quarter_width, quarter_width)]
        if shared:
            return everywhere.at[l, rows, columns(core * side_width, side_width)]
        return everywhere.at[l, rows]

    def send_own(kind, l):
        a, own, everywhere, shared = kinds[kind]
        slot = a * LAYERS + l
        if (kind, l) in SHARED_Y:
            mine = own.at[l, :, columns(tensor * quarter_width, quarter_width)]
        elif shared:
            mine = own.at[l, :, columns(core * side_width, side_width)]
        else:
            mine = own.at[l]
        for k in range(groups):
            if k == 0:
                c = remote(
                    mine, block(kind, l, dp), x_send.at[slot, 0], x_recv.at[slot, 0], x_peer
                )
            else:
                peer = (lax.rem(group + k, groups) * 2 + side, tensor)
                c = remote(
                    mine, block(kind, l, dp), z_send.at[slot, k], z_recv.at[slot, k], peer
                )
            c.start()
            ways[kind, l, "own", k] = c
            unsent.append(c)
        rows = pl.ds(pl.multiple_of(dp * length, 8), length)
        c = pltpu.make_async_copy(own.at[l], everywhere.at[l, rows], local.at[slot])
        c.start()
        missing.setdefault((kind, l), []).append(c.wait)

    def source_of(i):
        if i < groups - 1:
            return lax.rem(group + groups - 1 - i, groups) * 2 + side
        return lax.rem(group + 2 * groups - 1 - i, groups) * 2 + 1 - side

    def to_core(kind, l, i):
        a = kinds[kind][0]
        if kinds[kind][3]:
            slot = (a - 2) * LAYERS + l
            here = block(kind, l, source_of(i))
            c = remote(here, here, c_send.at[slot, i], c_recv.at[slot, i], core_peer)
            c.start()
            unsent.append(c)
            missing[kind, l].append(c.wait_recv)

    def pass_one(kind, l, k):
        slot = kinds[kind][0] * LAYERS + l
        ways[kind, l, "own", k].wait_recv()
        here = block(kind, l, source_of(k - 1))
        c = remote(here, here, x_send.at[slot, k], x_recv.at[slot, k], x_peer)
        c.start()
        ways[kind, l, "x", k] = c
        unsent.append(c)
        to_core(kind, l, k - 1)

    def pass_on(kind, l):
        for k in range(1, groups):
            pass_one(kind, l, k)

    def take_one(kind, l, k):
        ways[kind, l, "own" if k == 0 else "x", k].wait_recv()
        to_core(kind, l, groups - 1 + k)

    def take_across(kind, l):
        for k in range(groups):
            take_one(kind, l, k)

    def share_one(kind, l, i):
        slot = (kinds[kind][0] - 2) * LAYERS + l
        here = block(kind, l, source_of(i))
        c = remote(here, here, y_send.at[slot, i], y_recv.at[slot, i], y_peer)
        c.start()
        ways[kind, l, "y", i] = c
        unsent.append(c)

    def share_y(kind, l, part=0, parts=1):
        if (kind, l) in SHARED_Y:
            for i in range(part * (n - 1) // parts, (part + 1) * (n - 1) // parts):
                share_one(kind, l, i)

    def take_y(kind, l):
        if (kind, l) in SHARED_Y:
            slot = (kinds[kind][0] - 2) * LAYERS + l
            for i in range(n - 1):
                ways[kind, l, "y", i].wait_recv()
                here = block(kind, l, source_of(i), lax.rem(tensor + 2, 4))
                c = remote(here, here, d_send.at[slot, i], d_recv.at[slot, i], core_peer)
                c.start()
                unsent.append(c)
                missing[kind, l].append(c.wait_recv)

    def complete(kind, l):
        for wait in missing.pop((kind, l)):
            wait()
        if (kind, l) in leaving:
            settle_slices(kind, l)

    slices = {
        "normed": (0, slices_out, normed_all, True),
        "grad_att": (1, slices_out, grad_att_all, True),
        "gains": (2, gains_out, gains_all, False),
    }

    def sliced(kind, ref, l, index):
        if slices[kind][3]:
            rows = pl.ds(pl.multiple_of(core * (length // 2), 8), length // 2)
            return ref.at[l, index, rows]
        return ref.at[l, index]

    def send_slices(kind, l):
        b, own, everywhere, halves = slices[kind]
        slot = b * LAYERS + l
        held_at = LAYERS - 1 - l if kind == "grad_att" else l
        sent = []
        for k in range(1, n):
            to = lax.rem(dp + k, n)
            c = remote(
                sliced(kind, own, held_at, to),
                sliced(kind, everywhere, l, dp),
                a_send.at[slot, k],
                a_recv.at[slot, k],
                (to, tensor),
            )
            c.start()
            ways[kind, l, k] = c
            sent.append(c.wait_send)
        c = pltpu.make_async_copy(
            own.at[held_at, dp], everywhere.at[l, dp], local.at[4 * LAYERS + slot]
        )
        c.start()
        missing[kind, l] = []
        leaving[kind, l] = sent + [c.wait]

    def settle_slices(kind, l):
        for wait in leaving.pop((kind, l)):
            wait()

    def take_slices(kind, l):
        b, _, everywhere, halves = slices[kind]
        slot = b * LAYERS + l
        for k in range(1, n):
            ways[kind, l, k].wait_recv()
            if halves:
                source = lax.rem(dp + n - k, n)
                here = sliced(kind, everywhere, l, source)
                c = remote(here, here, b_send.at[slot, k], b_recv.at[slot, k], core_peer)
                c.start()
                unsent.append(c)
                missing[kind, l].append(c.wait_recv)

    def cut(dst, l, src):
        for t in range(n):
            dst[l, t] = src[:, t * piece : (t + 1) * piece]

    def tensor_sum(j, tile, base, dest, meanwhile):
        def copy(stage, k, src, dst, peer):
            return remote(src, dst, sum_send.at[j, stage, k], sum_recv.at[j, stage, k], peer)

        def at(k):
            return pl.ds(pl.multiple_of(k * TILE, 128), TILE)

        def mine(k):
            return columns(core * side_width + k * TILE, TILE)

        def other(k):
            return columns((1 - core) * side_width + k * TILE, TILE)

        def first(k):
            return copy(0, k, part.at[:, at(k)], from_core.at[j % 2, :, at(k)], core_peer)

        def second(k):
            return copy(1, k, half.at[:, at(k)], from_y.at[j % 2, :, at(k)], y_peer)

        def third(k):
            return copy(2, k, dest.at[:, mine(k)], dest.at[:, mine(k)], core_peer)

        def begin(k):
            part[:, at(k)] = tile(other(k))
            first(k).start()

        def middle(k):
            own = tile(mine(k))
            first(k).wait_recv()
            half[:, at(k)] = own + from_core[j % 2, :, at(k)]
            second(k).start()

        def finish(k):
            second(k).wait_recv()
            total = half[:, at(k)] + from_y[j % 2, :, at(k)]
            if base is not None:
                total = base[:, mine(k)] + total
            dest[:, mine(k)] = total
            third(k).start()

        def settle(k):
            third(k).wait_recv()
            first(k).wait_send()
            second(k).wait_send()
            third(k).wait_send()

        each(chunks, begin)
        each(chunks, middle)
        meanwhile()
        each(chunks, finish)
        each(chunks, settle)

    def inverse_rms(values):
        return lax.rsqrt(jnp.mean(values * values, axis=-1, keepdims=True) + epsilon)

    def normalize(src, gain, l, out, out_wide):
        def rows_of(i):
            rows = pl.ds(pl.multiple_of(i * ROWS, ROWS), ROWS)
            values = src[rows, :]
            normed = (values * inverse_rms(values) * gain[l : l + 1, :]).astype(low)
            out[rows, :] = normed
            out_wide[rows, :] = normed.astype(full)

        each(length // ROWS, rows_of)

    def norm_backward(grad, values_ref, gain, l, row, before, out, out_low, out_wide):
        def rows_of(i, total):
            rows = pl.ds(pl.multiple_of(i * ROWS, ROWS), ROWS)
            values = values_ref[rows, :]
            grad_normed = grad[rows, :]
            inverse = inverse_rms(values)
            normalized = values * inverse
            term = grad_normed * normalized
            total = total + term[:8] + term[8:]
            scaled = grad_normed * gain[l : l + 1, :]
            back = inverse * (
                scaled - normalized * jnp.mean(scaled * normalized, axis=-1, keepdims=True)
            )
            after = before[rows, :] + back
            out[rows, :] = after
            if out_low is not None:
                after_low = after.astype(low)
                out_low[rows, :] = after_low
                out_wide[rows, :] = after_low.astype(full)
            return total

        total = lax.fori_loop(0, length // ROWS, rows_of, jnp.zeros((8, width), full))
        gain_rows[row : row + 1, :] = jnp.sum(total, axis=0, keepdims=True)

    def turned(values, direction):
        u, w = values[:turn], values[turn:]
        c, s = cosine[...], sine[...]
        return jnp.concatenate([u * c - direction * w * s, w * c + direction * u * s], axis=0)

    def head(ref, l, h):
        return ref[l, h * HD : (h + 1) * HD, :]

    def scores_t(l, h):
        raw = tn(head(key_t, l, h // share), head(query_t, l, h)) * scale
        return jnp.where(allowed[...] > 0.5, raw, masked_score)

    def attend(l):
        for i in range(3):
            loads[l, i].wait()
        source = normed_low[...]
        for ref, dst, count, rope in (
            (v_query, query_t, heads, True),
            (v_key, key_t, kv_heads, True),
            (v_value, value_t, kv_heads, False),
        ):
            projected = jnp.transpose(nn(source, ref[l])) if ref is v_query else nt(ref[l], source)
            for h in range(count):
                values = projected[h * HD : (h + 1) * HD]
                values = turned(values, 1.0) if rope else values
                dst[l, h * HD : (h + 1) * HD, :] = values.astype(low)
        for h in range(heads):
            scores = scores_t(l, h)
            row_max = jnp.max(scores, axis=0, keepdims=True)
            exponent = jnp.exp(scores - row_max)
            row_total = jnp.sum(exponent, axis=0, keepdims=True)
            probabilities = (exponent / row_total).astype(low)
            logsum[l, h : h + 1, :] = row_max + jnp.log(row_total)
            mixed = nn(head(value_t, l, h // share), probabilities)
            mixed_t[l, h * HD : (h + 1) * HD, :] = mixed.astype(low).astype(full)
        mixed = jnp.transpose(mixed_t[l])
        mixed_out[l] = mixed
        left_low[:, : heads * HD] = mixed.astype(low)

    def attention_back(l):
        grad_mixed_t = jnp.transpose(nt(normed_low[...], v_output[l]).astype(low).astype(full))
        for g in range(kv_heads):
            grad_value = jnp.zeros((HD, length), full)
            grad_key = jnp.zeros((HD, length), full)
            for h in range(g * share, (g + 1) * share):
                grad_mixed = grad_mixed_t[h * HD : (h + 1) * HD]
                grad_mixed_low = grad_mixed.astype(low)
                again = jnp.exp(scores_t(l, h) - logsum[l, h : h + 1, :])
                grad_value += nt(grad_mixed_low, again.astype(low))
                grad_probs = tn(head(value_t, l, g), grad_mixed_low)
                row_dot = jnp.sum(grad_mixed * head(mixed_t, l, h), axis=0, keepdims=True)
                grad_scores = (again * (grad_probs - row_dot) * scale).astype(low)
                grad_query = nn(head(key_t, l, g), grad_scores)
                grad_key += nt(head(query_t, l, h), grad_scores)
                wide[h * HD : (h + 1) * HD, :] = turned(grad_query, -1.0).astype(low).astype(full)
            at = (heads + g) * HD
            wide[at : at + HD, :] = turned(grad_key, -1.0).astype(low).astype(full)
            at = (heads + kv_heads + g) * HD
            wide[at : at + HD, :] = grad_value.astype(low).astype(full)
        rows = jnp.transpose(wide[...])
        qkv_out[l] = rows
        left_low[:, : rows.shape[1]] = rows.astype(low)

    step = hidden_units // 2
    nothing = lambda: None

    def attention_layer(l, meanwhile):
        normalize(stream.at[2 * l], attn_gain, l, normed_low, normed_two_out.at[l])
        cut(slices_out, l, normed_two_out.at[l])
        send_slices("normed", l)
        attend(l)
        send_own("mixed", l)
        loads[l, 3].wait()
        tensor_sum(
            2 * l,
            lambda at: nn(left_low[:, : heads * HD], v_output[l, :, at]),
            stream.at[2 * l],
            stream.at[2 * l + 1],
            meanwhile,
        )

    def mlp_layer(l, meanwhile):
        normalize(stream.at[2 * l + 1], mlp_gain, l, normed_low, normed_two_out.at[l])
        send_own("normed_two", l)
        loads[l, 4].wait()
        loads[l, 5].wait()

        def units(i):
            at = columns(i * TILE, TILE)
            source = normed_low[...]
            gate = nn(source, v_gate[l, :, at])
            up = nn(source, v_up[l, :, at])
            gate_pre[l, :, at] = gate
            up_pre[l, :, at] = up
            left_low[:, at] = (gate * jax.nn.sigmoid(gate) * up).astype(low)

        each(hidden_units // TILE, units)
        loads[l, 6].wait()
        tensor_sum(
            2 * l + 1,
            lambda at: nn(left_low[...], v_down[l, :, at]),
            stream.at[2 * l + 1],
            stream.at[2 * l + 2],
            meanwhile,
        )

    def mlp_back(l, meanwhile):
        def units(i):
            at = columns(i * TILE, TILE)
            grad_act = nt(normed_low[...], v_down[l, at, :])
            left, right, _ = mlp_grads(gate_pre[l, :, at], up_pre[l, :, at], grad_act)
            left_low[:, at] = left
            right_low[:, at] = right

        each(hidden_units // TILE, units)
        j = 2 * LAYERS + 2 * (LAYERS - 1 - l)
        tensor_sum(
            j,
            lambda at: nt(left_low[...], v_gate[l, at, :]) + nt(right_low[...], v_up[l, at, :]),
            None,
            grads.at[j % 2],
            meanwhile,
        )
        norm_backward(
            grads.at[j % 2],
            stream.at[2 * l + 1],
            mlp_gain,
            l,
            LAYERS + l,
            upstream,
            upstream,
            normed_low,
            part_wide,
        )
        settle_slices("normed", LAYERS - 1 - l)
        cut(slices_out, LAYERS - 1 - l, part_wide)
        send_slices("grad_att", l)

    part_wide = grads.at[2]

    def attention_layer_back(l, meanwhile):
        attention_back(l)
        if l == 0:
            send_own("qkv", l)
        j = 2 * LAYERS + 2 * (LAYERS - 1 - l) + 1
        q_end, k_end = heads * HD, (heads + kv_heads) * HD
        v_end = (heads + 2 * kv_heads) * HD
        tensor_sum(
            j,
            lambda at: nt(left_low[:, :q_end], v_query[l, at, :])
            + nn(left_low[:, q_end:k_end], v_key[l, :, at])
            + nn(left_low[:, k_end:v_end], v_value[l, :, at]),
            None,
            grads.at[j % 2],
            meanwhile,
        )
        last = l == 0
        norm_backward(
            grads.at[j % 2],
            stream.at[2 * l],
            attn_gain,
            l,
            l,
            upstream,
            upstream,
            None if last else normed_low,
            None if last else g_out.at[l - 1],
        )

    window = cut_a.shape[0]
    start = jnp.minimum(dp * piece // 128 * 128, width - window)
    offset = pl.multiple_of(dp * piece - start, 8)

    def stream_tokens(count, copies, body):
        def go(i, slot):
            for c in copies(i, slot):
                c.start()

        go(0, 0)

        def step(i):
            slot = lax.rem(i, 2)
            for c in copies(i, slot):
                c.wait()

            @pl.when(i + 1 < count)
            def _():
                go(i + 1, 1 - slot)

            body(slot)

        each(count, step)

    def mlp_gradients(l):
        def copies(i, slot):
            rows = pl.ds(pl.multiple_of(i * TOKENS, 8), TOKENS)
            return (
                pltpu.make_async_copy(
                    normed_two_all.at[l, rows], token_a.at[slot], fetch.at[0, slot]
                ),
                pltpu.make_async_copy(g_all.at[l, rows], token_b.at[slot], fetch.at[1, slot]),
            )

        sum_g[...] = jnp.zeros_like(sum_g)
        sum_u[...] = jnp.zeros_like(sum_u)
        sum_d[...] = jnp.zeros_like(sum_d)

        def body(slot):
            low_a[...] = token_a[slot].astype(low)
            low_b[...] = token_b[slot].astype(low)
            cut_a[...] = jnp.transpose(token_a[slot, :, columns(start, window)]).astype(low)
            cut_b[...] = jnp.transpose(token_b[slot, :, columns(start, window)]).astype(low)

            def units(i):
                at = columns(i * TILE, TILE)
                gate = nn(low_a[...], v_gate[l, :, at])
                up = nn(low_a[...], v_up[l, :, at])
                grad_act = nt(low_b[...], v_down[l, at, :])
                left, right, activated = mlp_grads(gate, up, grad_act)
                sum_g[:, at] += nn(cut_a[...], left)
                sum_u[:, at] += nn(cut_a[...], right)
                sum_d[:, at] += nn(cut_b[...], activated)

            each(hidden_units // TILE, units)

        stream_tokens(n * length // TOKENS, copies, body)
        outs = [
            pltpu.make_async_copy(src.at[pl.ds(offset, piece)], dst.at[l], edge.at[4 + i])
            for i, (src, dst) in enumerate(((sum_g, grad_g), (sum_u, grad_u), (sum_d, grad_d)))
        ]
        for c in outs:
            c.start()
        for c in outs:
            c.wait()

    def attention_gradients(l):
        blocks = TOKENS // length

        def copies(i, slot):
            rows = pl.ds(pl.multiple_of(i * TOKENS, 8), TOKENS)
            several = pl.ds(i * blocks, blocks)
            return (
                pltpu.make_async_copy(qkv_all.at[l, rows], state_qkv.at[slot], fetch.at[2, slot]),
                pltpu.make_async_copy(
                    mixed_all.at[l, rows], state_mixed.at[slot], fetch.at[3, slot]
                ),
                pltpu.make_async_copy(
                    normed_all.at[l, several], state_a.at[slot], fetch.at[4, slot]
                ),
                pltpu.make_async_copy(
                    grad_att_all.at[l, several], state_b.at[slot], fetch.at[5, slot]
                ),
            )

        for ref in (sum_q, sum_k, sum_v, sum_o):
            ref[...] = jnp.zeros_like(ref)
        q_end, k_end = heads * HD, (heads + kv_heads) * HD

        def body(slot):
            for b in range(blocks):
                rows = slice(b * length, (b + 1) * length)
                normed = jnp.transpose(state_a[slot, b]).astype(low)
                grad_att = jnp.transpose(state_b[slot, b]).astype(low)
                qkv = state_qkv[slot, rows, :].astype(low)
                sum_q[...] += nn(normed, qkv[:, :q_end])
                sum_k[...] += nn(normed, qkv[:, q_end:k_end])
                sum_v[...] += nn(normed, qkv[:, k_end:])
                sum_o[...] += nn(grad_att, state_mixed[slot, rows, :].astype(low))

        stream_tokens(n * length // TOKENS, copies, body)
        outs = [
            pltpu.make_async_copy(src, dst.at[l], edge.at[7 + i])
            for i, (src, dst) in enumerate(
                ((sum_q, grad_q), (sum_k, grad_k), (sum_v, grad_v), (sum_o, grad_o))
            )
        ]
        for c in outs:
            c.start()
        for c in outs:
            c.wait()

    def steps(*calls):
        def run():
            for call, *what in calls:
                call(*what)

        return run

    for c in arriving:
        c.wait()
    g_out[LAYERS - 1] = upstream[...].astype(low).astype(full)
    send_own("g", LAYERS - 1)
    gain_rows[...] = jnp.zeros_like(gain_rows)

    attention_layer(0, nothing)
    mlp_layer(0, steps((pass_on, "g", 1), (take_slices, "normed", 0)))
    attention_layer(1, steps((pass_on, "mixed", 0), (take_across, "g", 1)))
    mlp_layer(1, steps((pass_on, "normed_two", 0), (take_across, "mixed", 0)))
    going = [pltpu.make_async_copy(stream.at[2 * LAYERS], hidden_out, edge.at[2])]
    going[0].start()
    normed_low[...] = g_out[LAYERS - 1].astype(low)
    mlp_back(1, steps((take_slices, "normed", 1), (take_across, "normed_two", 0)))
    attention_layer_back(1, steps((pass_on, "mixed", 1), (share_y, "normed_two", 0, 0, 3)))
    send_own("g", 0)
    send_own("qkv", 1)
    mlp_back(0, steps((take_across, "mixed", 1), (share_y, "normed_two", 0, 1, 3)))
    attention_layer_back(0, steps((pass_on, "normed_two", 1), (share_y, "normed_two", 0, 2, 3)))
    going.append(pltpu.make_async_copy(upstream, grad_input, edge.at[3]))
    going[1].start()
    cut(gains_out, 0, gain_rows)
    send_slices("gains", 0)
    for call, *what in (
        (take_slices, "grad_att", 1),
        (pass_on, "g", 0),
        (take_across, "normed_two", 1),
        (take_y, "normed_two", 0),
        (take_across, "g", 0),
        (share_y, "g", 0),
        (complete, "normed_two", 1),
        (complete, "g", 1),
        (pass_on, "qkv", 1),
        (mlp_gradients, 1),
        (take_y, "g", 0),
        (take_across, "qkv", 1),
        (complete, "normed_two", 0),
        (complete, "g", 0),
        (mlp_gradients, 0),
        (take_slices, "grad_att", 0),
        (pass_on, "qkv", 0),
        (complete, "qkv", 1),
        (complete, "mixed", 1),
        (complete, "normed", 1),
        (complete, "grad_att", 1),
        (attention_gradients, 1),
        (take_across, "qkv", 0),
        (take_slices, "gains", 0),
        (complete, "gains", 0),
        (complete, "qkv", 0),
        (complete, "mixed", 0),
        (complete, "normed", 0),
        (complete, "grad_att", 0),
        (attention_gradients, 0),
    ):
        call(*what)
    assert not missing
    for c in unsent:
        c.wait_send()
    for key in list(leaving):
        settle_slices(*key)
    for c in going:
        c.wait()


def layers(n, hidden_in, cotangent, cosine, sine, allowed, attn_gain, mlp_gain, weights):
    length, width = hidden_in.shape
    w_query, w_key, w_value, w_output, w_gate, w_up, w_down = weights
    q_width, kv_width, hidden_units = w_query.shape[2], w_key.shape[1], w_gate.shape[2]
    qkv_width = q_width + 2 * kv_width
    piece = width // n
    f32 = lambda *shape: jax.ShapeDtypeStruct(shape, full)
    out_shape = [
        f32(length, width),
        f32(length, width),
        f32(LAYERS, piece, q_width),
        f32(LAYERS, piece, kv_width),
        f32(LAYERS, piece, kv_width),
        f32(LAYERS, piece, q_width),
        f32(LAYERS, piece, hidden_units),
        f32(LAYERS, piece, hidden_units),
        f32(LAYERS, piece, hidden_units),
        f32(LAYERS, n * length, q_width),
        f32(LAYERS, n * length, qkv_width),
        f32(LAYERS, n * length, width),
        f32(LAYERS, n * length, width),
        f32(LAYERS, n, length, piece),
        f32(LAYERS, n, length, piece),
        f32(1, n, 8, piece),
    ]
    vmem = pl.BlockSpec(memory_space=pltpu.VMEM)
    anywhere = pl.BlockSpec(memory_space=pl.ANY)
    dma = pltpu.SemaphoreType.DMA
    keep = lambda dtype, *shape: pltpu.VMEM(shape, dtype)
    sums = 4 * LAYERS
    chunks = width // 2 // TILE
    window = pl.cdiv(piece + 128 - math.gcd(piece, 128), 128) * 128
    return pl.pallas_call(
        functools.partial(layers_kernel, n),
        out_shape=out_shape,
        in_specs=[anywhere] * 2 + [vmem] * 5 + [anywhere] * 7,
        out_specs=[anywhere] * 16,
        scratch_shapes=[keep(low, *w.shape) for w in weights]
        + [
            keep(full, 2 * LAYERS + 1, length, width),
            keep(full, 3, length, width),
            keep(full, length, width),
            keep(low, length, width),
            keep(low, length, hidden_units),
            keep(low, length, hidden_units),
            keep(full, LAYERS, length, hidden_units),
            keep(full, LAYERS, length, hidden_units),
            keep(low, LAYERS, q_width, length),
            keep(low, LAYERS, kv_width, length),
            keep(low, LAYERS, kv_width, length),
            keep(full, LAYERS, q_width, length),
            keep(full, LAYERS, 8, length),
            keep(full, LAYERS, length, q_width),
            keep(full, LAYERS, length, qkv_width),
            keep(full, LAYERS, length, width),
            keep(full, LAYERS, length, width),
            keep(full, LAYERS, n, length, piece),
            keep(full, 1, n, 8, piece),
            keep(full, 8, width),
            keep(full, qkv_width, length),
            keep(full, length, width // 2),
            keep(full, 2, length, width // 2),
            keep(full, length, width // 2),
            keep(full, 2, length, width // 2),
            keep(full, 2, TOKENS, width),
            keep(full, 2, TOKENS, width),
            keep(low, TOKENS, width),
            keep(low, TOKENS, width),
            keep(low, window, TOKENS),
            keep(low, window, TOKENS),
            keep(full, window, hidden_units),
            keep(full, window, hidden_units),
            keep(full, window, hidden_units),
            keep(full, 2, TOKENS, qkv_width),
            keep(full, 2, TOKENS, q_width),
            keep(full, 2, TOKENS // length, length, piece),
            keep(full, 2, TOKENS // length, length, piece),
            keep(full, piece, q_width),
            keep(full, piece, kv_width),
            keep(full, piece, kv_width),
            keep(full, piece, q_width),
            dma((LAYERS, 7)),
            dma((sums, 3, chunks)),
            dma((sums, 3, chunks)),
            dma((4 * LAYERS, n // 2)),
            dma((4 * LAYERS, n // 2)),
            dma((4 * LAYERS, n // 2)),
            dma((4 * LAYERS, n // 2)),
            dma((2 * LAYERS, n)),
            dma((2 * LAYERS, n)),
            dma((3 * LAYERS, n)),
            dma((3 * LAYERS, n)),
            dma((2 * LAYERS, n)),
            dma((2 * LAYERS, n)),
            dma((2 * LAYERS, n)),
            dma((2 * LAYERS, n)),
            dma((2 * LAYERS, n)),
            dma((2 * LAYERS, n)),
            dma((7 * LAYERS,)),
            dma((11,)),
            dma((6, 2)),
        ],
        compiler_params=pltpu.CompilerParams(
            collective_id=0, has_side_effects=True, vmem_limit_bytes=66_000_000
        ),
        name="layers",
    )(hidden_in, cotangent, cosine, sine, allowed, attn_gain, mlp_gain, *weights)


def shards(
    hidden_in,
    cotangent,
    segment_ids,
    positions,
    w_query,
    w_key,
    w_value,
    w_output,
    w_gate,
    w_up,
    w_down,
    attn_gain,
    mlp_gain,
):
    n = lax.axis_size("dp")
    length = hidden_in.shape[0]
    weights = (
        w_query,
        jnp.swapaxes(w_key, 1, 2),
        jnp.swapaxes(w_value, 1, 2),
        w_output,
        w_gate,
        w_up,
        w_down,
    )
    half_dim = HD // 2
    frequencies = rope_base ** (-(jnp.arange(half_dim).astype(jnp.float32) * 2.0 / HD))
    angles = frequencies[:, None] * positions[0].astype(jnp.float32)[None, :]
    segments = segment_ids[0]
    token_order = jnp.arange(length)
    allowed = (segments[:, None] == segments[None, :]) & (
        token_order[:, None] <= token_order[None, :]
    )
    outs = layers(
        n,
        hidden_in,
        cotangent,
        jnp.cos(angles),
        jnp.sin(angles),
        allowed.astype(jnp.float32),
        attn_gain,
        mlp_gain,
        weights,
    )
    hidden, grad_input, grad_q, grad_k, grad_v, grad_o, grad_g, grad_u, grad_d = outs[:9]
    gain_sums = jnp.sum(outs[-1][0], axis=0)
    return (
        hidden,
        grad_input,
        grad_q,
        grad_k,
        grad_v,
        jnp.swapaxes(grad_o, 1, 2),
        grad_g,
        grad_u,
        jnp.swapaxes(grad_d, 1, 2),
        gain_sums[:LAYERS],
        gain_sums[LAYERS : 2 * LAYERS],
    )


def solution(mesh):
    return jax.shard_map(
        shards,
        mesh=mesh,
        in_specs=(
            P("dp", None),
            P("dp", None),
            P("dp", None),
            P("dp", None),
            P(None, None, "tensor"),
            P(None, None, "tensor"),
            P(None, None, "tensor"),
            P(None, "tensor", None),
            P(None, None, "tensor"),
            P(None, None, "tensor"),
            P(None, "tensor", None),
            P(),
            P(),
        ),
        out_specs=(
            P("dp", None),
            P("dp", None),
            P(None, "dp", "tensor"),
            P(None, "dp", "tensor"),
            P(None, "dp", "tensor"),
            P(None, "tensor", "dp"),
            P(None, "dp", "tensor"),
            P(None, "dp", "tensor"),
            P(None, "tensor", "dp"),
            P(None, "dp"),
            P(None, "dp"),
        ),
        check_vma=False,
    )
```

```python
import functools
import math

import jax
import jax.numpy as jnp
from jax import lax
from jax.experimental import pallas as pl
from jax.experimental.pallas import tpu as pltpu
from jax.sharding import PartitionSpec as P

HD = 96
LAYERS = 2
TILE = 256
ROWS = 16
TOKENS = 256
SHARED_Y = (("g", 1), ("normed_two", 0), ("g", 0))
MESH = pl.DeviceIdType.MESH


epsilon = 1e-05
rope_base = 100000.0
masked_score = -1e30
low = jnp.bfloat16
full = jnp.float32


def nn(a, b):
    return lax.dot_general(a, b, (((1,), (0,)), ((), ())), preferred_element_type=full)


def nt(a, b):
    return lax.dot_general(a, b, (((1,), (1,)), ((), ())), preferred_element_type=full)


def tn(a, b):
    return lax.dot_general(a, b, (((0,), (0,)), ((), ())), preferred_element_type=full)


def mlp_grads(gate_pre, up_pre, grad_act):
    sigmoid_gate = jax.nn.sigmoid(gate_pre)
    grad_gate_low = (
        grad_act * up_pre * sigmoid_gate * (1.0 + gate_pre * (1.0 - sigmoid_gate))
    ).astype(low)
    grad_up_low = (grad_act * gate_pre * sigmoid_gate).astype(low)
    activated = (gate_pre * sigmoid_gate * up_pre).astype(low)
    return grad_gate_low, grad_up_low, activated


def each(count, body):
    def step(i, carry):
        body(i)
        return carry

    lax.fori_loop(0, count, step, 0)


def columns(start, size):
    return pl.ds(pl.multiple_of(start, 128), size)


def layers_kernel(n, *refs):
    (
        hidden_in,
        cotangent,
        cosine,
        sine,
        allowed,
        attn_gain,
        mlp_gain,
        w_query,
        w_key,
        w_value,
        w_output,
        w_gate,
        w_up,
        w_down,
        hidden_out,
        grad_input,
        grad_q,
        grad_k,
        grad_v,
        grad_o,
        grad_g,
        grad_u,
        grad_d,
        mixed_all,
        qkv_all,
        normed_two_all,
        g_all,
        normed_all,
        grad_att_all,
        gains_all,
        v_query,
        v_key,
        v_value,
        v_output,
        v_gate,
        v_up,
        v_down,
        stream,
        grads,
        upstream,
        normed_low,
        left_low,
        right_low,
        gate_pre,
        up_pre,
        query_t,
        key_t,
        value_t,
        mixed_t,
        logsum,
        mixed_out,
        qkv_out,
        normed_two_out,
        g_out,
        slices_out,
        gains_out,
        gain_rows,
        wide,
        part,
        from_core,
        half,
        from_y,
        token_a,
        token_b,
        low_a,
        low_b,
        cut_a,
        cut_b,
        sum_g,
        sum_u,
        sum_d,
        state_qkv,
        state_mixed,
        state_a,
        state_b,
        sum_q,
        sum_k,
        sum_v,
        sum_o,
        w_sem,
        sum_send,
        sum_recv,
        z_send,
        z_recv,
        x_send,
        x_recv,
        c_send,
        c_recv,
        a_send,
        a_recv,
        b_send,
        b_recv,
        y_send,
        y_recv,
        d_send,
        d_recv,
        e_send,
        e_recv,
        f_send,
        f_recv,
        local,
        edge,
        fetch,
    ) = refs
    length, width = hidden_in.shape
    heads = w_query.shape[2] // HD
    kv_heads = w_key.shape[1] // HD
    share = heads // kv_heads
    hidden_units = w_gate.shape[2]
    piece = width // n
    side_width = width // 2
    chunks = side_width // TILE
    turn = HD // 2
    scale = HD ** (-0.5)

    dp = lax.axis_index("dp")
    tensor = lax.axis_index("tensor")
    core = tensor % 2
    side = dp % 2
    group = dp // 2
    groups = n // 2
    core_peer = (dp, tensor + 1 - 2 * core)
    y_peer = (dp, lax.rem(tensor + 2, 4))
    x_peer = (dp + 1 - 2 * side, tensor)

    stored = (w_query, w_key, w_value, w_output, w_gate, w_up, w_down)
    held = (v_query, v_key, v_value, v_output, v_gate, v_up, v_down)
    loads = {}
    for l in range(LAYERS):
        for i, (src, dst) in enumerate(zip(stored, held)):
            loads[l, i] = pltpu.make_async_copy(src.at[l], dst.at[l], w_sem.at[l, i])
            loads[l, i].start()

    arriving = [
        pltpu.make_async_copy(hidden_in, stream.at[0], edge.at[0]),
        pltpu.make_async_copy(cotangent, upstream, edge.at[1]),
    ]
    for c in arriving:
        c.start()

    barrier = pltpu.get_barrier_semaphore()
    greeted = [core_peer, y_peer] + [(lax.rem(dp + k, n), tensor) for k in range(1, n)]
    for peer in greeted:
        pl.semaphore_signal(barrier, inc=1, device_id=peer, device_id_type=MESH)
    pl.semaphore_wait(barrier, len(greeted))

    def remote(src, dst, s, r, peer):
        return pltpu.make_async_remote_copy(
            src_ref=src, dst_ref=dst, send_sem=s, recv_sem=r, device_id=peer, device_id_type=MESH
        )

    unsent = []
    missing = {}
    leaving = {}

    ways = {}
    kinds = {
        "mixed": (0, mixed_out, mixed_all, False),
        "qkv": (1, qkv_out, qkv_all, False),
        "normed_two": (2, normed_two_out, normed_two_all, True),
        "g": (3, g_out, g_all, True),
    }

    quarter_width = width // 4

    def block(kind, l, index, owner=None):
        _, _, everywhere, shared = kinds[kind]
        rows = pl.ds(pl.multiple_of(index * length, 8), length)
        if (kind, l) in SHARED_Y:
            at = tensor if owner is None else owner
            return everywhere.at[l, rows, columns(at * quarter_width, quarter_width)]
        if shared:
            return everywhere.at[l, rows, columns(core * side_width, side_width)]
        return everywhere.at[l, rows]

    def send_own(kind, l):
        a, own, everywhere, shared = kinds[kind]
        slot = a * LAYERS + l
        if (kind, l) in SHARED_Y:
            mine = own.at[l, :, columns(tensor * quarter_width, quarter_width)]
        elif shared:
            mine = own.at[l, :, columns(core * side_width, side_width)]
        else:
            mine = own.at[l]
        for k in range(groups):
            if k == 0:
                c = remote(
                    mine, block(kind, l, dp), x_send.at[slot, 0], x_recv.at[slot, 0], x_peer
                )
            else:
                peer = (lax.rem(group + k, groups) * 2 + side, tensor)
                c = remote(
                    mine, block(kind, l, dp), z_send.at[slot, k], z_recv.at[slot, k], peer
                )
            c.start()
            ways[kind, l, "own", k] = c
            unsent.append(c)
        rows = pl.ds(pl.multiple_of(dp * length, 8), length)
        c = pltpu.make_async_copy(own.at[l], everywhere.at[l, rows], local.at[slot])
        c.start()
        missing.setdefault((kind, l), []).append(c.wait)

    def source_of(i):
        if i < groups - 1:
            return lax.rem(group + groups - 1 - i, groups) * 2 + side
        return lax.rem(group + 2 * groups - 1 - i, groups) * 2 + 1 - side

    def to_core(kind, l, i):
        a = kinds[kind][0]
        if kinds[kind][3]:
            slot = (a - 2) * LAYERS + l
            here = block(kind, l, source_of(i))
            c = remote(here, here, c_send.at[slot, i], c_recv.at[slot, i], core_peer)
            c.start()
            unsent.append(c)
            missing[kind, l].append(c.wait_recv)

    def pass_one(kind, l, k):
        slot = kinds[kind][0] * LAYERS + l
        ways[kind, l, "own", k].wait_recv()
        here = block(kind, l, source_of(k - 1))
        c = remote(here, here, x_send.at[slot, k], x_recv.at[slot, k], x_peer)
        c.start()
        ways[kind, l, "x", k] = c
        unsent.append(c)
        to_core(kind, l, k - 1)

    def pass_part(kind, l, part, parts):
        for k in range(1 + part * (groups - 1) // parts, 1 + (part + 1) * (groups - 1) // parts):
            pass_one(kind, l, k)

    def pass_on(kind, l):
        pass_part(kind, l, 0, 1)

    def take_one(kind, l, k):
        ways[kind, l, "own" if k == 0 else "x", k].wait_recv()
        to_core(kind, l, groups - 1 + k)

    def take_across(kind, l):
        for k in range(groups):
            take_one(kind, l, k)

    def share_one(kind, l, i):
        slot = (kinds[kind][0] - 2) * LAYERS + l
        here = block(kind, l, source_of(i))
        c = remote(here, here, y_send.at[slot, i], y_recv.at[slot, i], y_peer)
        c.start()
        ways[kind, l, "y", i] = c
        unsent.append(c)

    def share_y(kind, l, part=0, parts=1):
        if (kind, l) in SHARED_Y:
            for i in range(part * (n - 1) // parts, (part + 1) * (n - 1) // parts):
                share_one(kind, l, i)

    def take_y(kind, l):
        if (kind, l) in SHARED_Y:
            slot = (kinds[kind][0] - 2) * LAYERS + l
            for i in range(n - 1):
                ways[kind, l, "y", i].wait_recv()
                here = block(kind, l, source_of(i), lax.rem(tensor + 2, 4))
                c = remote(here, here, d_send.at[slot, i], d_recv.at[slot, i], core_peer)
                c.start()
                unsent.append(c)
                missing[kind, l].append(c.wait_recv)

    def complete(kind, l):
        for wait in missing.pop((kind, l)):
            wait()
        if (kind, l) in leaving:
            settle_slices(kind, l)

    slices = {
        "normed": (0, slices_out, normed_all, True),
        "grad_att": (1, slices_out, grad_att_all, True),
        "gains": (2, gains_out, gains_all, False),
    }

    slice_parts = 4 if piece % 32 == 0 else 2
    slice_rows = piece // slice_parts
    slice_mine = tensor if slice_parts == 4 else core

    def sliced(kind, l, index, owner=None):
        everywhere = slices[kind][2]
        if slices[kind][3]:
            at = slice_mine if owner is None else owner
            rows = pl.ds(pl.multiple_of(at * slice_rows, 8), slice_rows)
            return everywhere.at[l, index, rows]
        return everywhere.at[l, index]

    def sliced_own(kind, slot, index, whole=False):
        own = slices[kind][1]
        if not slices[kind][3]:
            return own.at[slot, index]
        if whole:
            return own.at[slot, pl.ds(pl.multiple_of(index * piece, 8), piece)]
        first = pl.multiple_of(index * piece + slice_mine * slice_rows, 8)
        return own.at[slot, pl.ds(first, slice_rows)]

    def send_slices(kind, l):
        b, own, everywhere, halves = slices[kind]
        slot = b * LAYERS + l
        held_at = LAYERS - 1 - l if kind == "grad_att" else l
        sent = []
        for k in range(1, n):
            to = lax.rem(dp + k, n)
            c = remote(
                sliced_own(kind, held_at, to),
                sliced(kind, l, dp),
                a_send.at[slot, k],
                a_recv.at[slot, k],
                (to, tensor),
            )
            c.start()
            ways[kind, l, k] = c
            sent.append(c.wait_send)
        c = pltpu.make_async_copy(
            sliced_own(kind, held_at, dp, True), everywhere.at[l, dp], local.at[4 * LAYERS + slot]
        )
        c.start()
        missing[kind, l] = []
        leaving[kind, l] = sent + [c.wait]

    def settle_slices(kind, l):
        for wait in leaving.pop((kind, l)):
            wait()

    def take_slices(kind, l):
        b, _, everywhere, divided = slices[kind]
        slot = b * LAYERS + l
        for k in range(1, n):
            ways[kind, l, k].wait_recv()
            if divided:
                here = sliced(kind, l, lax.rem(dp + n - k, n))
                c = remote(here, here, b_send.at[slot, k], b_recv.at[slot, k], core_peer)
                c.start()
                unsent.append(c)
                missing[kind, l].append(c.wait_recv)
                if slice_parts == 4:
                    c = remote(here, here, e_send.at[slot, k], e_recv.at[slot, k], y_peer)
                    c.start()
                    unsent.append(c)
                    ways[kind, l, "y", k] = c

    def take_slices_y(kind, l):
        slot = slices[kind][0] * LAYERS + l
        if slice_parts == 4:
            for k in range(1, n):
                ways[kind, l, "y", k].wait_recv()
                here = sliced(kind, l, lax.rem(dp + n - k, n), lax.rem(tensor + 2, 4))
                c = remote(here, here, f_send.at[slot, k], f_recv.at[slot, k], core_peer)
                c.start()
                unsent.append(c)
                missing[kind, l].append(c.wait_recv)

    def turn_over(dst, src):
        for t in range(width // 128):
            at = slice(t * 128, (t + 1) * 128)
            dst[at, :] = jnp.transpose(src[:, at])

    def cut(dst, l, src):
        for t in range(n):
            dst[l, t] = src[:, t * piece : (t + 1) * piece]

    def tensor_sum(j, tile, base, dest, meanwhile):
        def copy(stage, k, src, dst, peer):
            return remote(src, dst, sum_send.at[j, stage, k], sum_recv.at[j, stage, k], peer)

        def at(k):
            return pl.ds(pl.multiple_of(k * TILE, 128), TILE)

        def mine(k):
            return columns(core * side_width + k * TILE, TILE)

        def other(k):
            return columns((1 - core) * side_width + k * TILE, TILE)

        def first(k):
            return copy(0, k, part.at[:, at(k)], from_core.at[j % 2, :, at(k)], core_peer)

        def second(k):
            return copy(1, k, half.at[:, at(k)], from_y.at[j % 2, :, at(k)], y_peer)

        def third(k):
            return copy(2, k, dest.at[:, mine(k)], dest.at[:, mine(k)], core_peer)

        def begin(k):
            part[:, at(k)] = tile(other(k))
            first(k).start()

        def middle(k):
            own = tile(mine(k))
            first(k).wait_recv()
            half[:, at(k)] = own + from_core[j % 2, :, at(k)]
            second(k).start()

        def finish(k):
            second(k).wait_recv()
            total = half[:, at(k)] + from_y[j % 2, :, at(k)]
            if base is not None:
                total = base[:, mine(k)] + total
            dest[:, mine(k)] = total
            third(k).start()

        def settle(k):
            third(k).wait_recv()
            first(k).wait_send()
            second(k).wait_send()
            third(k).wait_send()

        each(chunks, begin)
        each(chunks, middle)
        meanwhile()
        each(chunks, finish)
        each(chunks, settle)

    def inverse_rms(values):
        return lax.rsqrt(jnp.mean(values * values, axis=-1, keepdims=True) + epsilon)

    def normalize(src, gain, l, out, out_wide):
        def rows_of(i):
            rows = pl.ds(pl.multiple_of(i * ROWS, ROWS), ROWS)
            values = src[rows, :]
            normed = (values * inverse_rms(values) * gain[l : l + 1, :]).astype(low)
            out[rows, :] = normed
            out_wide[rows, :] = normed.astype(full)

        each(length // ROWS, rows_of)

    def norm_backward(grad, values_ref, gain, l, row, before, out, out_low, out_wide):
        def rows_of(i, total):
            rows = pl.ds(pl.multiple_of(i * ROWS, ROWS), ROWS)
            values = values_ref[rows, :]
            grad_normed = grad[rows, :]
            inverse = inverse_rms(values)
            normalized = values * inverse
            term = grad_normed * normalized
            total = total + term[:8] + term[8:]
            scaled = grad_normed * gain[l : l + 1, :]
            back = inverse * (
                scaled - normalized * jnp.mean(scaled * normalized, axis=-1, keepdims=True)
            )
            after = before[rows, :] + back
            out[rows, :] = after
            if out_low is not None:
                after_low = after.astype(low)
                out_low[rows, :] = after_low
                out_wide[rows, :] = after_low.astype(full)
            return total

        total = lax.fori_loop(0, length // ROWS, rows_of, jnp.zeros((8, width), full))
        gain_rows[row : row + 1, :] = jnp.sum(total, axis=0, keepdims=True)

    def turned(values, direction):
        u, w = values[:turn], values[turn:]
        c, s = cosine[...], sine[...]
        return jnp.concatenate([u * c - direction * w * s, w * c + direction * u * s], axis=0)

    def head(ref, l, h):
        return ref[l, h * HD : (h + 1) * HD, :]

    def scores_t(l, h):
        raw = tn(head(key_t, l, h // share), head(query_t, l, h)) * scale
        return jnp.where(allowed[...] > 0.5, raw, masked_score)

    def attend(l):
        for i in range(3):
            loads[l, i].wait()
        source = normed_low[...]
        for ref, dst, count, rope in (
            (v_query, query_t, heads, True),
            (v_key, key_t, kv_heads, True),
            (v_value, value_t, kv_heads, False),
        ):
            projected = jnp.transpose(nn(source, ref[l])) if ref is v_query else nt(ref[l], source)
            for h in range(count):
                values = projected[h * HD : (h + 1) * HD]
                values = turned(values, 1.0) if rope else values
                dst[l, h * HD : (h + 1) * HD, :] = values.astype(low)
        for h in range(heads):
            scores = scores_t(l, h)
            row_max = jnp.max(scores, axis=0, keepdims=True)
            exponent = jnp.exp(scores - row_max)
            row_total = jnp.sum(exponent, axis=0, keepdims=True)
            probabilities = (exponent / row_total).astype(low)
            logsum[l, h : h + 1, :] = row_max + jnp.log(row_total)
            mixed = nn(head(value_t, l, h // share), probabilities)
            mixed_t[l, h * HD : (h + 1) * HD, :] = mixed.astype(low).astype(full)
        mixed = jnp.transpose(mixed_t[l])
        mixed_out[l] = mixed
        left_low[:, : heads * HD] = mixed.astype(low)

    def attention_back(l):
        grad_mixed_t = jnp.transpose(nt(normed_low[...], v_output[l]).astype(low).astype(full))
        for g in range(kv_heads):
            grad_value = jnp.zeros((HD, length), full)
            grad_key = jnp.zeros((HD, length), full)
            for h in range(g * share, (g + 1) * share):
                grad_mixed = grad_mixed_t[h * HD : (h + 1) * HD]
                grad_mixed_low = grad_mixed.astype(low)
                again = jnp.exp(scores_t(l, h) - logsum[l, h : h + 1, :])
                grad_value += nt(grad_mixed_low, again.astype(low))
                grad_probs = tn(head(value_t, l, g), grad_mixed_low)
                row_dot = jnp.sum(grad_mixed * head(mixed_t, l, h), axis=0, keepdims=True)
                grad_scores = (again * (grad_probs - row_dot) * scale).astype(low)
                grad_query = nn(head(key_t, l, g), grad_scores)
                grad_key += nt(head(query_t, l, h), grad_scores)
                wide[h * HD : (h + 1) * HD, :] = turned(grad_query, -1.0).astype(low).astype(full)
            at = (heads + g) * HD
            wide[at : at + HD, :] = turned(grad_key, -1.0).astype(low).astype(full)
            at = (heads + kv_heads + g) * HD
            wide[at : at + HD, :] = grad_value.astype(low).astype(full)
        rows = jnp.transpose(wide[...])
        qkv_out[l] = rows
        left_low[:, : rows.shape[1]] = rows.astype(low)

    step = hidden_units // 2
    nothing = lambda: None

    def attention_layer(l, meanwhile):
        normalize(stream.at[2 * l], attn_gain, l, normed_low, normed_two_out.at[l])
        turn_over(slices_out.at[l], normed_two_out.at[l])
        send_slices("normed", l)
        attend(l)
        send_own("mixed", l)
        loads[l, 3].wait()
        tensor_sum(
            2 * l,
            lambda at: nn(left_low[:, : heads * HD], v_output[l, :, at]),
            stream.at[2 * l],
            stream.at[2 * l + 1],
            meanwhile,
        )

    def mlp_layer(l, meanwhile):
        normalize(stream.at[2 * l + 1], mlp_gain, l, normed_low, normed_two_out.at[l])
        send_own("normed_two", l)
        loads[l, 4].wait()
        loads[l, 5].wait()

        def units(i):
            at = columns(i * TILE, TILE)
            source = normed_low[...]
            gate = nn(source, v_gate[l, :, at])
            up = nn(source, v_up[l, :, at])
            gate_pre[l, :, at] = gate
            up_pre[l, :, at] = up
            left_low[:, at] = (gate * jax.nn.sigmoid(gate) * up).astype(low)

        each(hidden_units // TILE, units)
        loads[l, 6].wait()
        tensor_sum(
            2 * l + 1,
            lambda at: nn(left_low[...], v_down[l, :, at]),
            stream.at[2 * l + 1],
            stream.at[2 * l + 2],
            meanwhile,
        )

    def mlp_back(l, meanwhile):
        def units(i):
            at = columns(i * TILE, TILE)
            grad_act = nt(normed_low[...], v_down[l, at, :])
            left, right, _ = mlp_grads(gate_pre[l, :, at], up_pre[l, :, at], grad_act)
            left_low[:, at] = left
            right_low[:, at] = right

        each(hidden_units // TILE, units)
        j = 2 * LAYERS + 2 * (LAYERS - 1 - l)
        tensor_sum(
            j,
            lambda at: nt(left_low[...], v_gate[l, at, :]) + nt(right_low[...], v_up[l, at, :]),
            None,
            grads.at[j % 2],
            meanwhile,
        )
        norm_backward(
            grads.at[j % 2],
            stream.at[2 * l + 1],
            mlp_gain,
            l,
            LAYERS + l,
            upstream,
            upstream,
            normed_low,
            part_wide,
        )
        settle_slices("normed", LAYERS - 1 - l)
        turn_over(slices_out.at[LAYERS - 1 - l], part_wide)
        send_slices("grad_att", l)

    part_wide = grads.at[2]

    def attention_layer_back(l, meanwhile):
        attention_back(l)
        if l == 0:
            send_own("qkv", l)
        j = 2 * LAYERS + 2 * (LAYERS - 1 - l) + 1
        q_end, k_end = heads * HD, (heads + kv_heads) * HD
        v_end = (heads + 2 * kv_heads) * HD
        tensor_sum(
            j,
            lambda at: nt(left_low[:, :q_end], v_query[l, at, :])
            + nn(left_low[:, q_end:k_end], v_key[l, :, at])
            + nn(left_low[:, k_end:v_end], v_value[l, :, at]),
            None,
            grads.at[j % 2],
            meanwhile,
        )
        last = l == 0
        norm_backward(
            grads.at[j % 2],
            stream.at[2 * l],
            attn_gain,
            l,
            l,
            upstream,
            upstream,
            None if last else normed_low,
            None if last else g_out.at[l - 1],
        )

    window = cut_a.shape[0]
    start = jnp.minimum(dp * piece // 128 * 128, width - window)
    offset = pl.multiple_of(dp * piece - start, 8)

    def stream_tokens(first, count, copies, body):
        def go(i, slot):
            for c in copies(i, slot):
                c.start()

        go(first, 0)

        def step(i):
            slot = lax.rem(i, 2)
            for c in copies(first + i, slot):
                c.wait()

            @pl.when(i + 1 < count)
            def _():
                go(first + i + 1, 1 - slot)

            body(slot)

        each(count, step)

    def mlp_gradients(l, share=0, shares=1):
        def copies(i, slot):
            rows = pl.ds(pl.multiple_of(i * TOKENS, 8), TOKENS)
            return (
                pltpu.make_async_copy(
                    normed_two_all.at[l, rows], token_a.at[slot], fetch.at[0, slot]
                ),
                pltpu.make_async_copy(g_all.at[l, rows], token_b.at[slot], fetch.at[1, slot]),
            )

        if share == 0:
            sum_g[...] = jnp.zeros_like(sum_g)
            sum_u[...] = jnp.zeros_like(sum_u)
            sum_d[...] = jnp.zeros_like(sum_d)

        def body(slot):
            low_a[...] = token_a[slot].astype(low)
            low_b[...] = token_b[slot].astype(low)
            cut_a[...] = jnp.transpose(token_a[slot, :, columns(start, window)]).astype(low)
            cut_b[...] = jnp.transpose(token_b[slot, :, columns(start, window)]).astype(low)

            def units(i):
                at = columns(i * TILE, TILE)
                gate = nn(low_a[...], v_gate[l, :, at])
                up = nn(low_a[...], v_up[l, :, at])
                grad_act = nt(low_b[...], v_down[l, at, :])
                left, right, activated = mlp_grads(gate, up, grad_act)
                sum_g[:, at] += nn(cut_a[...], left)
                sum_u[:, at] += nn(cut_a[...], right)
                sum_d[:, at] += nn(cut_b[...], activated)

            each(hidden_units // TILE, units)

        count = n * length // TOKENS // shares
        stream_tokens(share * count, count, copies, body)
        if share < shares - 1:
            return
        outs = [
            pltpu.make_async_copy(src.at[pl.ds(offset, piece)], dst.at[l], edge.at[4 + i])
            for i, (src, dst) in enumerate(((sum_g, grad_g), (sum_u, grad_u), (sum_d, grad_d)))
        ]
        for c in outs:
            c.start()
        for c in outs:
            c.wait()

    def attention_gradients(l):
        blocks = TOKENS // length

        def copies(i, slot):
            rows = pl.ds(pl.multiple_of(i * TOKENS, 8), TOKENS)
            several = pl.ds(i * blocks, blocks)
            return (
                pltpu.make_async_copy(qkv_all.at[l, rows], state_qkv.at[slot], fetch.at[2, slot]),
                pltpu.make_async_copy(
                    mixed_all.at[l, rows], state_mixed.at[slot], fetch.at[3, slot]
                ),
                pltpu.make_async_copy(
                    normed_all.at[l, several], state_a.at[slot], fetch.at[4, slot]
                ),
                pltpu.make_async_copy(
                    grad_att_all.at[l, several], state_b.at[slot], fetch.at[5, slot]
                ),
            )

        for ref in (sum_q, sum_k, sum_v, sum_o):
            ref[...] = jnp.zeros_like(ref)
        q_end, k_end = heads * HD, (heads + kv_heads) * HD

        def body(slot):
            for b in range(blocks):
                rows = slice(b * length, (b + 1) * length)
                normed = state_a[slot, b].astype(low)
                grad_att = state_b[slot, b].astype(low)
                qkv = state_qkv[slot, rows, :].astype(low)
                sum_q[...] += nn(normed, qkv[:, :q_end])
                sum_k[...] += nn(normed, qkv[:, q_end:k_end])
                sum_v[...] += nn(normed, qkv[:, k_end:])
                sum_o[...] += nn(grad_att, state_mixed[slot, rows, :].astype(low))

        stream_tokens(0, n * length // TOKENS, copies, body)
        outs = [
            pltpu.make_async_copy(src, dst.at[l], edge.at[7 + i])
            for i, (src, dst) in enumerate(
                ((sum_q, grad_q), (sum_k, grad_k), (sum_v, grad_v), (sum_o, grad_o))
            )
        ]
        for c in outs:
            c.start()
        for c in outs:
            c.wait()

    def steps(*calls):
        def run():
            for call, *what in calls:
                call(*what)

        return run

    for c in arriving:
        c.wait()
    g_out[LAYERS - 1] = upstream[...].astype(low).astype(full)
    send_own("g", LAYERS - 1)
    gain_rows[...] = jnp.zeros_like(gain_rows)

    attention_layer(0, nothing)
    mlp_layer(0, steps((pass_on, "g", 1), (take_slices, "normed", 0)))
    attention_layer(
        1,
        steps((pass_on, "mixed", 0), (take_across, "g", 1), (share_y, "g", 1, 0, 3)),
    )
    mlp_layer(
        1,
        steps((pass_on, "normed_two", 0), (take_across, "mixed", 0), (share_y, "g", 1, 1, 3)),
    )
    going = [pltpu.make_async_copy(stream.at[2 * LAYERS], hidden_out, edge.at[2])]
    going[0].start()
    normed_low[...] = g_out[LAYERS - 1].astype(low)
    mlp_back(
        1,
        steps(
            (take_slices, "normed", 1),
            (take_across, "normed_two", 0),
            (pass_on, "mixed", 1),
            (share_y, "g", 1, 2, 3),
        ),
    )
    attention_layer_back(1, steps((take_across, "mixed", 1), (share_y, "normed_two", 0, 0, 3)))
    send_own("g", 0)
    send_own("qkv", 1)
    mlp_back(0, steps((pass_on, "normed_two", 1), (share_y, "normed_two", 0, 1, 3)))
    attention_layer_back(
        0,
        steps(
            (take_slices, "grad_att", 1),
            (pass_on, "g", 0),
            (take_across, "normed_two", 1),
            (share_y, "normed_two", 0, 2, 3),
        ),
    )
    going.append(pltpu.make_async_copy(upstream, grad_input, edge.at[3]))
    going[1].start()
    cut(gains_out, 0, gain_rows)
    send_slices("gains", 0)
    for call, *what in (
        (take_across, "g", 0),
        (share_y, "g", 0),
        (take_slices, "grad_att", 0),
        (take_y, "g", 1),
        (take_slices_y, "normed", 0),
        (take_slices_y, "normed", 1),
        (take_slices_y, "grad_att", 1),
        (take_y, "normed_two", 0),
        (complete, "normed_two", 1),
        (complete, "g", 1),
        (mlp_gradients, 1, 0, 2),
        (pass_on, "qkv", 1),
        (mlp_gradients, 1, 1, 2),
        (take_y, "g", 0),
        (take_across, "qkv", 1),
        (complete, "normed_two", 0),
        (complete, "g", 0),
        (mlp_gradients, 0, 0, 4),
        (pass_part, "qkv", 0, 0, 3),
        (mlp_gradients, 0, 1, 4),
        (pass_part, "qkv", 0, 1, 3),
        (mlp_gradients, 0, 2, 4),
        (pass_part, "qkv", 0, 2, 3),
        (mlp_gradients, 0, 3, 4),
        (complete, "qkv", 1),
        (complete, "mixed", 1),
        (complete, "normed", 1),
        (complete, "grad_att", 1),
        (attention_gradients, 1),
        (take_across, "qkv", 0),
        (take_slices_y, "grad_att", 0),
        (take_slices, "gains", 0),
        (complete, "gains", 0),
        (complete, "qkv", 0),
        (complete, "mixed", 0),
        (complete, "normed", 0),
        (complete, "grad_att", 0),
        (attention_gradients, 0),
    ):
        call(*what)
    assert not missing
    for c in unsent:
        c.wait_send()
    for key in list(leaving):
        settle_slices(*key)
    for c in going:
        c.wait()


def layers(n, hidden_in, cotangent, cosine, sine, allowed, attn_gain, mlp_gain, weights):
    length, width = hidden_in.shape
    w_query, w_key, w_value, w_output, w_gate, w_up, w_down = weights
    q_width, kv_width, hidden_units = w_query.shape[2], w_key.shape[1], w_gate.shape[2]
    qkv_width = q_width + 2 * kv_width
    piece = width // n
    f32 = lambda *shape: jax.ShapeDtypeStruct(shape, full)
    out_shape = [
        f32(length, width),
        f32(length, width),
        f32(LAYERS, piece, q_width),
        f32(LAYERS, piece, kv_width),
        f32(LAYERS, piece, kv_width),
        f32(LAYERS, piece, q_width),
        f32(LAYERS, piece, hidden_units),
        f32(LAYERS, piece, hidden_units),
        f32(LAYERS, piece, hidden_units),
        f32(LAYERS, n * length, q_width),
        f32(LAYERS, n * length, qkv_width),
        f32(LAYERS, n * length, width),
        f32(LAYERS, n * length, width),
        f32(LAYERS, n, piece, length),
        f32(LAYERS, n, piece, length),
        f32(1, n, 8, piece),
    ]
    vmem = pl.BlockSpec(memory_space=pltpu.VMEM)
    anywhere = pl.BlockSpec(memory_space=pl.ANY)
    dma = pltpu.SemaphoreType.DMA
    keep = lambda dtype, *shape: pltpu.VMEM(shape, dtype)
    sums = 4 * LAYERS
    chunks = width // 2 // TILE
    window = pl.cdiv(piece + 128 - math.gcd(piece, 128), 128) * 128
    return pl.pallas_call(
        functools.partial(layers_kernel, n),
        out_shape=out_shape,
        in_specs=[anywhere] * 2 + [vmem] * 5 + [anywhere] * 7,
        out_specs=[anywhere] * 16,
        scratch_shapes=[keep(low, *w.shape) for w in weights]
        + [
            keep(full, 2 * LAYERS + 1, length, width),
            keep(full, 3, length, width),
            keep(full, length, width),
            keep(low, length, width),
            keep(low, length, hidden_units),
            keep(low, length, hidden_units),
            keep(full, LAYERS, length, hidden_units),
            keep(full, LAYERS, length, hidden_units),
            keep(low, LAYERS, q_width, length),
            keep(low, LAYERS, kv_width, length),
            keep(low, LAYERS, kv_width, length),
            keep(full, LAYERS, q_width, length),
            keep(full, LAYERS, 8, length),
            keep(full, LAYERS, length, q_width),
            keep(full, LAYERS, length, qkv_width),
            keep(full, LAYERS, length, width),
            keep(full, LAYERS, length, width),
            keep(full, LAYERS, width, length),
            keep(full, 1, n, 8, piece),
            keep(full, 8, width),
            keep(full, qkv_width, length),
            keep(full, length, width // 2),
            keep(full, 2, length, width // 2),
            keep(full, length, width // 2),
            keep(full, 2, length, width // 2),
            keep(full, 2, TOKENS, width),
            keep(full, 2, TOKENS, width),
            keep(low, TOKENS, width),
            keep(low, TOKENS, width),
            keep(low, window, TOKENS),
            keep(low, window, TOKENS),
            keep(full, window, hidden_units),
            keep(full, window, hidden_units),
            keep(full, window, hidden_units),
            keep(full, 2, TOKENS, qkv_width),
            keep(full, 2, TOKENS, q_width),
            keep(full, 2, TOKENS // length, piece, length),
            keep(full, 2, TOKENS // length, piece, length),
            keep(full, piece, q_width),
            keep(full, piece, kv_width),
            keep(full, piece, kv_width),
            keep(full, piece, q_width),
            dma((LAYERS, 7)),
            dma((sums, 3, chunks)),
            dma((sums, 3, chunks)),
            dma((4 * LAYERS, n // 2)),
            dma((4 * LAYERS, n // 2)),
            dma((4 * LAYERS, n // 2)),
            dma((4 * LAYERS, n // 2)),
            dma((2 * LAYERS, n)),
            dma((2 * LAYERS, n)),
            dma((3 * LAYERS, n)),
            dma((3 * LAYERS, n)),
            dma((2 * LAYERS, n)),
            dma((2 * LAYERS, n)),
            dma((2 * LAYERS, n)),
            dma((2 * LAYERS, n)),
            dma((2 * LAYERS, n)),
            dma((2 * LAYERS, n)),
            dma((2 * LAYERS, n)),
            dma((2 * LAYERS, n)),
            dma((2 * LAYERS, n)),
            dma((2 * LAYERS, n)),
            dma((7 * LAYERS,)),
            dma((11,)),
            dma((6, 2)),
        ],
        compiler_params=pltpu.CompilerParams(
            collective_id=0, has_side_effects=True, vmem_limit_bytes=66_000_000
        ),
        name="layers",
    )(hidden_in, cotangent, cosine, sine, allowed, attn_gain, mlp_gain, *weights)


def shards(
    hidden_in,
    cotangent,
    segment_ids,
    positions,
    w_query,
    w_key,
    w_value,
    w_output,
    w_gate,
    w_up,
    w_down,
    attn_gain,
    mlp_gain,
):
    n = lax.axis_size("dp")
    length = hidden_in.shape[0]
    weights = (
        w_query,
        jnp.swapaxes(w_key, 1, 2),
        jnp.swapaxes(w_value, 1, 2),
        w_output,
        w_gate,
        w_up,
        w_down,
    )
    half_dim = HD // 2
    frequencies = rope_base ** (-(jnp.arange(half_dim).astype(jnp.float32) * 2.0 / HD))
    angles = frequencies[:, None] * positions[0].astype(jnp.float32)[None, :]
    segments = segment_ids[0]
    token_order = jnp.arange(length)
    allowed = (segments[:, None] == segments[None, :]) & (
        token_order[:, None] <= token_order[None, :]
    )
    outs = layers(
        n,
        hidden_in,
        cotangent,
        jnp.cos(angles),
        jnp.sin(angles),
        allowed.astype(jnp.float32),
        attn_gain,
        mlp_gain,
        weights,
    )
    hidden, grad_input, grad_q, grad_k, grad_v, grad_o, grad_g, grad_u, grad_d = outs[:9]
    gain_sums = jnp.sum(outs[-1][0], axis=0)
    return (
        hidden,
        grad_input,
        grad_q,
        grad_k,
        grad_v,
        jnp.swapaxes(grad_o, 1, 2),
        grad_g,
        grad_u,
        jnp.swapaxes(grad_d, 1, 2),
        gain_sums[:LAYERS],
        gain_sums[LAYERS : 2 * LAYERS],
    )


def solution(mesh):
    return jax.shard_map(
        shards,
        mesh=mesh,
        in_specs=(
            P("dp", None),
            P("dp", None),
            P("dp", None),
            P("dp", None),
            P(None, None, "tensor"),
            P(None, None, "tensor"),
            P(None, None, "tensor"),
            P(None, "tensor", None),
            P(None, None, "tensor"),
            P(None, None, "tensor"),
            P(None, "tensor", None),
            P(),
            P(),
        ),
        out_specs=(
            P("dp", None),
            P("dp", None),
            P(None, "dp", "tensor"),
            P(None, "dp", "tensor"),
            P(None, "dp", "tensor"),
            P(None, "tensor", "dp"),
            P(None, "dp", "tensor"),
            P(None, "dp", "tensor"),
            P(None, "tensor", "dp"),
            P(None, "dp"),
            P(None, "dp"),
        ),
        check_vma=False,
    )
```

```python
import functools
import math

import jax
import jax.numpy as jnp
from jax import lax
from jax.experimental import pallas as pl
from jax.experimental.pallas import tpu as pltpu
from jax.sharding import PartitionSpec as P

HD = 96
LAYERS = 2
TILE = 256
UNITS = 512
ROWS = 16
TOKENS = 256
SHARED_Y = (("g", 1), ("normed_two", 0), ("g", 0))
MESH = pl.DeviceIdType.MESH


epsilon = 1e-05
rope_base = 100000.0
masked_score = -1e30
low = jnp.bfloat16
full = jnp.float32


def nn(a, b):
    return lax.dot_general(a, b, (((1,), (0,)), ((), ())), preferred_element_type=full)


def nt(a, b):
    return lax.dot_general(a, b, (((1,), (1,)), ((), ())), preferred_element_type=full)


def tn(a, b):
    return lax.dot_general(a, b, (((0,), (0,)), ((), ())), preferred_element_type=full)


def mlp_grads(gate_pre, up_pre, grad_act):
    sigmoid_gate = jax.nn.sigmoid(gate_pre)
    grad_gate_low = (
        grad_act * up_pre * sigmoid_gate * (1.0 + gate_pre * (1.0 - sigmoid_gate))
    ).astype(low)
    grad_up_low = (grad_act * gate_pre * sigmoid_gate).astype(low)
    activated = (gate_pre * sigmoid_gate * up_pre).astype(low)
    return grad_gate_low, grad_up_low, activated


def each(count, body):
    def step(i, carry):
        body(i)
        return carry

    lax.fori_loop(0, count, step, 0)


def columns(start, size):
    return pl.ds(pl.multiple_of(start, 128), size)


def layers_kernel(n, *refs):
    (
        hidden_in,
        cotangent,
        cosine,
        sine,
        allowed,
        attn_gain,
        mlp_gain,
        w_query,
        w_key,
        w_value,
        w_output,
        w_gate,
        w_up,
        w_down,
        hidden_out,
        grad_input,
        grad_q,
        grad_k,
        grad_v,
        grad_o,
        grad_g,
        grad_u,
        grad_d,
        mixed_all,
        query_all,
        keyval_all,
        normed_two_all,
        g_all,
        normed_all,
        grad_att_all,
        gains_all,
        v_query,
        v_key,
        v_value,
        v_output,
        v_gate,
        v_up,
        v_down,
        stream,
        grads,
        upstream,
        normed_low,
        left_low,
        right_low,
        gate_pre,
        up_pre,
        query_t,
        key_t,
        value_t,
        mixed_t,
        logsum,
        mixed_out,
        qkv_out,
        normed_two_out,
        g_out,
        slices_out,
        gains_out,
        gain_rows,
        wide,
        part,
        from_core,
        half,
        from_y,
        token_a,
        token_b,
        low_a,
        low_b,
        cut_a,
        cut_b,
        sum_g,
        sum_u,
        sum_d,
        state_qkv,
        state_mixed,
        state_a,
        state_b,
        sum_q,
        sum_k,
        sum_v,
        sum_o,
        w_sem,
        sum_send,
        sum_recv,
        z_send,
        z_recv,
        x_send,
        x_recv,
        c_send,
        c_recv,
        a_send,
        a_recv,
        b_send,
        b_recv,
        y_send,
        y_recv,
        d_send,
        d_recv,
        e_send,
        e_recv,
        f_send,
        f_recv,
        local,
        edge,
        fetch,
    ) = refs
    length, width = hidden_in.shape
    heads = w_query.shape[2] // HD
    kv_heads = w_key.shape[1] // HD
    share = heads // kv_heads
    hidden_units = w_gate.shape[2]
    piece = width // n
    side_width = width // 2
    chunks = side_width // TILE
    turn = HD // 2
    scale = HD ** (-0.5)

    dp = lax.axis_index("dp")
    tensor = lax.axis_index("tensor")
    core = tensor % 2
    side = dp % 2
    group = dp // 2
    groups = n // 2
    core_peer = (dp, tensor + 1 - 2 * core)
    y_peer = (dp, lax.rem(tensor + 2, 4))
    x_peer = (dp + 1 - 2 * side, tensor)

    stored = (w_query, w_key, w_value, w_output, w_gate, w_up, w_down)
    held = (v_query, v_key, v_value, v_output, v_gate, v_up, v_down)
    loads = {}
    for l in range(LAYERS):
        for i, (src, dst) in enumerate(zip(stored, held)):
            loads[l, i] = pltpu.make_async_copy(src.at[l], dst.at[l], w_sem.at[l, i])
            loads[l, i].start()

    arriving = [
        pltpu.make_async_copy(hidden_in, stream.at[0], edge.at[0]),
        pltpu.make_async_copy(cotangent, upstream, edge.at[1]),
    ]
    for c in arriving:
        c.start()

    barrier = pltpu.get_barrier_semaphore()
    greeted = [core_peer, y_peer] + [(lax.rem(dp + k, n), tensor) for k in range(1, n)]
    for peer in greeted:
        pl.semaphore_signal(barrier, inc=1, device_id=peer, device_id_type=MESH)
    pl.semaphore_wait(barrier, len(greeted))

    def remote(src, dst, s, r, peer):
        return pltpu.make_async_remote_copy(
            src_ref=src, dst_ref=dst, send_sem=s, recv_sem=r, device_id=peer, device_id_type=MESH
        )

    unsent = []
    missing = {}
    leaving = {}

    ways = {}
    kinds = {
        "mixed": (0, mixed_out, mixed_all, False),
        "query": (1, qkv_out, query_all, False),
        "normed_two": (2, normed_two_out, normed_two_all, True),
        "g": (3, g_out, g_all, True),
        "keyval": (4, qkv_out, keyval_all, False),
    }
    spans = {"query": slice(0, heads * HD), "keyval": slice(heads * HD, qkv_out.shape[2])}

    quarter_width = width // 4

    def block(kind, l, index, owner=None):
        _, _, everywhere, shared = kinds[kind]
        rows = pl.ds(pl.multiple_of(index * length, 8), length)
        if (kind, l) in SHARED_Y:
            at = tensor if owner is None else owner
            return everywhere.at[l, rows, columns(at * quarter_width, quarter_width)]
        if shared:
            return everywhere.at[l, rows, columns(core * side_width, side_width)]
        return everywhere.at[l, rows]

    def own_of(kind, l):
        own = kinds[kind][1]
        return own.at[l, :, spans[kind]] if kind in spans else own.at[l]

    def send_own(kind, l):
        a, own, everywhere, shared = kinds[kind]
        slot = a * LAYERS + l
        if (kind, l) in SHARED_Y:
            mine = own.at[l, :, columns(tensor * quarter_width, quarter_width)]
        elif shared:
            mine = own.at[l, :, columns(core * side_width, side_width)]
        else:
            mine = own_of(kind, l)
        for k in range(groups):
            if k == 0:
                c = remote(
                    mine, block(kind, l, dp), x_send.at[slot, 0], x_recv.at[slot, 0], x_peer
                )
            else:
                peer = (lax.rem(group + k, groups) * 2 + side, tensor)
                c = remote(
                    mine, block(kind, l, dp), z_send.at[slot, k], z_recv.at[slot, k], peer
                )
            c.start()
            ways[kind, l, "own", k] = c
            unsent.append(c)
        rows = pl.ds(pl.multiple_of(dp * length, 8), length)
        c = pltpu.make_async_copy(own_of(kind, l), everywhere.at[l, rows], local.at[slot])
        c.start()
        missing.setdefault((kind, l), []).append(c.wait)

    def source_of(i):
        if i < groups - 1:
            return lax.rem(group + groups - 1 - i, groups) * 2 + side
        return lax.rem(group + 2 * groups - 1 - i, groups) * 2 + 1 - side

    def to_core(kind, l, i):
        a = kinds[kind][0]
        if kinds[kind][3]:
            slot = (a - 2) * LAYERS + l
            here = block(kind, l, source_of(i))
            c = remote(here, here, c_send.at[slot, i], c_recv.at[slot, i], core_peer)
            c.start()
            unsent.append(c)
            missing[kind, l].append(c.wait_recv)

    def pass_one(kind, l, k):
        slot = kinds[kind][0] * LAYERS + l
        ways[kind, l, "own", k].wait_recv()
        here = block(kind, l, source_of(k - 1))
        c = remote(here, here, x_send.at[slot, k], x_recv.at[slot, k], x_peer)
        c.start()
        ways[kind, l, "x", k] = c
        unsent.append(c)
        to_core(kind, l, k - 1)

    def pass_part(kind, l, part, parts):
        for k in range(1 + part * (groups - 1) // parts, 1 + (part + 1) * (groups - 1) // parts):
            pass_one(kind, l, k)

    def pass_on(kind, l):
        pass_part(kind, l, 0, 1)

    def take_one(kind, l, k):
        ways[kind, l, "own" if k == 0 else "x", k].wait_recv()
        to_core(kind, l, groups - 1 + k)

    def take_across(kind, l):
        for k in range(groups):
            take_one(kind, l, k)

    def share_one(kind, l, i):
        slot = (kinds[kind][0] - 2) * LAYERS + l
        here = block(kind, l, source_of(i))
        c = remote(here, here, y_send.at[slot, i], y_recv.at[slot, i], y_peer)
        c.start()
        ways[kind, l, "y", i] = c
        unsent.append(c)

    def share_y(kind, l, part=0, parts=1):
        if (kind, l) in SHARED_Y:
            for i in range(part * (n - 1) // parts, (part + 1) * (n - 1) // parts):
                share_one(kind, l, i)

    def take_y(kind, l):
        if (kind, l) in SHARED_Y:
            slot = (kinds[kind][0] - 2) * LAYERS + l
            for i in range(n - 1):
                ways[kind, l, "y", i].wait_recv()
                here = block(kind, l, source_of(i), lax.rem(tensor + 2, 4))
                c = remote(here, here, d_send.at[slot, i], d_recv.at[slot, i], core_peer)
                c.start()
                unsent.append(c)
                missing[kind, l].append(c.wait_recv)

    def complete(kind, l):
        for wait in missing.pop((kind, l)):
            wait()
        if (kind, l) in leaving:
            settle_slices(kind, l)

    slices = {
        "normed": (0, slices_out, normed_all, True),
        "grad_att": (1, slices_out, grad_att_all, True),
        "gains": (2, gains_out, gains_all, False),
    }

    slice_parts = 4 if piece % 32 == 0 else 2
    slice_rows = piece // slice_parts
    slice_mine = tensor if slice_parts == 4 else core

    def sliced(kind, l, index, owner=None):
        everywhere = slices[kind][2]
        if slices[kind][3]:
            at = slice_mine if owner is None else owner
            rows = pl.ds(pl.multiple_of(at * slice_rows, 8), slice_rows)
            return everywhere.at[l, index, rows]
        return everywhere.at[l, index]

    def sliced_own(kind, slot, index, whole=False):
        own = slices[kind][1]
        if not slices[kind][3]:
            return own.at[slot, index]
        if whole:
            return own.at[slot, pl.ds(pl.multiple_of(index * piece, 8), piece)]
        first = pl.multiple_of(index * piece + slice_mine * slice_rows, 8)
        return own.at[slot, pl.ds(first, slice_rows)]

    def send_slices(kind, l):
        b, own, everywhere, halves = slices[kind]
        slot = b * LAYERS + l
        held_at = LAYERS - 1 - l if kind == "grad_att" else l
        sent = []
        for k in range(1, n):
            to = lax.rem(dp + k, n)
            c = remote(
                sliced_own(kind, held_at, to),
                sliced(kind, l, dp),
                a_send.at[slot, k],
                a_recv.at[slot, k],
                (to, tensor),
            )
            c.start()
            ways[kind, l, k] = c
            sent.append(c.wait_send)
        c = pltpu.make_async_copy(
            sliced_own(kind, held_at, dp, True), everywhere.at[l, dp], local.at[5 * LAYERS + slot]
        )
        c.start()
        missing[kind, l] = []
        leaving[kind, l] = sent + [c.wait]

    def settle_slices(kind, l):
        for wait in leaving.pop((kind, l)):
            wait()

    def take_slices(kind, l):
        b, _, everywhere, divided = slices[kind]
        slot = b * LAYERS + l
        for k in range(1, n):
            ways[kind, l, k].wait_recv()
            if divided:
                here = sliced(kind, l, lax.rem(dp + n - k, n))
                c = remote(here, here, b_send.at[slot, k], b_recv.at[slot, k], core_peer)
                c.start()
                unsent.append(c)
                missing[kind, l].append(c.wait_recv)
                if slice_parts == 4:
                    c = remote(here, here, e_send.at[slot, k], e_recv.at[slot, k], y_peer)
                    c.start()
                    unsent.append(c)
                    ways[kind, l, "y", k] = c

    def take_slices_y(kind, l):
        slot = slices[kind][0] * LAYERS + l
        if slice_parts == 4:
            for k in range(1, n):
                ways[kind, l, "y", k].wait_recv()
                here = sliced(kind, l, lax.rem(dp + n - k, n), lax.rem(tensor + 2, 4))
                c = remote(here, here, f_send.at[slot, k], f_recv.at[slot, k], core_peer)
                c.start()
                unsent.append(c)
                missing[kind, l].append(c.wait_recv)

    def turn_over(dst, src):
        for t in range(width // 128):
            at = slice(t * 128, (t + 1) * 128)
            dst[at, :] = jnp.transpose(src[:, at])

    def cut(dst, l, src):
        for t in range(n):
            dst[l, t] = src[:, t * piece : (t + 1) * piece]

    def tensor_sum(j, tile, base, dest, meanwhile):
        def copy(stage, k, src, dst, peer):
            return remote(src, dst, sum_send.at[j, stage, k], sum_recv.at[j, stage, k], peer)

        def at(k):
            return pl.ds(pl.multiple_of(k * TILE, 128), TILE)

        def mine(k):
            return columns(core * side_width + k * TILE, TILE)

        def other(k):
            return columns((1 - core) * side_width + k * TILE, TILE)

        def first(k):
            return copy(0, k, part.at[:, at(k)], from_core.at[j % 2, :, at(k)], core_peer)

        def second(k):
            return copy(1, k, half.at[:, at(k)], from_y.at[j % 2, :, at(k)], y_peer)

        def third(k):
            return copy(2, k, dest.at[:, mine(k)], dest.at[:, mine(k)], core_peer)

        def begin(k):
            part[:, at(k)] = tile(other(k))
            first(k).start()

        def middle(k):
            own = tile(mine(k))
            first(k).wait_recv()
            half[:, at(k)] = own + from_core[j % 2, :, at(k)]
            second(k).start()

        def finish(k):
            second(k).wait_recv()
            total = half[:, at(k)] + from_y[j % 2, :, at(k)]
            if base is not None:
                total = base[:, mine(k)] + total
            dest[:, mine(k)] = total
            third(k).start()

        def settle(k):
            third(k).wait_recv()
            first(k).wait_send()
            second(k).wait_send()
            third(k).wait_send()

        each(chunks, begin)
        each(chunks, middle)
        meanwhile()
        each(chunks, finish)
        each(chunks, settle)

    def inverse_rms(values):
        return lax.rsqrt(jnp.mean(values * values, axis=-1, keepdims=True) + epsilon)

    def normalize(src, gain, l, out, out_wide):
        def rows_of(i):
            rows = pl.ds(pl.multiple_of(i * ROWS, ROWS), ROWS)
            values = src[rows, :]
            normed = (values * inverse_rms(values) * gain[l : l + 1, :]).astype(low)
            out[rows, :] = normed
            out_wide[rows, :] = normed.astype(full)

        each(length // ROWS, rows_of)

    def norm_backward(grad, values_ref, gain, l, row, before, out, out_low, out_wide):
        def rows_of(i, total):
            rows = pl.ds(pl.multiple_of(i * ROWS, ROWS), ROWS)
            values = values_ref[rows, :]
            grad_normed = grad[rows, :]
            inverse = inverse_rms(values)
            normalized = values * inverse
            term = grad_normed * normalized
            total = total + term[:8] + term[8:]
            scaled = grad_normed * gain[l : l + 1, :]
            back = inverse * (
                scaled - normalized * jnp.mean(scaled * normalized, axis=-1, keepdims=True)
            )
            after = before[rows, :] + back
            out[rows, :] = after
            if out_low is not None:
                after_low = after.astype(low)
                out_low[rows, :] = after_low
                out_wide[rows, :] = after_low.astype(full)
            return total

        total = lax.fori_loop(0, length // ROWS, rows_of, jnp.zeros((8, width), full))
        gain_rows[row : row + 1, :] = jnp.sum(total, axis=0, keepdims=True)

    def turned(values, direction):
        u, w = values[:turn], values[turn:]
        c, s = cosine[...], sine[...]
        return jnp.concatenate([u * c - direction * w * s, w * c + direction * u * s], axis=0)

    def head(ref, l, h):
        return ref[l, h * HD : (h + 1) * HD, :]

    def scores_t(l, h):
        raw = tn(head(key_t, l, h // share), head(query_t, l, h)) * scale
        return jnp.where(allowed[...] > 0.5, raw, masked_score)

    def steps(*calls):
        def run():
            for call, *what in calls:
                call(*what)

        return run

    def attend(l):
        for i in range(3):
            loads[l, i].wait()
        source = normed_low[...]
        for ref, dst, count, rope in (
            (v_query, query_t, heads, True),
            (v_key, key_t, kv_heads, True),
            (v_value, value_t, kv_heads, False),
        ):
            projected = jnp.transpose(nn(source, ref[l])) if ref is v_query else nt(ref[l], source)
            for h in range(count):
                values = projected[h * HD : (h + 1) * HD]
                values = turned(values, 1.0) if rope else values
                dst[l, h * HD : (h + 1) * HD, :] = values.astype(low)
        for h in range(heads):
            scores = scores_t(l, h)
            row_max = jnp.max(scores, axis=0, keepdims=True)
            exponent = jnp.exp(scores - row_max)
            row_total = jnp.sum(exponent, axis=0, keepdims=True)
            probabilities = (exponent / row_total).astype(low)
            logsum[l, h : h + 1, :] = row_max + jnp.log(row_total)
            mixed = nn(head(value_t, l, h // share), probabilities)
            mixed_t[l, h * HD : (h + 1) * HD, :] = mixed.astype(low).astype(full)
        mixed = jnp.transpose(mixed_t[l])
        mixed_out[l] = mixed
        left_low[:, : heads * HD] = mixed.astype(low)

    def attention_back(l):
        grad_mixed_t = jnp.transpose(nt(normed_low[...], v_output[l]).astype(low).astype(full))
        for g in range(kv_heads):
            grad_value = jnp.zeros((HD, length), full)
            grad_key = jnp.zeros((HD, length), full)
            for h in range(g * share, (g + 1) * share):
                grad_mixed = grad_mixed_t[h * HD : (h + 1) * HD]
                grad_mixed_low = grad_mixed.astype(low)
                again = jnp.exp(scores_t(l, h) - logsum[l, h : h + 1, :])
                grad_value += nt(grad_mixed_low, again.astype(low))
                grad_probs = tn(head(value_t, l, g), grad_mixed_low)
                row_dot = jnp.sum(grad_mixed * head(mixed_t, l, h), axis=0, keepdims=True)
                grad_scores = (again * (grad_probs - row_dot) * scale).astype(low)
                grad_query = nn(head(key_t, l, g), grad_scores)
                grad_key += nt(head(query_t, l, h), grad_scores)
                wide[h * HD : (h + 1) * HD, :] = turned(grad_query, -1.0).astype(low).astype(full)
            at = (heads + g) * HD
            wide[at : at + HD, :] = turned(grad_key, -1.0).astype(low).astype(full)
            at = (heads + kv_heads + g) * HD
            wide[at : at + HD, :] = grad_value.astype(low).astype(full)
        rows = jnp.transpose(wide[...])
        qkv_out[l] = rows
        left_low[:, : rows.shape[1]] = rows.astype(low)

    step = hidden_units // 2
    nothing = lambda: None

    def turn_normed(l):
        turn_over(slices_out.at[l], normed_two_out.at[l])
        send_slices("normed", l)

    def turn_grad_att(l):
        settle_slices("normed", LAYERS - 1 - l)
        turn_over(slices_out.at[LAYERS - 1 - l], part_wide)
        send_slices("grad_att", l)

    def attention_layer(l, meanwhile):
        normalize(stream.at[2 * l], attn_gain, l, normed_low, normed_two_out.at[l])
        attend(l)
        send_own("mixed", l)
        loads[l, 3].wait()
        tensor_sum(
            2 * l,
            lambda at: nn(left_low[:, : heads * HD], v_output[l, :, at]),
            stream.at[2 * l],
            stream.at[2 * l + 1],
            steps((turn_normed, l), (meanwhile,)),
        )

    def mlp_layer(l, meanwhile):
        normalize(stream.at[2 * l + 1], mlp_gain, l, normed_low, normed_two_out.at[l])
        send_own("normed_two", l)
        loads[l, 4].wait()
        loads[l, 5].wait()

        def units(i):
            at = columns(i * TILE, TILE)
            source = normed_low[...]
            gate = nn(source, v_gate[l, :, at])
            up = nn(source, v_up[l, :, at])
            gate_pre[l, :, at] = gate
            up_pre[l, :, at] = up
            left_low[:, at] = (gate * jax.nn.sigmoid(gate) * up).astype(low)

        each(hidden_units // TILE, units)
        loads[l, 6].wait()
        tensor_sum(
            2 * l + 1,
            lambda at: nn(left_low[...], v_down[l, :, at]),
            stream.at[2 * l + 1],
            stream.at[2 * l + 2],
            meanwhile,
        )

    def mlp_back(l, meanwhile):
        def units(i):
            at = columns(i * TILE, TILE)
            grad_act = nt(normed_low[...], v_down[l, at, :])
            left, right, _ = mlp_grads(gate_pre[l, :, at], up_pre[l, :, at], grad_act)
            left_low[:, at] = left
            right_low[:, at] = right

        each(hidden_units // TILE, units)
        j = 2 * LAYERS + 2 * (LAYERS - 1 - l)
        tensor_sum(
            j,
            lambda at: nt(left_low[...], v_gate[l, at, :]) + nt(right_low[...], v_up[l, at, :]),
            None,
            grads.at[j % 2],
            meanwhile,
        )
        norm_backward(
            grads.at[j % 2],
            stream.at[2 * l + 1],
            mlp_gain,
            l,
            LAYERS + l,
            upstream,
            upstream,
            normed_low,
            part_wide,
        )

    part_wide = grads.at[2]

    def attention_layer_back(l, meanwhile):
        attention_back(l)
        send_own("query", l)
        if l == 0:
            send_own("keyval", l)
        j = 2 * LAYERS + 2 * (LAYERS - 1 - l) + 1
        q_end, k_end = heads * HD, (heads + kv_heads) * HD
        v_end = (heads + 2 * kv_heads) * HD
        tensor_sum(
            j,
            lambda at: nt(left_low[:, :q_end], v_query[l, at, :])
            + nn(left_low[:, q_end:k_end], v_key[l, :, at])
            + nn(left_low[:, k_end:v_end], v_value[l, :, at]),
            None,
            grads.at[j % 2],
            steps((turn_grad_att, l), (meanwhile,)),
        )
        last = l == 0
        norm_backward(
            grads.at[j % 2],
            stream.at[2 * l],
            attn_gain,
            l,
            l,
            upstream,
            upstream,
            None if last else normed_low,
            None if last else g_out.at[l - 1],
        )

    window = cut_a.shape[0]
    start = jnp.minimum(dp * piece // 128 * 128, width - window)
    offset = pl.multiple_of(dp * piece - start, 8)

    def stream_tokens(first, count, copies, body):
        def go(i, slot):
            for c in copies(i, slot):
                c.start()

        go(first, 0)

        def step(i):
            slot = lax.rem(i, 2)
            for c in copies(first + i, slot):
                c.wait()

            @pl.when(i + 1 < count)
            def _():
                go(first + i + 1, 1 - slot)

            body(slot)

        each(count, step)

    def mlp_gradients(l, share=0, shares=1):
        def copies(i, slot):
            rows = pl.ds(pl.multiple_of(i * TOKENS, 8), TOKENS)
            return (
                pltpu.make_async_copy(
                    normed_two_all.at[l, rows], token_a.at[slot], fetch.at[0, slot]
                ),
                pltpu.make_async_copy(g_all.at[l, rows], token_b.at[slot], fetch.at[1, slot]),
            )

        if share == 0:
            sum_g[...] = jnp.zeros_like(sum_g)
            sum_u[...] = jnp.zeros_like(sum_u)
            sum_d[...] = jnp.zeros_like(sum_d)

        def body(slot):
            low_a[...] = token_a[slot].astype(low)
            low_b[...] = token_b[slot].astype(low)
            cut_a[...] = jnp.transpose(token_a[slot, :, columns(start, window)]).astype(low)
            cut_b[...] = jnp.transpose(token_b[slot, :, columns(start, window)]).astype(low)

            def units(i):
                at = columns(i * UNITS, UNITS)
                gate = nn(low_a[...], v_gate[l, :, at])
                up = nn(low_a[...], v_up[l, :, at])
                grad_act = nt(low_b[...], v_down[l, at, :])
                left, right, activated = mlp_grads(gate, up, grad_act)
                sum_g[:, at] += nn(cut_a[...], left)
                sum_u[:, at] += nn(cut_a[...], right)
                sum_d[:, at] += nn(cut_b[...], activated)

            each(hidden_units // UNITS, units)

        count = n * length // TOKENS // shares
        stream_tokens(share * count, count, copies, body)
        if share < shares - 1:
            return
        outs = [
            pltpu.make_async_copy(src.at[pl.ds(offset, piece)], dst.at[l], edge.at[4 + i])
            for i, (src, dst) in enumerate(((sum_g, grad_g), (sum_u, grad_u), (sum_d, grad_d)))
        ]
        for c in outs:
            c.start()
        for c in outs:
            c.wait()

    def attention_gradients(l):
        blocks = TOKENS // length

        def copies(i, slot):
            rows = pl.ds(pl.multiple_of(i * TOKENS, 8), TOKENS)
            return (
                pltpu.make_async_copy(
                    query_all.at[l, rows],
                    state_qkv.at[slot, :, spans["query"]],
                    fetch.at[2, slot],
                ),
                pltpu.make_async_copy(
                    keyval_all.at[l, rows],
                    state_qkv.at[slot, :, spans["keyval"]],
                    fetch.at[4 + 2 * blocks, slot],
                ),
                pltpu.make_async_copy(
                    mixed_all.at[l, rows], state_mixed.at[slot], fetch.at[3, slot]
                ),
            ) + tuple(
                pltpu.make_async_copy(
                    src.at[l, i * blocks + b],
                    dst.at[slot, :, pl.ds(b * length, length)],
                    fetch.at[at + b, slot],
                )
                for src, dst, at in ((normed_all, state_a, 4), (grad_att_all, state_b, 4 + blocks))
                for b in range(blocks)
            )

        for ref in (sum_q, sum_k, sum_v, sum_o):
            ref[...] = jnp.zeros_like(ref)
        q_end, k_end = heads * HD, (heads + kv_heads) * HD

        def body(slot):
            normed = state_a[slot].astype(low)
            qkv = state_qkv[slot].astype(low)
            sum_q[...] += nn(normed, qkv[:, :q_end])
            sum_k[...] += nn(normed, qkv[:, q_end:k_end])
            sum_v[...] += nn(normed, qkv[:, k_end:])
            sum_o[...] += nn(state_b[slot].astype(low), state_mixed[slot].astype(low))

        stream_tokens(0, n * length // TOKENS, copies, body)
        outs = [
            pltpu.make_async_copy(src, dst.at[l], edge.at[7 + i])
            for i, (src, dst) in enumerate(
                ((sum_q, grad_q), (sum_k, grad_k), (sum_v, grad_v), (sum_o, grad_o))
            )
        ]
        for c in outs:
            c.start()
        for c in outs:
            c.wait()

    for c in arriving:
        c.wait()
    g_out[LAYERS - 1] = upstream[...].astype(low).astype(full)
    send_own("g", LAYERS - 1)
    gain_rows[...] = jnp.zeros_like(gain_rows)

    attention_layer(0, nothing)
    mlp_layer(0, steps((pass_on, "g", 1), (take_slices, "normed", 0)))
    attention_layer(
        1,
        steps((pass_on, "mixed", 0), (take_across, "g", 1), (share_y, "g", 1, 0, 3)),
    )
    mlp_layer(
        1,
        steps((pass_on, "normed_two", 0), (take_across, "mixed", 0), (share_y, "g", 1, 1, 3)),
    )
    going = [pltpu.make_async_copy(stream.at[2 * LAYERS], hidden_out, edge.at[2])]
    going[0].start()
    normed_low[...] = g_out[LAYERS - 1].astype(low)
    mlp_back(
        1,
        steps(
            (take_slices, "normed", 1),
            (pass_on, "mixed", 1),
            (take_across, "normed_two", 0),
            (share_y, "g", 1, 2, 3),
        ),
    )
    attention_layer_back(
        1,
        steps(
            (pass_on, "normed_two", 1),
            (take_across, "mixed", 1),
            (share_y, "normed_two", 0, 0, 3),
        ),
    )
    send_own("g", 0)
    send_own("keyval", 1)
    mlp_back(
        0,
        steps(
            (take_slices, "grad_att", 1),
            (pass_on, "query", 1),
            (share_y, "normed_two", 0, 1, 3),
            (take_y, "g", 1),
            (take_slices_y, "normed", 0),
        ),
    )
    attention_layer_back(
        0,
        steps(
            (pass_on, "g", 0),
            (take_across, "normed_two", 1),
            (share_y, "normed_two", 0, 2, 3),
            (complete, "normed_two", 1),
            (complete, "g", 1),
            (mlp_gradients, 1, 0, 4),
        ),
    )
    going.append(pltpu.make_async_copy(upstream, grad_input, edge.at[3]))
    going[1].start()
    cut(gains_out, 0, gain_rows)
    send_slices("gains", 0)
    for call, *what in (
        (pass_on, "keyval", 1),
        (take_across, "g", 0),
        (share_y, "g", 0),
        (take_slices_y, "normed", 1),
        (take_slices_y, "grad_att", 1),
        (take_y, "normed_two", 0),
        (take_across, "query", 1),
        (mlp_gradients, 1, 1, 4),
        (take_slices, "grad_att", 0),
        (pass_part, "query", 0, 0, 3),
        (mlp_gradients, 1, 2, 4),
        (pass_part, "query", 0, 1, 3),
        (pass_part, "query", 0, 2, 3),
        (mlp_gradients, 1, 3, 4),
        (pass_part, "keyval", 0, 0, 3),
        (take_across, "keyval", 1),
        (take_y, "g", 0),
        (pass_part, "keyval", 0, 1, 3),
        (complete, "normed_two", 0),
        (complete, "g", 0),
        (mlp_gradients, 0, 0, 4),
        (pass_part, "keyval", 0, 2, 3),
        (take_across, "query", 0),
        (mlp_gradients, 0, 1, 4),
        (mlp_gradients, 0, 2, 4),
        (mlp_gradients, 0, 3, 4),
        (complete, "query", 1),
        (complete, "keyval", 1),
        (complete, "mixed", 1),
        (complete, "normed", 1),
        (complete, "grad_att", 1),
        (attention_gradients, 1),
        (take_across, "keyval", 0),
        (take_slices_y, "grad_att", 0),
        (take_slices, "gains", 0),
        (complete, "gains", 0),
        (complete, "query", 0),
        (complete, "keyval", 0),
        (complete, "mixed", 0),
        (complete, "normed", 0),
        (complete, "grad_att", 0),
        (attention_gradients, 0),
    ):
        call(*what)
    assert not missing
    for c in unsent:
        c.wait_send()
    for key in list(leaving):
        settle_slices(*key)
    for c in going:
        c.wait()


def layers(n, hidden_in, cotangent, cosine, sine, allowed, attn_gain, mlp_gain, weights):
    length, width = hidden_in.shape
    w_query, w_key, w_value, w_output, w_gate, w_up, w_down = weights
    q_width, kv_width, hidden_units = w_query.shape[2], w_key.shape[1], w_gate.shape[2]
    qkv_width = q_width + 2 * kv_width
    piece = width // n
    f32 = lambda *shape: jax.ShapeDtypeStruct(shape, full)
    out_shape = [
        f32(length, width),
        f32(length, width),
        f32(LAYERS, piece, q_width),
        f32(LAYERS, piece, kv_width),
        f32(LAYERS, piece, kv_width),
        f32(LAYERS, piece, q_width),
        f32(LAYERS, piece, hidden_units),
        f32(LAYERS, piece, hidden_units),
        f32(LAYERS, piece, hidden_units),
        f32(LAYERS, n * length, q_width),
        f32(LAYERS, n * length, q_width),
        f32(LAYERS, n * length, 2 * kv_width),
        f32(LAYERS, n * length, width),
        f32(LAYERS, n * length, width),
        f32(LAYERS, n, piece, length),
        f32(LAYERS, n, piece, length),
        f32(1, n, 8, piece),
    ]
    vmem = pl.BlockSpec(memory_space=pltpu.VMEM)
    anywhere = pl.BlockSpec(memory_space=pl.ANY)
    dma = pltpu.SemaphoreType.DMA
    keep = lambda dtype, *shape: pltpu.VMEM(shape, dtype)
    sums = 4 * LAYERS
    chunks = width // 2 // TILE
    window = pl.cdiv(piece + 128 - math.gcd(piece, 128), 128) * 128
    return pl.pallas_call(
        functools.partial(layers_kernel, n),
        out_shape=out_shape,
        in_specs=[anywhere] * 2 + [vmem] * 5 + [anywhere] * 7,
        out_specs=[anywhere] * 17,
        scratch_shapes=[keep(low, *w.shape) for w in weights]
        + [
            keep(full, 2 * LAYERS + 1, length, width),
            keep(full, 3, length, width),
            keep(full, length, width),
            keep(low, length, width),
            keep(low, length, hidden_units),
            keep(low, length, hidden_units),
            keep(full, LAYERS, length, hidden_units),
            keep(full, LAYERS, length, hidden_units),
            keep(low, LAYERS, q_width, length),
            keep(low, LAYERS, kv_width, length),
            keep(low, LAYERS, kv_width, length),
            keep(full, LAYERS, q_width, length),
            keep(full, LAYERS, 8, length),
            keep(full, LAYERS, length, q_width),
            keep(full, LAYERS, length, qkv_width),
            keep(full, LAYERS, length, width),
            keep(full, LAYERS, length, width),
            keep(full, LAYERS, width, length),
            keep(full, 1, n, 8, piece),
            keep(full, 8, width),
            keep(full, qkv_width, length),
            keep(full, length, width // 2),
            keep(full, 2, length, width // 2),
            keep(full, length, width // 2),
            keep(full, 2, length, width // 2),
            keep(full, 2, TOKENS, width),
            keep(full, 2, TOKENS, width),
            keep(low, TOKENS, width),
            keep(low, TOKENS, width),
            keep(low, window, TOKENS),
            keep(low, window, TOKENS),
            keep(full, window, hidden_units),
            keep(full, window, hidden_units),
            keep(full, window, hidden_units),
            keep(full, 2, TOKENS, qkv_width),
            keep(full, 2, TOKENS, q_width),
            keep(full, 2, piece, TOKENS),
            keep(full, 2, piece, TOKENS),
            keep(full, piece, q_width),
            keep(full, piece, kv_width),
            keep(full, piece, kv_width),
            keep(full, piece, q_width),
            dma((LAYERS, 7)),
            dma((sums, 3, chunks)),
            dma((sums, 3, chunks)),
            dma((5 * LAYERS, n // 2)),
            dma((5 * LAYERS, n // 2)),
            dma((5 * LAYERS, n // 2)),
            dma((5 * LAYERS, n // 2)),
            dma((2 * LAYERS, n)),
            dma((2 * LAYERS, n)),
            dma((3 * LAYERS, n)),
            dma((3 * LAYERS, n)),
            dma((2 * LAYERS, n)),
            dma((2 * LAYERS, n)),
            dma((2 * LAYERS, n)),
            dma((2 * LAYERS, n)),
            dma((2 * LAYERS, n)),
            dma((2 * LAYERS, n)),
            dma((2 * LAYERS, n)),
            dma((2 * LAYERS, n)),
            dma((2 * LAYERS, n)),
            dma((2 * LAYERS, n)),
            dma((8 * LAYERS,)),
            dma((11,)),
            dma((5 + 2 * (TOKENS // length), 2)),
        ],
        compiler_params=pltpu.CompilerParams(
            collective_id=0, has_side_effects=True, vmem_limit_bytes=66_000_000
        ),
        name="layers",
    )(hidden_in, cotangent, cosine, sine, allowed, attn_gain, mlp_gain, *weights)


def shards(
    hidden_in,
    cotangent,
    segment_ids,
    positions,
    w_query,
    w_key,
    w_value,
    w_output,
    w_gate,
    w_up,
    w_down,
    attn_gain,
    mlp_gain,
):
    n = lax.axis_size("dp")
    length = hidden_in.shape[0]
    weights = (
        w_query,
        jnp.swapaxes(w_key, 1, 2),
        jnp.swapaxes(w_value, 1, 2),
        w_output,
        w_gate,
        w_up,
        w_down,
    )
    half_dim = HD // 2
    frequencies = rope_base ** (-(jnp.arange(half_dim).astype(jnp.float32) * 2.0 / HD))
    angles = frequencies[:, None] * positions[0].astype(jnp.float32)[None, :]
    segments = segment_ids[0]
    token_order = jnp.arange(length)
    allowed = (segments[:, None] == segments[None, :]) & (
        token_order[:, None] <= token_order[None, :]
    )
    outs = layers(
        n,
        hidden_in,
        cotangent,
        jnp.cos(angles),
        jnp.sin(angles),
        allowed.astype(jnp.float32),
        attn_gain,
        mlp_gain,
        weights,
    )
    hidden, grad_input, grad_q, grad_k, grad_v, grad_o, grad_g, grad_u, grad_d = outs[:9]
    gain_sums = jnp.sum(outs[-1][0], axis=0)
    return (
        hidden,
        grad_input,
        grad_q,
        grad_k,
        grad_v,
        jnp.swapaxes(grad_o, 1, 2),
        grad_g,
        grad_u,
        jnp.swapaxes(grad_d, 1, 2),
        gain_sums[:LAYERS],
        gain_sums[LAYERS : 2 * LAYERS],
    )


def solution(mesh):
    return jax.shard_map(
        shards,
        mesh=mesh,
        in_specs=(
            P("dp", None),
            P("dp", None),
            P("dp", None),
            P("dp", None),
            P(None, None, "tensor"),
            P(None, None, "tensor"),
            P(None, None, "tensor"),
            P(None, "tensor", None),
            P(None, None, "tensor"),
            P(None, None, "tensor"),
            P(None, "tensor", None),
            P(),
            P(),
        ),
        out_specs=(
            P("dp", None),
            P("dp", None),
            P(None, "dp", "tensor"),
            P(None, "dp", "tensor"),
            P(None, "dp", "tensor"),
            P(None, "tensor", "dp"),
            P(None, "dp", "tensor"),
            P(None, "dp", "tensor"),
            P(None, "tensor", "dp"),
            P(None, "dp"),
            P(None, "dp"),
        ),
        check_vma=False,
    )
```

```python
import functools
import math

import jax
import jax.numpy as jnp
from jax import lax
from jax.experimental import pallas as pl
from jax.experimental.pallas import tpu as pltpu
from jax.sharding import PartitionSpec as P

HD = 96
LAYERS = 2
TILE = 256
UNITS = 512
RELAYED = (
    ("g", 1),
    ("mixed", 0),
    ("normed_two", 0),
    ("mixed", 1),
    ("normed_two", 1),
    ("query", 1),
    ("g", 0),
    ("keyval", 1),
    ("query", 0),
    ("keyval", 0),
)
ROWS = 16
TOKENS = 256
SHARED_Y = (("g", 1), ("normed_two", 0), ("g", 0))
MESH = pl.DeviceIdType.MESH


epsilon = 1e-05
rope_base = 100000.0
masked_score = -1e30
low = jnp.bfloat16
full = jnp.float32


def nn(a, b):
    return lax.dot_general(a, b, (((1,), (0,)), ((), ())), preferred_element_type=full)


def nt(a, b):
    return lax.dot_general(a, b, (((1,), (1,)), ((), ())), preferred_element_type=full)


def tn(a, b):
    return lax.dot_general(a, b, (((0,), (0,)), ((), ())), preferred_element_type=full)


def mlp_grads(gate_pre, up_pre, grad_act):
    sigmoid_gate = jax.nn.sigmoid(gate_pre)
    grad_gate_low = (
        grad_act * up_pre * sigmoid_gate * (1.0 + gate_pre * (1.0 - sigmoid_gate))
    ).astype(low)
    grad_up_low = (grad_act * gate_pre * sigmoid_gate).astype(low)
    activated = (gate_pre * sigmoid_gate * up_pre).astype(low)
    return grad_gate_low, grad_up_low, activated


def each(count, body):
    def step(i, carry):
        body(i)
        return carry

    lax.fori_loop(0, count, step, 0)


def columns(start, size):
    return pl.ds(pl.multiple_of(start, 128), size)


def layers_kernel(n, *refs):
    (
        hidden_in,
        cotangent,
        cosine,
        sine,
        allowed,
        attn_gain,
        mlp_gain,
        w_query,
        w_key,
        w_value,
        w_output,
        w_gate,
        w_up,
        w_down,
        hidden_out,
        grad_input,
        grad_q,
        grad_k,
        grad_v,
        grad_o,
        grad_g,
        grad_u,
        grad_d,
        mixed_all,
        query_all,
        keyval_all,
        normed_two_all,
        g_all,
        normed_all,
        grad_att_all,
        gains_all,
        v_query,
        v_key,
        v_value,
        v_output,
        v_gate,
        v_up,
        v_down,
        stream,
        grads,
        upstream,
        normed_low,
        left_low,
        right_low,
        gate_pre,
        up_pre,
        query_t,
        key_t,
        value_t,
        mixed_t,
        logsum,
        mixed_out,
        qkv_out,
        normed_two_out,
        g_out,
        slices_out,
        gains_out,
        gain_rows,
        wide,
        part,
        from_core,
        half,
        from_y,
        token_a,
        token_b,
        low_a,
        low_b,
        cut_a,
        cut_b,
        sum_g,
        sum_u,
        sum_d,
        state_qkv,
        state_mixed,
        state_a,
        state_b,
        sum_q,
        sum_k,
        sum_v,
        sum_o,
        w_sem,
        sum_send,
        sum_recv,
        z_send,
        z_down,
        z_recv,
        x_send,
        x_recv,
        c_send,
        c_recv,
        a_send,
        a_recv,
        b_send,
        b_recv,
        y_send,
        y_recv,
        d_send,
        d_recv,
        e_send,
        e_recv,
        f_send,
        f_recv,
        local,
        edge,
        fetch,
    ) = refs
    length, width = hidden_in.shape
    heads = w_query.shape[2] // HD
    kv_heads = w_key.shape[1] // HD
    share = heads // kv_heads
    hidden_units = w_gate.shape[2]
    piece = width // n
    side_width = width // 2
    chunks = side_width // TILE
    turn = HD // 2
    scale = HD ** (-0.5)

    dp = lax.axis_index("dp")
    tensor = lax.axis_index("tensor")
    core = tensor % 2
    side = dp % 2
    group = dp // 2
    groups = n // 2
    core_peer = (dp, tensor + 1 - 2 * core)
    y_peer = (dp, lax.rem(tensor + 2, 4))
    x_peer = (dp + 1 - 2 * side, tensor)

    stored = (w_query, w_key, w_value, w_output, w_gate, w_up, w_down)
    held = (v_query, v_key, v_value, v_output, v_gate, v_up, v_down)
    loads = {}
    for l in range(LAYERS):
        for i, (src, dst) in enumerate(zip(stored, held)):
            loads[l, i] = pltpu.make_async_copy(src.at[l], dst.at[l], w_sem.at[l, i])
            loads[l, i].start()

    arriving = [
        pltpu.make_async_copy(hidden_in, stream.at[0], edge.at[0]),
        pltpu.make_async_copy(cotangent, upstream, edge.at[1]),
    ]
    for c in arriving:
        c.start()

    barrier = pltpu.get_barrier_semaphore()
    greeted = [core_peer, y_peer] + [(lax.rem(dp + k, n), tensor) for k in range(1, n)]
    for peer in greeted:
        pl.semaphore_signal(barrier, inc=1, device_id=peer, device_id_type=MESH)
    pl.semaphore_wait(barrier, len(greeted))

    def remote(src, dst, s, r, peer):
        return pltpu.make_async_remote_copy(
            src_ref=src, dst_ref=dst, send_sem=s, recv_sem=r, device_id=peer, device_id_type=MESH
        )

    unsent = []
    missing = {}
    conditional = []
    leaving = {}

    ways = {}
    kinds = {
        "mixed": (0, mixed_out, mixed_all, False),
        "query": (1, qkv_out, query_all, False),
        "normed_two": (2, normed_two_out, normed_two_all, True),
        "g": (3, g_out, g_all, True),
        "keyval": (4, qkv_out, keyval_all, False),
    }
    spans = {"query": slice(0, heads * HD), "keyval": slice(heads * HD, qkv_out.shape[2])}

    quarter_width = width // 4

    def block(kind, l, index, owner=None):
        _, _, everywhere, shared = kinds[kind]
        rows = pl.ds(pl.multiple_of(index * length, 8), length)
        if (kind, l) in SHARED_Y:
            at = tensor if owner is None else owner
            return everywhere.at[l, rows, columns(at * quarter_width, quarter_width)]
        if shared:
            return everywhere.at[l, rows, columns(core * side_width, side_width)]
        return everywhere.at[l, rows]

    def own_of(kind, l):
        own = kinds[kind][1]
        return own.at[l, :, spans[kind]] if kind in spans else own.at[l]

    def send_own(kind, l):
        a, own, everywhere, shared = kinds[kind]
        slot = a * LAYERS + l
        if (kind, l) in SHARED_Y:
            mine = own.at[l, :, columns(tensor * quarter_width, quarter_width)]
        elif shared:
            mine = own.at[l, :, columns(core * side_width, side_width)]
        else:
            mine = own_of(kind, l)
        relayed = (kind, l) in RELAYED
        if relayed:
            send_if(
                group < groups - 1,
                lambda: remote(
                    mine,
                    block(kind, l, dp),
                    z_send.at[slot, 0],
                    z_recv.at[slot, 1],
                    ((group + 1) * 2 + side, tensor),
                ),
            )
            send_if(
                group > 0,
                lambda: remote(
                    mine,
                    block(kind, l, dp),
                    z_down.at[slot],
                    z_recv.at[slot, groups - 1],
                    ((group - 1) * 2 + side, tensor),
                ),
            )
        for k in range(1 if relayed else groups):
            if k == 0:
                c = remote(
                    mine, block(kind, l, dp), x_send.at[slot, 0], x_recv.at[slot, 0], x_peer
                )
            else:
                peer = (lax.rem(group + k, groups) * 2 + side, tensor)
                c = remote(
                    mine, block(kind, l, dp), z_send.at[slot, k], z_recv.at[slot, k], peer
                )
            c.start()
            ways[kind, l, "own", k] = c
            unsent.append(c)
        rows = pl.ds(pl.multiple_of(dp * length, 8), length)
        c = pltpu.make_async_copy(own_of(kind, l), everywhere.at[l, rows], local.at[slot])
        c.start()
        missing.setdefault((kind, l), []).append(c.wait)

    def send_if(condition, make):
        @pl.when(condition)
        def _():
            make().start()

        conditional.append((condition, make))

    both = jnp.minimum(group, groups - 1 - group)
    longer_below = (group > groups - 1 - group).astype(jnp.int32)

    def ranked(j):
        single = (j >= 2 * both).astype(jnp.int32)
        below = single * longer_below + (1 - single) * (1 - j % 2)
        distance = single * (j - both + 1) + (1 - single) * (j // 2 + 1)
        return below, distance

    def behind(kind, l, j):
        if (kind, l) in RELAYED:
            below, distance = ranked(j)
            return below * distance + (1 - below) * (groups - distance)
        return j + 1

    def source_of(kind, l, i):
        across = i >= groups - 1
        j = i - groups if across else i
        steps_back = 0 if j < 0 else behind(kind, l, j)
        return lax.rem(group + groups - steps_back, groups) * 2 + (1 - side if across else side)

    def to_core(kind, l, i):
        a = kinds[kind][0]
        if kinds[kind][3]:
            slot = (a - 2) * LAYERS + l
            here = block(kind, l, source_of(kind, l, i))
            c = remote(here, here, c_send.at[slot, i], c_recv.at[slot, i], core_peer)
            c.start()
            unsent.append(c)
            missing[kind, l].append(c.wait_recv)

    def pass_one(kind, l, k):
        slot = kinds[kind][0] * LAYERS + l
        here = block(kind, l, source_of(kind, l, k - 1))
        if (kind, l) in RELAYED:
            below, _ = ranked(k - 1)
            steps_back = behind(kind, l, k - 1)
            remote(
                here, here, z_send.at[slot, k], z_recv.at[slot, steps_back], x_peer
            ).wait_recv()
            send_if(
                jnp.logical_and(below == 1, group < groups - 1),
                lambda: remote(
                    here,
                    here,
                    z_send.at[slot, k],
                    z_recv.at[slot, steps_back + 1],
                    ((group + 1) * 2 + side, tensor),
                ),
            )
            send_if(
                jnp.logical_and(below == 0, group > 0),
                lambda: remote(
                    here,
                    here,
                    z_send.at[slot, k],
                    z_recv.at[slot, steps_back - 1],
                    ((group - 1) * 2 + side, tensor),
                ),
            )
        else:
            ways[kind, l, "own", k].wait_recv()
        c = remote(here, here, x_send.at[slot, k], x_recv.at[slot, k], x_peer)
        c.start()
        ways[kind, l, "x", k] = c
        unsent.append(c)
        to_core(kind, l, k - 1)

    def pass_part(kind, l, part, parts):
        for k in range(1 + part * (groups - 1) // parts, 1 + (part + 1) * (groups - 1) // parts):
            pass_one(kind, l, k)

    def pass_on(kind, l):
        pass_part(kind, l, 0, 1)

    def take_one(kind, l, k):
        ways[kind, l, "own" if k == 0 else "x", k].wait_recv()
        to_core(kind, l, groups - 1 + k)

    def take_across(kind, l):
        for k in range(groups):
            take_one(kind, l, k)

    def share_one(kind, l, i):
        slot = (kinds[kind][0] - 2) * LAYERS + l
        here = block(kind, l, source_of(kind, l, i))
        c = remote(here, here, y_send.at[slot, i], y_recv.at[slot, i], y_peer)
        c.start()
        ways[kind, l, "y", i] = c
        unsent.append(c)

    def share_y(kind, l, part=0, parts=1):
        if (kind, l) in SHARED_Y:
            for i in range(part * (n - 1) // parts, (part + 1) * (n - 1) // parts):
                share_one(kind, l, i)

    def share_own(kind, l):
        if (kind, l) in SHARED_Y:
            for i in range(groups - 1):
                share_one(kind, l, i)

    def share_across(kind, l):
        if (kind, l) in SHARED_Y:
            for i in range(groups - 1, n - 1):
                share_one(kind, l, i)

    def take_y(kind, l):
        if (kind, l) in SHARED_Y:
            slot = (kinds[kind][0] - 2) * LAYERS + l
            for i in range(n - 1):
                ways[kind, l, "y", i].wait_recv()
                here = block(kind, l, source_of(kind, l, i), lax.rem(tensor + 2, 4))
                c = remote(here, here, d_send.at[slot, i], d_recv.at[slot, i], core_peer)
                c.start()
                unsent.append(c)
                missing[kind, l].append(c.wait_recv)

    def complete(kind, l):
        for wait in missing.pop((kind, l)):
            wait()
        if (kind, l) in leaving:
            settle_slices(kind, l)

    slices = {
        "normed": (0, slices_out, normed_all, True),
        "grad_att": (1, slices_out, grad_att_all, True),
        "gains": (2, gains_out, gains_all, False),
    }

    slice_parts = 4 if piece % 32 == 0 else 2
    slice_rows = piece // slice_parts
    slice_mine = tensor if slice_parts == 4 else core

    def sliced(kind, l, index, owner=None):
        everywhere = slices[kind][2]
        if slices[kind][3]:
            at = slice_mine if owner is None else owner
            rows = pl.ds(pl.multiple_of(at * slice_rows, 8), slice_rows)
            return everywhere.at[l, index, rows]
        return everywhere.at[l, index]

    def sliced_own(kind, slot, index, whole=False):
        own = slices[kind][1]
        if not slices[kind][3]:
            return own.at[slot, index]
        if whole:
            return own.at[slot, pl.ds(pl.multiple_of(index * piece, 8), piece)]
        first = pl.multiple_of(index * piece + slice_mine * slice_rows, 8)
        return own.at[slot, pl.ds(first, slice_rows)]

    def send_slices(kind, l):
        b, own, everywhere, halves = slices[kind]
        slot = b * LAYERS + l
        held_at = LAYERS - 1 - l if kind == "grad_att" else l
        sent = []
        for k in range(1, n):
            to = lax.rem(dp + k, n)
            c = remote(
                sliced_own(kind, held_at, to),
                sliced(kind, l, dp),
                a_send.at[slot, k],
                a_recv.at[slot, k],
                (to, tensor),
            )
            c.start()
            ways[kind, l, k] = c
            sent.append(c.wait_send)
        c = pltpu.make_async_copy(
            sliced_own(kind, held_at, dp, True), everywhere.at[l, dp], local.at[5 * LAYERS + slot]
        )
        c.start()
        missing[kind, l] = []
        leaving[kind, l] = sent + [c.wait]

    def settle_slices(kind, l):
        for wait in leaving.pop((kind, l)):
            wait()

    def take_slices(kind, l):
        b, _, everywhere, divided = slices[kind]
        slot = b * LAYERS + l
        for k in range(1, n):
            ways[kind, l, k].wait_recv()
            if divided:
                here = sliced(kind, l, lax.rem(dp + n - k, n))
                c = remote(here, here, b_send.at[slot, k], b_recv.at[slot, k], core_peer)
                c.start()
                unsent.append(c)
                missing[kind, l].append(c.wait_recv)
                if slice_parts == 4:
                    c = remote(here, here, e_send.at[slot, k], e_recv.at[slot, k], y_peer)
                    c.start()
                    unsent.append(c)
                    ways[kind, l, "y", k] = c

    def take_slices_y(kind, l):
        slot = slices[kind][0] * LAYERS + l
        if slice_parts == 4:
            for k in range(1, n):
                ways[kind, l, "y", k].wait_recv()
                here = sliced(kind, l, lax.rem(dp + n - k, n), lax.rem(tensor + 2, 4))
                c = remote(here, here, f_send.at[slot, k], f_recv.at[slot, k], core_peer)
                c.start()
                unsent.append(c)
                missing[kind, l].append(c.wait_recv)

    def turn_over(dst, src):
        for t in range(width // 128):
            at = slice(t * 128, (t + 1) * 128)
            dst[at, :] = jnp.transpose(src[:, at])

    def cut(dst, l, src):
        for t in range(n):
            dst[l, t] = src[:, t * piece : (t + 1) * piece]

    def tensor_sum(j, tile, base, dest, meanwhile):
        def copy(stage, k, src, dst, peer):
            return remote(src, dst, sum_send.at[j, stage, k], sum_recv.at[j, stage, k], peer)

        def at(k):
            return pl.ds(pl.multiple_of(k * TILE, 128), TILE)

        def mine(k):
            return columns(core * side_width + k * TILE, TILE)

        def other(k):
            return columns((1 - core) * side_width + k * TILE, TILE)

        def first(k):
            return copy(0, k, part.at[:, at(k)], from_core.at[j % 2, :, at(k)], core_peer)

        def second(k):
            return copy(1, k, half.at[:, at(k)], from_y.at[j % 2, :, at(k)], y_peer)

        def third(k):
            return copy(2, k, dest.at[:, mine(k)], dest.at[:, mine(k)], core_peer)

        def begin(k):
            part[:, at(k)] = tile(other(k))
            first(k).start()

        def middle(k):
            own = tile(mine(k))
            first(k).wait_recv()
            half[:, at(k)] = own + from_core[j % 2, :, at(k)]
            second(k).start()

        def finish(k):
            second(k).wait_recv()
            total = half[:, at(k)] + from_y[j % 2, :, at(k)]
            if base is not None:
                total = base[:, mine(k)] + total
            dest[:, mine(k)] = total
            third(k).start()

        def settle(k):
            third(k).wait_recv()
            first(k).wait_send()
            second(k).wait_send()
            third(k).wait_send()

        each(chunks, begin)
        each(chunks, middle)
        meanwhile()
        each(chunks, finish)
        each(chunks, settle)

    def inverse_rms(values):
        return lax.rsqrt(jnp.mean(values * values, axis=-1, keepdims=True) + epsilon)

    def normalize(src, gain, l, out, out_wide):
        def rows_of(i):
            rows = pl.ds(pl.multiple_of(i * ROWS, ROWS), ROWS)
            values = src[rows, :]
            normed = (values * inverse_rms(values) * gain[l : l + 1, :]).astype(low)
            out[rows, :] = normed
            out_wide[rows, :] = normed.astype(full)

        each(length // ROWS, rows_of)

    def norm_backward(grad, values_ref, gain, l, row, before, out, out_low, out_wide):
        def rows_of(i, total):
            rows = pl.ds(pl.multiple_of(i * ROWS, ROWS), ROWS)
            values = values_ref[rows, :]
            grad_normed = grad[rows, :]
            inverse = inverse_rms(values)
            normalized = values * inverse
            term = grad_normed * normalized
            total = total + term[:8] + term[8:]
            scaled = grad_normed * gain[l : l + 1, :]
            back = inverse * (
                scaled - normalized * jnp.mean(scaled * normalized, axis=-1, keepdims=True)
            )
            after = before[rows, :] + back
            out[rows, :] = after
            if out_low is not None:
                after_low = after.astype(low)
                out_low[rows, :] = after_low
                out_wide[rows, :] = after_low.astype(full)
            return total

        total = lax.fori_loop(0, length // ROWS, rows_of, jnp.zeros((8, width), full))
        gain_rows[row : row + 1, :] = jnp.sum(total, axis=0, keepdims=True)

    def turned(values, direction):
        u, w = values[:turn], values[turn:]
        c, s = cosine[...], sine[...]
        return jnp.concatenate([u * c - direction * w * s, w * c + direction * u * s], axis=0)

    def head(ref, l, h):
        return ref[l, h * HD : (h + 1) * HD, :]

    def scores_t(l, h):
        raw = tn(head(key_t, l, h // share), head(query_t, l, h)) * scale
        return jnp.where(allowed[...] > 0.5, raw, masked_score)

    def steps(*calls):
        def run():
            for call, *what in calls:
                call(*what)

        return run

    def attend(l):
        for i in range(3):
            loads[l, i].wait()
        source = normed_low[...]
        for ref, dst, count, rope in (
            (v_query, query_t, heads, True),
            (v_key, key_t, kv_heads, True),
            (v_value, value_t, kv_heads, False),
        ):
            projected = jnp.transpose(nn(source, ref[l])) if ref is v_query else nt(ref[l], source)
            for h in range(count):
                values = projected[h * HD : (h + 1) * HD]
                values = turned(values, 1.0) if rope else values
                dst[l, h * HD : (h + 1) * HD, :] = values.astype(low)
        for h in range(heads):
            scores = scores_t(l, h)
            row_max = jnp.max(scores, axis=0, keepdims=True)
            exponent = jnp.exp(scores - row_max)
            row_total = jnp.sum(exponent, axis=0, keepdims=True)
            probabilities = (exponent / row_total).astype(low)
            logsum[l, h : h + 1, :] = row_max + jnp.log(row_total)
            mixed = nn(head(value_t, l, h // share), probabilities)
            mixed_t[l, h * HD : (h + 1) * HD, :] = mixed.astype(low).astype(full)
        mixed = jnp.transpose(mixed_t[l])
        mixed_out[l] = mixed
        left_low[:, : heads * HD] = mixed.astype(low)

    def attention_back(l):
        grad_mixed_t = jnp.transpose(nt(normed_low[...], v_output[l]).astype(low).astype(full))
        for g in range(kv_heads):
            grad_value = jnp.zeros((HD, length), full)
            grad_key = jnp.zeros((HD, length), full)
            for h in range(g * share, (g + 1) * share):
                grad_mixed = grad_mixed_t[h * HD : (h + 1) * HD]
                grad_mixed_low = grad_mixed.astype(low)
                again = jnp.exp(scores_t(l, h) - logsum[l, h : h + 1, :])
                grad_value += nt(grad_mixed_low, again.astype(low))
                grad_probs = tn(head(value_t, l, g), grad_mixed_low)
                row_dot = jnp.sum(grad_mixed * head(mixed_t, l, h), axis=0, keepdims=True)
                grad_scores = (again * (grad_probs - row_dot) * scale).astype(low)
                grad_query = nn(head(key_t, l, g), grad_scores)
                grad_key += nt(head(query_t, l, h), grad_scores)
                wide[h * HD : (h + 1) * HD, :] = turned(grad_query, -1.0).astype(low).astype(full)
            at = (heads + g) * HD
            wide[at : at + HD, :] = turned(grad_key, -1.0).astype(low).astype(full)
            at = (heads + kv_heads + g) * HD
            wide[at : at + HD, :] = grad_value.astype(low).astype(full)
        rows = jnp.transpose(wide[...])
        qkv_out[l] = rows
        left_low[:, : rows.shape[1]] = rows.astype(low)

    step = hidden_units // 2
    nothing = lambda: None

    def turn_normed(l):
        turn_over(slices_out.at[l], normed_two_out.at[l])
        send_slices("normed", l)

    def turn_grad_att(l):
        settle_slices("normed", LAYERS - 1 - l)
        turn_over(slices_out.at[LAYERS - 1 - l], part_wide)
        send_slices("grad_att", l)

    def attention_layer(l, meanwhile):
        normalize(stream.at[2 * l], attn_gain, l, normed_low, normed_two_out.at[l])
        attend(l)
        send_own("mixed", l)
        loads[l, 3].wait()
        tensor_sum(
            2 * l,
            lambda at: nn(left_low[:, : heads * HD], v_output[l, :, at]),
            stream.at[2 * l],
            stream.at[2 * l + 1],
            steps((turn_normed, l), (meanwhile,)),
        )

    def mlp_layer(l, meanwhile):
        normalize(stream.at[2 * l + 1], mlp_gain, l, normed_low, normed_two_out.at[l])
        send_own("normed_two", l)
        loads[l, 4].wait()
        loads[l, 5].wait()

        def units(i):
            at = columns(i * TILE, TILE)
            source = normed_low[...]
            gate = nn(source, v_gate[l, :, at])
            up = nn(source, v_up[l, :, at])
            gate_pre[l, :, at] = gate
            up_pre[l, :, at] = up
            left_low[:, at] = (gate * jax.nn.sigmoid(gate) * up).astype(low)

        each(hidden_units // TILE, units)
        loads[l, 6].wait()
        tensor_sum(
            2 * l + 1,
            lambda at: nn(left_low[...], v_down[l, :, at]),
            stream.at[2 * l + 1],
            stream.at[2 * l + 2],
            meanwhile,
        )

    def mlp_back(l, meanwhile):
        def units(i):
            at = columns(i * TILE, TILE)
            grad_act = nt(normed_low[...], v_down[l, at, :])
            left, right, _ = mlp_grads(gate_pre[l, :, at], up_pre[l, :, at], grad_act)
            left_low[:, at] = left
            right_low[:, at] = right

        each(hidden_units // TILE, units)
        j = 2 * LAYERS + 2 * (LAYERS - 1 - l)
        tensor_sum(
            j,
            lambda at: nt(left_low[...], v_gate[l, at, :]) + nt(right_low[...], v_up[l, at, :]),
            None,
            grads.at[j % 2],
            meanwhile,
        )
        norm_backward(
            grads.at[j % 2],
            stream.at[2 * l + 1],
            mlp_gain,
            l,
            LAYERS + l,
            upstream,
            upstream,
            normed_low,
            part_wide,
        )

    part_wide = grads.at[2]

    def attention_layer_back(l, meanwhile):
        attention_back(l)
        send_own("query", l)
        if l == 0:
            send_own("keyval", l)
        j = 2 * LAYERS + 2 * (LAYERS - 1 - l) + 1
        q_end, k_end = heads * HD, (heads + kv_heads) * HD
        v_end = (heads + 2 * kv_heads) * HD
        tensor_sum(
            j,
            lambda at: nt(left_low[:, :q_end], v_query[l, at, :])
            + nn(left_low[:, q_end:k_end], v_key[l, :, at])
            + nn(left_low[:, k_end:v_end], v_value[l, :, at]),
            None,
            grads.at[j % 2],
            steps((turn_grad_att, l), (meanwhile,)),
        )
        last = l == 0
        norm_backward(
            grads.at[j % 2],
            stream.at[2 * l],
            attn_gain,
            l,
            l,
            upstream,
            upstream,
            None if last else normed_low,
            None if last else g_out.at[l - 1],
        )

    window = cut_a.shape[0]
    start = jnp.minimum(dp * piece // 128 * 128, width - window)
    offset = pl.multiple_of(dp * piece - start, 8)

    def stream_tokens(first, count, copies, body):
        def go(i, slot):
            for c in copies(i, slot):
                c.start()

        go(first, 0)

        def step(i):
            slot = lax.rem(i, 2)
            for c in copies(first + i, slot):
                c.wait()

            @pl.when(i + 1 < count)
            def _():
                go(first + i + 1, 1 - slot)

            body(slot)

        each(count, step)

    def mlp_gradients(l, share=0, shares=1):
        def copies(i, slot):
            rows = pl.ds(pl.multiple_of(i * TOKENS, 8), TOKENS)
            return (
                pltpu.make_async_copy(
                    normed_two_all.at[l, rows], token_a.at[slot], fetch.at[0, slot]
                ),
                pltpu.make_async_copy(g_all.at[l, rows], token_b.at[slot], fetch.at[1, slot]),
            )

        if share == 0:
            sum_g[...] = jnp.zeros_like(sum_g)
            sum_u[...] = jnp.zeros_like(sum_u)
            sum_d[...] = jnp.zeros_like(sum_d)

        def body(slot):
            low_a[...] = token_a[slot].astype(low)
            low_b[...] = token_b[slot].astype(low)
            cut_a[...] = jnp.transpose(token_a[slot, :, columns(start, window)]).astype(low)
            cut_b[...] = jnp.transpose(token_b[slot, :, columns(start, window)]).astype(low)

            def units(i):
                at = columns(i * UNITS, UNITS)
                gate = nn(low_a[...], v_gate[l, :, at])
                up = nn(low_a[...], v_up[l, :, at])
                grad_act = nt(low_b[...], v_down[l, at, :])
                left, right, activated = mlp_grads(gate, up, grad_act)
                sum_g[:, at] += nn(cut_a[...], left)
                sum_u[:, at] += nn(cut_a[...], right)
                sum_d[:, at] += nn(cut_b[...], activated)

            each(hidden_units // UNITS, units)

        count = n * length // TOKENS // shares
        stream_tokens(share * count, count, copies, body)
        if share < shares - 1:
            return
        outs = [
            pltpu.make_async_copy(src.at[pl.ds(offset, piece)], dst.at[l], edge.at[4 + i])
            for i, (src, dst) in enumerate(((sum_g, grad_g), (sum_u, grad_u), (sum_d, grad_d)))
        ]
        for c in outs:
            c.start()
        for c in outs:
            c.wait()

    def attention_gradients(l):
        blocks = TOKENS // length

        def copies(i, slot):
            rows = pl.ds(pl.multiple_of(i * TOKENS, 8), TOKENS)
            return (
                pltpu.make_async_copy(
                    query_all.at[l, rows],
                    state_qkv.at[slot, :, spans["query"]],
                    fetch.at[2, slot],
                ),
                pltpu.make_async_copy(
                    keyval_all.at[l, rows],
                    state_qkv.at[slot, :, spans["keyval"]],
                    fetch.at[4 + 2 * blocks, slot],
                ),
                pltpu.make_async_copy(
                    mixed_all.at[l, rows], state_mixed.at[slot], fetch.at[3, slot]
                ),
            ) + tuple(
                pltpu.make_async_copy(
                    src.at[l, i * blocks + b],
                    dst.at[slot, :, pl.ds(b * length, length)],
                    fetch.at[at + b, slot],
                )
                for src, dst, at in ((normed_all, state_a, 4), (grad_att_all, state_b, 4 + blocks))
                for b in range(blocks)
            )

        for ref in (sum_q, sum_k, sum_v, sum_o):
            ref[...] = jnp.zeros_like(ref)
        q_end, k_end = heads * HD, (heads + kv_heads) * HD

        def body(slot):
            normed = state_a[slot].astype(low)
            qkv = state_qkv[slot].astype(low)
            sum_q[...] += nn(normed, qkv[:, :q_end])
            sum_k[...] += nn(normed, qkv[:, q_end:k_end])
            sum_v[...] += nn(normed, qkv[:, k_end:])
            sum_o[...] += nn(state_b[slot].astype(low), state_mixed[slot].astype(low))

        stream_tokens(0, n * length // TOKENS, copies, body)
        outs = [
            pltpu.make_async_copy(src, dst.at[l], edge.at[7 + i])
            for i, (src, dst) in enumerate(
                ((sum_q, grad_q), (sum_k, grad_k), (sum_v, grad_v), (sum_o, grad_o))
            )
        ]
        for c in outs:
            c.start()
        for c in outs:
            c.wait()

    for c in arriving:
        c.wait()
    g_out[LAYERS - 1] = upstream[...].astype(low).astype(full)
    send_own("g", LAYERS - 1)
    gain_rows[...] = jnp.zeros_like(gain_rows)

    attention_layer(0, nothing)
    mlp_layer(
        0,
        steps(
            (pass_on, "g", 1),
            (take_slices, "normed", 0),
        ),
    )
    attention_layer(
        1,
        steps(
            (pass_on, "mixed", 0),
            (take_across, "g", 1),
            (share_y, "g", 1, 0, 3),
        ),
    )
    mlp_layer(
        1,
        steps(
            (pass_on, "normed_two", 0),
            (take_across, "mixed", 0),
            (share_y, "g", 1, 1, 3),
        ),
    )
    going = [pltpu.make_async_copy(stream.at[2 * LAYERS], hidden_out, edge.at[2])]
    going[0].start()
    normed_low[...] = g_out[LAYERS - 1].astype(low)
    mlp_back(
        1,
        steps(
            (take_slices, "normed", 1),
            (pass_on, "mixed", 1),
            (take_across, "normed_two", 0),
            (share_y, "g", 1, 2, 3),
        ),
    )
    attention_layer_back(
        1,
        steps(
            (pass_on, "normed_two", 1),
            (take_across, "mixed", 1),
            (share_y, "normed_two", 0, 0, 3),
        ),
    )
    send_own("g", 0)
    send_own("keyval", 1)
    mlp_back(
        0,
        steps(
            (take_slices, "grad_att", 1),
            (pass_on, "query", 1),
            (share_y, "normed_two", 0, 1, 3),
            (take_y, "g", 1),
            (take_slices_y, "normed", 0),
        ),
    )
    attention_layer_back(
        0,
        steps(
            (pass_on, "g", 0),
            (share_own, "g", 0),
            (take_across, "normed_two", 1),
            (share_y, "normed_two", 0, 2, 3),
            (complete, "normed_two", 1),
            (complete, "g", 1),
            (mlp_gradients, 1, 0, 4),
        ),
    )
    going.append(pltpu.make_async_copy(upstream, grad_input, edge.at[3]))
    going[1].start()
    cut(gains_out, 0, gain_rows)
    send_slices("gains", 0)
    for call, *what in (
        (pass_on, "keyval", 1),
        (take_across, "g", 0),
        (share_across, "g", 0),
        (take_slices_y, "normed", 1),
        (take_slices_y, "grad_att", 1),
        (take_y, "normed_two", 0),
        (take_across, "query", 1),
        (mlp_gradients, 1, 1, 4),
        (take_slices, "grad_att", 0),
        (pass_part, "query", 0, 0, 3),
        (mlp_gradients, 1, 2, 4),
        (pass_part, "query", 0, 1, 3),
        (pass_part, "query", 0, 2, 3),
        (mlp_gradients, 1, 3, 4),
        (pass_part, "keyval", 0, 0, 3),
        (take_across, "keyval", 1),
        (take_y, "g", 0),
        (pass_part, "keyval", 0, 1, 3),
        (complete, "normed_two", 0),
        (complete, "g", 0),
        (mlp_gradients, 0, 0, 4),
        (pass_part, "keyval", 0, 2, 3),
        (take_across, "query", 0),
        (mlp_gradients, 0, 1, 4),
        (mlp_gradients, 0, 2, 4),
        (mlp_gradients, 0, 3, 4),
        (complete, "query", 1),
        (complete, "keyval", 1),
        (complete, "mixed", 1),
        (complete, "normed", 1),
        (complete, "grad_att", 1),
        (attention_gradients, 1),
        (take_across, "keyval", 0),
        (take_slices_y, "grad_att", 0),
        (take_slices, "gains", 0),
        (complete, "gains", 0),
        (complete, "query", 0),
        (complete, "keyval", 0),
        (complete, "mixed", 0),
        (complete, "normed", 0),
        (complete, "grad_att", 0),
        (attention_gradients, 0),
    ):
        call(*what)
    assert not missing
    for c in unsent:
        c.wait_send()
    for condition, make in conditional:

        @pl.when(condition)
        def _():
            make().wait_send()

    for key in list(leaving):
        settle_slices(*key)
    for c in going:
        c.wait()


def layers(n, hidden_in, cotangent, cosine, sine, allowed, attn_gain, mlp_gain, weights):
    length, width = hidden_in.shape
    w_query, w_key, w_value, w_output, w_gate, w_up, w_down = weights
    q_width, kv_width, hidden_units = w_query.shape[2], w_key.shape[1], w_gate.shape[2]
    qkv_width = q_width + 2 * kv_width
    piece = width // n
    f32 = lambda *shape: jax.ShapeDtypeStruct(shape, full)
    out_shape = [
        f32(length, width),
        f32(length, width),
        f32(LAYERS, piece, q_width),
        f32(LAYERS, piece, kv_width),
        f32(LAYERS, piece, kv_width),
        f32(LAYERS, piece, q_width),
        f32(LAYERS, piece, hidden_units),
        f32(LAYERS, piece, hidden_units),
        f32(LAYERS, piece, hidden_units),
        f32(LAYERS, n * length, q_width),
        f32(LAYERS, n * length, q_width),
        f32(LAYERS, n * length, 2 * kv_width),
        f32(LAYERS, n * length, width),
        f32(LAYERS, n * length, width),
        f32(LAYERS, n, piece, length),
        f32(LAYERS, n, piece, length),
        f32(1, n, 8, piece),
    ]
    vmem = pl.BlockSpec(memory_space=pltpu.VMEM)
    anywhere = pl.BlockSpec(memory_space=pl.ANY)
    dma = pltpu.SemaphoreType.DMA
    keep = lambda dtype, *shape: pltpu.VMEM(shape, dtype)
    sums = 4 * LAYERS
    chunks = width // 2 // TILE
    window = pl.cdiv(piece + 128 - math.gcd(piece, 128), 128) * 128
    return pl.pallas_call(
        functools.partial(layers_kernel, n),
        out_shape=out_shape,
        in_specs=[anywhere] * 2 + [vmem] * 5 + [anywhere] * 7,
        out_specs=[anywhere] * 17,
        scratch_shapes=[keep(low, *w.shape) for w in weights]
        + [
            keep(full, 2 * LAYERS + 1, length, width),
            keep(full, 3, length, width),
            keep(full, length, width),
            keep(low, length, width),
            keep(low, length, hidden_units),
            keep(low, length, hidden_units),
            keep(full, LAYERS, length, hidden_units),
            keep(full, LAYERS, length, hidden_units),
            keep(low, LAYERS, q_width, length),
            keep(low, LAYERS, kv_width, length),
            keep(low, LAYERS, kv_width, length),
            keep(full, LAYERS, q_width, length),
            keep(full, LAYERS, 8, length),
            keep(full, LAYERS, length, q_width),
            keep(full, LAYERS, length, qkv_width),
            keep(full, LAYERS, length, width),
            keep(full, LAYERS, length, width),
            keep(full, LAYERS, width, length),
            keep(full, 1, n, 8, piece),
            keep(full, 8, width),
            keep(full, qkv_width, length),
            keep(full, length, width // 2),
            keep(full, 2, length, width // 2),
            keep(full, length, width // 2),
            keep(full, 2, length, width // 2),
            keep(full, 2, TOKENS, width),
            keep(full, 2, TOKENS, width),
            keep(low, TOKENS, width),
            keep(low, TOKENS, width),
            keep(low, window, TOKENS),
            keep(low, window, TOKENS),
            keep(full, window, hidden_units),
            keep(full, window, hidden_units),
            keep(full, window, hidden_units),
            keep(full, 2, TOKENS, qkv_width),
            keep(full, 2, TOKENS, q_width),
            keep(full, 2, piece, TOKENS),
            keep(full, 2, piece, TOKENS),
            keep(full, piece, q_width),
            keep(full, piece, kv_width),
            keep(full, piece, kv_width),
            keep(full, piece, q_width),
            dma((LAYERS, 7)),
            dma((sums, 3, chunks)),
            dma((sums, 3, chunks)),
            dma((5 * LAYERS, n // 2)),
            dma((5 * LAYERS,)),
            dma((5 * LAYERS, n // 2)),
            dma((5 * LAYERS, n // 2)),
            dma((5 * LAYERS, n // 2)),
            dma((2 * LAYERS, n)),
            dma((2 * LAYERS, n)),
            dma((3 * LAYERS, n)),
            dma((3 * LAYERS, n)),
            dma((2 * LAYERS, n)),
            dma((2 * LAYERS, n)),
            dma((2 * LAYERS, n)),
            dma((2 * LAYERS, n)),
            dma((2 * LAYERS, n)),
            dma((2 * LAYERS, n)),
            dma((2 * LAYERS, n)),
            dma((2 * LAYERS, n)),
            dma((2 * LAYERS, n)),
            dma((2 * LAYERS, n)),
            dma((8 * LAYERS,)),
            dma((11,)),
            dma((5 + 2 * (TOKENS // length), 2)),
        ],
        compiler_params=pltpu.CompilerParams(
            collective_id=0, has_side_effects=True, vmem_limit_bytes=66_000_000
        ),
        name="layers",
    )(hidden_in, cotangent, cosine, sine, allowed, attn_gain, mlp_gain, *weights)


def shards(
    hidden_in,
    cotangent,
    segment_ids,
    positions,
    w_query,
    w_key,
    w_value,
    w_output,
    w_gate,
    w_up,
    w_down,
    attn_gain,
    mlp_gain,
):
    n = lax.axis_size("dp")
    length = hidden_in.shape[0]
    weights = (
        w_query,
        jnp.swapaxes(w_key, 1, 2),
        jnp.swapaxes(w_value, 1, 2),
        w_output,
        w_gate,
        w_up,
        w_down,
    )
    half_dim = HD // 2
    frequencies = rope_base ** (-(jnp.arange(half_dim).astype(jnp.float32) * 2.0 / HD))
    angles = frequencies[:, None] * positions[0].astype(jnp.float32)[None, :]
    segments = segment_ids[0]
    token_order = jnp.arange(length)
    allowed = (segments[:, None] == segments[None, :]) & (
        token_order[:, None] <= token_order[None, :]
    )
    outs = layers(
        n,
        hidden_in,
        cotangent,
        jnp.cos(angles),
        jnp.sin(angles),
        allowed.astype(jnp.float32),
        attn_gain,
        mlp_gain,
        weights,
    )
    hidden, grad_input, grad_q, grad_k, grad_v, grad_o, grad_g, grad_u, grad_d = outs[:9]
    gain_sums = jnp.sum(outs[-1][0], axis=0)
    return (
        hidden,
        grad_input,
        grad_q,
        grad_k,
        grad_v,
        jnp.swapaxes(grad_o, 1, 2),
        grad_g,
        grad_u,
        jnp.swapaxes(grad_d, 1, 2),
        gain_sums[:LAYERS],
        gain_sums[LAYERS : 2 * LAYERS],
    )


def solution(mesh):
    return jax.shard_map(
        shards,
        mesh=mesh,
        in_specs=(
            P("dp", None),
            P("dp", None),
            P("dp", None),
            P("dp", None),
            P(None, None, "tensor"),
            P(None, None, "tensor"),
            P(None, None, "tensor"),
            P(None, "tensor", None),
            P(None, None, "tensor"),
            P(None, None, "tensor"),
            P(None, "tensor", None),
            P(),
            P(),
        ),
        out_specs=(
            P("dp", None),
            P("dp", None),
            P(None, "dp", "tensor"),
            P(None, "dp", "tensor"),
            P(None, "dp", "tensor"),
            P(None, "tensor", "dp"),
            P(None, "dp", "tensor"),
            P(None, "dp", "tensor"),
            P(None, "tensor", "dp"),
            P(None, "dp"),
            P(None, "dp"),
        ),
        check_vma=False,
    )
```

```python
import functools
import math

import jax
import jax.numpy as jnp
from jax import lax
from jax.experimental import pallas as pl
from jax.experimental.pallas import tpu as pltpu
from jax.sharding import PartitionSpec as P

HD = 96
LAYERS = 2
TILE = 256
UNITS = 512
RELAYED = (
    ("g", 1),
    ("mixed", 0),
    ("normed_two", 0),
    ("mixed", 1),
    ("normed_two", 1),
    ("query", 1),
    ("g", 0),
    ("keyval", 1),
    ("query", 0),
    ("keyval", 0),
)
ROWS = 16
TOKENS = 256
SHARED_Y = (("g", 1), ("normed_two", 0), ("g", 0))
MESH = pl.DeviceIdType.MESH


epsilon = 1e-05
rope_base = 100000.0
masked_score = -1e30
low = jnp.bfloat16
full = jnp.float32


def nn(a, b):
    return lax.dot_general(a, b, (((1,), (0,)), ((), ())), preferred_element_type=full)


def nt(a, b):
    return lax.dot_general(a, b, (((1,), (1,)), ((), ())), preferred_element_type=full)


def tn(a, b):
    return lax.dot_general(a, b, (((0,), (0,)), ((), ())), preferred_element_type=full)


def mlp_grads(gate_pre, up_pre, grad_act):
    sigmoid_gate = jax.nn.sigmoid(gate_pre)
    grad_gate_low = (
        grad_act * up_pre * sigmoid_gate * (1.0 + gate_pre * (1.0 - sigmoid_gate))
    ).astype(low)
    grad_up_low = (grad_act * gate_pre * sigmoid_gate).astype(low)
    activated = (gate_pre * sigmoid_gate * up_pre).astype(low)
    return grad_gate_low, grad_up_low, activated


def each(count, body):
    def step(i, carry):
        body(i)
        return carry

    lax.fori_loop(0, count, step, 0)


def columns(start, size):
    return pl.ds(pl.multiple_of(start, 128), size)


def layers_kernel(n, *refs):
    (
        hidden_in,
        cotangent,
        cosine,
        sine,
        allowed,
        attn_gain,
        mlp_gain,
        w_query,
        w_key,
        w_value,
        w_output,
        w_gate,
        w_up,
        w_down,
        hidden_out,
        grad_input,
        grad_q,
        grad_k,
        grad_v,
        grad_o,
        grad_g,
        grad_u,
        grad_d,
        mixed_all,
        query_all,
        keyval_all,
        normed_two_all,
        g_all,
        normed_all,
        grad_att_all,
        gains_all,
        v_query,
        v_key,
        v_value,
        v_output,
        v_gate,
        v_up,
        v_down,
        stream,
        grads,
        upstream,
        normed_low,
        left_low,
        right_low,
        gate_pre,
        up_pre,
        query_t,
        key_t,
        value_t,
        mixed_t,
        logsum,
        mixed_out,
        qkv_out,
        normed_two_out,
        g_out,
        slices_out,
        gains_out,
        gain_rows,
        wide,
        part,
        from_core,
        half,
        from_y,
        token_a,
        token_b,
        low_a,
        low_b,
        cut_a,
        cut_b,
        sum_g,
        sum_u,
        sum_d,
        state_qkv,
        state_mixed,
        state_a,
        state_b,
        sum_q,
        sum_k,
        sum_v,
        sum_o,
        w_sem,
        sum_send,
        sum_recv,
        z_send,
        z_down,
        z_recv,
        x_send,
        x_recv,
        c_send,
        c_recv,
        a_send,
        a_recv,
        b_send,
        b_recv,
        y_send,
        y_recv,
        d_send,
        d_recv,
        e_send,
        e_recv,
        f_send,
        f_recv,
        local,
        edge,
        fetch,
    ) = refs
    length, width = hidden_in.shape
    heads = w_query.shape[2] // HD
    kv_heads = w_key.shape[1] // HD
    share = heads // kv_heads
    hidden_units = w_gate.shape[2]
    piece = width // n
    side_width = width // 2
    chunks = side_width // TILE
    turn = HD // 2
    scale = HD ** (-0.5)

    dp = lax.axis_index("dp")
    tensor = lax.axis_index("tensor")
    core = tensor % 2
    side = dp % 2
    group = dp // 2
    groups = n // 2
    core_peer = (dp, tensor + 1 - 2 * core)
    y_peer = (dp, lax.rem(tensor + 2, 4))
    x_peer = (dp + 1 - 2 * side, tensor)

    stored = (w_query, w_key, w_value, w_output, w_gate, w_up, w_down)
    held = (v_query, v_key, v_value, v_output, v_gate, v_up, v_down)
    loads = {}
    for l in range(LAYERS):
        for i, (src, dst) in enumerate(zip(stored, held)):
            loads[l, i] = pltpu.make_async_copy(src.at[l], dst.at[l], w_sem.at[l, i])
            loads[l, i].start()

    arriving = [
        pltpu.make_async_copy(hidden_in, stream.at[0], edge.at[0]),
        pltpu.make_async_copy(cotangent, upstream, edge.at[1]),
    ]
    for c in arriving:
        c.start()

    barrier = pltpu.get_barrier_semaphore()
    greeted = [core_peer, y_peer] + [(lax.rem(dp + k, n), tensor) for k in range(1, n)]
    for peer in greeted:
        pl.semaphore_signal(barrier, inc=1, device_id=peer, device_id_type=MESH)
    pl.semaphore_wait(barrier, len(greeted))

    def remote(src, dst, s, r, peer):
        return pltpu.make_async_remote_copy(
            src_ref=src, dst_ref=dst, send_sem=s, recv_sem=r, device_id=peer, device_id_type=MESH
        )

    unsent = []
    missing = {}
    conditional = []
    leaving = {}

    ways = {}
    kinds = {
        "mixed": (0, mixed_out, mixed_all, False),
        "query": (1, qkv_out, query_all, False),
        "normed_two": (2, normed_two_out, normed_two_all, True),
        "g": (3, g_out, g_all, True),
        "keyval": (4, qkv_out, keyval_all, False),
    }
    spans = {"query": slice(0, heads * HD), "keyval": slice(heads * HD, qkv_out.shape[2])}

    quarter_width = width // 4

    def block(kind, l, index, owner=None):
        _, _, everywhere, shared = kinds[kind]
        rows = pl.ds(pl.multiple_of(index * length, 8), length)
        if (kind, l) in SHARED_Y:
            at = tensor if owner is None else owner
            return everywhere.at[l, rows, columns(at * quarter_width, quarter_width)]
        if shared:
            return everywhere.at[l, rows, columns(core * side_width, side_width)]
        return everywhere.at[l, rows]

    def own_of(kind, l):
        own = kinds[kind][1]
        return own.at[l, :, spans[kind]] if kind in spans else own.at[l]

    def send_own(kind, l):
        a, own, everywhere, shared = kinds[kind]
        slot = a * LAYERS + l
        if (kind, l) in SHARED_Y:
            mine = own.at[l, :, columns(tensor * quarter_width, quarter_width)]
        elif shared:
            mine = own.at[l, :, columns(core * side_width, side_width)]
        else:
            mine = own_of(kind, l)
        relayed = (kind, l) in RELAYED
        if relayed:
            send_if(
                group < groups - 1,
                lambda: remote(
                    mine,
                    block(kind, l, dp),
                    z_send.at[slot, 0],
                    z_recv.at[slot, 1],
                    ((group + 1) * 2 + side, tensor),
                ),
            )
            send_if(
                group > 0,
                lambda: remote(
                    mine,
                    block(kind, l, dp),
                    z_down.at[slot],
                    z_recv.at[slot, groups - 1],
                    ((group - 1) * 2 + side, tensor),
                ),
            )
        for k in range(1 if relayed else groups):
            if k == 0:
                c = remote(
                    mine, block(kind, l, dp), x_send.at[slot, 0], x_recv.at[slot, 0], x_peer
                )
            else:
                peer = (lax.rem(group + k, groups) * 2 + side, tensor)
                c = remote(
                    mine, block(kind, l, dp), z_send.at[slot, k], z_recv.at[slot, k], peer
                )
            c.start()
            ways[kind, l, "own", k] = c
            unsent.append(c)
        rows = pl.ds(pl.multiple_of(dp * length, 8), length)
        c = pltpu.make_async_copy(own_of(kind, l), everywhere.at[l, rows], local.at[slot])
        c.start()
        missing.setdefault((kind, l), []).append(c.wait)

    def send_if(condition, make):
        @pl.when(condition)
        def _():
            make().start()

        conditional.append((condition, make))

    both = jnp.minimum(group, groups - 1 - group)
    longer_below = (group > groups - 1 - group).astype(jnp.int32)

    def ranked(j):
        single = (j >= 2 * both).astype(jnp.int32)
        below = single * longer_below + (1 - single) * (1 - j % 2)
        distance = single * (j - both + 1) + (1 - single) * (j // 2 + 1)
        return below, distance

    def behind(kind, l, j):
        if (kind, l) in RELAYED:
            below, distance = ranked(j)
            return below * distance + (1 - below) * (groups - distance)
        return j + 1

    def source_of(kind, l, i):
        across = i >= groups - 1
        j = i - groups if across else i
        steps_back = 0 if j < 0 else behind(kind, l, j)
        return lax.rem(group + groups - steps_back, groups) * 2 + (1 - side if across else side)

    def to_core(kind, l, i):
        a = kinds[kind][0]
        if kinds[kind][3]:
            slot = (a - 2) * LAYERS + l
            here = block(kind, l, source_of(kind, l, i))
            c = remote(here, here, c_send.at[slot, i], c_recv.at[slot, i], core_peer)
            c.start()
            unsent.append(c)
            missing[kind, l].append(c.wait_recv)

    def pass_one(kind, l, k):
        slot = kinds[kind][0] * LAYERS + l
        here = block(kind, l, source_of(kind, l, k - 1))
        if (kind, l) in RELAYED:
            below, _ = ranked(k - 1)
            steps_back = behind(kind, l, k - 1)
            remote(
                here, here, z_send.at[slot, k], z_recv.at[slot, steps_back], x_peer
            ).wait_recv()
            send_if(
                jnp.logical_and(below == 1, group < groups - 1),
                lambda: remote(
                    here,
                    here,
                    z_send.at[slot, k],
                    z_recv.at[slot, steps_back + 1],
                    ((group + 1) * 2 + side, tensor),
                ),
            )
            send_if(
                jnp.logical_and(below == 0, group > 0),
                lambda: remote(
                    here,
                    here,
                    z_send.at[slot, k],
                    z_recv.at[slot, steps_back - 1],
                    ((group - 1) * 2 + side, tensor),
                ),
            )
        else:
            ways[kind, l, "own", k].wait_recv()
        c = remote(here, here, x_send.at[slot, k], x_recv.at[slot, k], x_peer)
        c.start()
        ways[kind, l, "x", k] = c
        unsent.append(c)
        to_core(kind, l, k - 1)

    def pass_part(kind, l, part, parts):
        for k in range(1 + part * (groups - 1) // parts, 1 + (part + 1) * (groups - 1) // parts):
            pass_one(kind, l, k)

    def pass_on(kind, l):
        pass_part(kind, l, 0, 1)

    def take_one(kind, l, k):
        ways[kind, l, "own" if k == 0 else "x", k].wait_recv()
        to_core(kind, l, groups - 1 + k)

    def take_across(kind, l):
        for k in range(groups):
            take_one(kind, l, k)

    def share_one(kind, l, i):
        slot = (kinds[kind][0] - 2) * LAYERS + l
        here = block(kind, l, source_of(kind, l, i))
        c = remote(here, here, y_send.at[slot, i], y_recv.at[slot, i], y_peer)
        c.start()
        ways[kind, l, "y", i] = c
        unsent.append(c)

    def share_y(kind, l, part=0, parts=1):
        if (kind, l) in SHARED_Y:
            for i in range(part * (n - 1) // parts, (part + 1) * (n - 1) // parts):
                share_one(kind, l, i)

    def share_own(kind, l):
        if (kind, l) in SHARED_Y:
            for i in range(groups - 1):
                share_one(kind, l, i)

    def share_across(kind, l):
        if (kind, l) in SHARED_Y:
            for i in range(groups - 1, n - 1):
                share_one(kind, l, i)

    def take_y(kind, l):
        if (kind, l) in SHARED_Y:
            slot = (kinds[kind][0] - 2) * LAYERS + l
            for i in range(n - 1):
                ways[kind, l, "y", i].wait_recv()
                here = block(kind, l, source_of(kind, l, i), lax.rem(tensor + 2, 4))
                c = remote(here, here, d_send.at[slot, i], d_recv.at[slot, i], core_peer)
                c.start()
                unsent.append(c)
                missing[kind, l].append(c.wait_recv)

    def complete(kind, l):
        for wait in missing.pop((kind, l)):
            wait()
        if (kind, l) in leaving:
            settle_slices(kind, l)

    slices = {
        "normed": (0, slices_out, normed_all, True),
        "grad_att": (1, slices_out, grad_att_all, True),
        "gains": (2, gains_out, gains_all, False),
    }

    slice_parts = 4 if piece % 32 == 0 else 2
    slice_rows = piece // slice_parts
    slice_mine = tensor if slice_parts == 4 else core

    def sliced(kind, l, index, owner=None):
        everywhere = slices[kind][2]
        if slices[kind][3]:
            at = slice_mine if owner is None else owner
            rows = pl.ds(pl.multiple_of(at * slice_rows, 8), slice_rows)
            return everywhere.at[l, index, rows]
        return everywhere.at[l, index]

    def sliced_own(kind, slot, index, whole=False):
        own = slices[kind][1]
        if not slices[kind][3]:
            return own.at[slot, index]
        if whole:
            return own.at[slot, pl.ds(pl.multiple_of(index * piece, 8), piece)]
        first = pl.multiple_of(index * piece + slice_mine * slice_rows, 8)
        return own.at[slot, pl.ds(first, slice_rows)]

    def send_slices(kind, l):
        b, own, everywhere, halves = slices[kind]
        slot = b * LAYERS + l
        held_at = LAYERS - 1 - l if kind == "grad_att" else l
        sent = []
        for k in range(1, n):
            to = lax.rem(dp + k, n)
            c = remote(
                sliced_own(kind, held_at, to),
                sliced(kind, l, dp),
                a_send.at[slot, k],
                a_recv.at[slot, k],
                (to, tensor),
            )
            c.start()
            ways[kind, l, k] = c
            sent.append(c.wait_send)
        c = pltpu.make_async_copy(
            sliced_own(kind, held_at, dp, True), everywhere.at[l, dp], local.at[5 * LAYERS + slot]
        )
        c.start()
        missing[kind, l] = []
        leaving[kind, l] = sent + [c.wait]

    def settle_slices(kind, l):
        for wait in leaving.pop((kind, l)):
            wait()

    def take_slices(kind, l):
        b, _, everywhere, divided = slices[kind]
        slot = b * LAYERS + l
        for k in range(1, n):
            ways[kind, l, k].wait_recv()
            if divided:
                here = sliced(kind, l, lax.rem(dp + n - k, n))
                c = remote(here, here, b_send.at[slot, k], b_recv.at[slot, k], core_peer)
                c.start()
                unsent.append(c)
                missing[kind, l].append(c.wait_recv)
                if slice_parts == 4:
                    c = remote(here, here, e_send.at[slot, k], e_recv.at[slot, k], y_peer)
                    c.start()
                    unsent.append(c)
                    ways[kind, l, "y", k] = c

    def take_slices_y(kind, l):
        slot = slices[kind][0] * LAYERS + l
        if slice_parts == 4:
            for k in range(1, n):
                ways[kind, l, "y", k].wait_recv()
                here = sliced(kind, l, lax.rem(dp + n - k, n), lax.rem(tensor + 2, 4))
                c = remote(here, here, f_send.at[slot, k], f_recv.at[slot, k], core_peer)
                c.start()
                unsent.append(c)
                missing[kind, l].append(c.wait_recv)

    def turn_over(dst, src):
        for t in range(width // 128):
            at = slice(t * 128, (t + 1) * 128)
            dst[at, :] = jnp.transpose(src[:, at])

    def cut(dst, l, src):
        for t in range(n):
            dst[l, t] = src[:, t * piece : (t + 1) * piece]

    def tensor_sum(j, tile, base, dest, meanwhile):
        def copy(stage, k, src, dst, peer):
            return remote(src, dst, sum_send.at[j, stage, k], sum_recv.at[j, stage, k], peer)

        def at(k):
            return pl.ds(pl.multiple_of(k * TILE, 128), TILE)

        def mine(k):
            return columns(core * side_width + k * TILE, TILE)

        def other(k):
            return columns((1 - core) * side_width + k * TILE, TILE)

        def first(k):
            return copy(0, k, part.at[:, at(k)], from_core.at[j % 2, :, at(k)], core_peer)

        def second(k):
            return copy(1, k, half.at[:, at(k)], from_y.at[j % 2, :, at(k)], y_peer)

        def third(k):
            return copy(2, k, dest.at[:, mine(k)], dest.at[:, mine(k)], core_peer)

        def begin(k):
            part[:, at(k)] = tile(other(k))
            first(k).start()

        def middle(k):
            own = tile(mine(k))
            first(k).wait_recv()
            half[:, at(k)] = own + from_core[j % 2, :, at(k)]
            second(k).start()

        def finish(k):
            second(k).wait_recv()
            total = half[:, at(k)] + from_y[j % 2, :, at(k)]
            if base is not None:
                total = base[:, mine(k)] + total
            dest[:, mine(k)] = total
            third(k).start()

        def settle(k):
            third(k).wait_recv()
            first(k).wait_send()
            second(k).wait_send()
            third(k).wait_send()

        each(chunks, begin)
        each(chunks, middle)
        meanwhile()
        each(chunks, finish)
        each(chunks, settle)

    def inverse_rms(values):
        return lax.rsqrt(jnp.mean(values * values, axis=-1, keepdims=True) + epsilon)

    def normalize(src, gain, l, out, out_wide):
        def rows_of(i):
            rows = pl.ds(pl.multiple_of(i * ROWS, ROWS), ROWS)
            values = src[rows, :]
            normed = (values * inverse_rms(values) * gain[l : l + 1, :]).astype(low)
            out[rows, :] = normed
            out_wide[rows, :] = normed.astype(full)

        each(length // ROWS, rows_of)

    def norm_backward(grad, values_ref, gain, l, row, before, out, out_low, out_wide):
        def rows_of(i, total):
            rows = pl.ds(pl.multiple_of(i * ROWS, ROWS), ROWS)
            values = values_ref[rows, :]
            grad_normed = grad[rows, :]
            inverse = inverse_rms(values)
            normalized = values * inverse
            term = grad_normed * normalized
            total = total + term[:8] + term[8:]
            scaled = grad_normed * gain[l : l + 1, :]
            back = inverse * (
                scaled - normalized * jnp.mean(scaled * normalized, axis=-1, keepdims=True)
            )
            after = before[rows, :] + back
            out[rows, :] = after
            if out_low is not None:
                after_low = after.astype(low)
                out_low[rows, :] = after_low
                out_wide[rows, :] = after_low.astype(full)
            return total

        total = lax.fori_loop(0, length // ROWS, rows_of, jnp.zeros((8, width), full))
        gain_rows[row : row + 1, :] = jnp.sum(total, axis=0, keepdims=True)

    def turned(values, direction):
        u, w = values[:turn], values[turn:]
        c, s = cosine[...], sine[...]
        return jnp.concatenate([u * c - direction * w * s, w * c + direction * u * s], axis=0)

    def head(ref, l, h):
        return ref[l, h * HD : (h + 1) * HD, :]

    def scores_t(l, h):
        raw = tn(head(key_t, l, h // share), head(query_t, l, h)) * scale
        return jnp.where(allowed[...] > 0.5, raw, masked_score)

    def steps(*calls):
        def run():
            for call, *what in calls:
                call(*what)

        return run

    def attend(l):
        for i in range(3):
            loads[l, i].wait()
        source = normed_low[...]
        for ref, dst, count, rope in (
            (v_query, query_t, heads, True),
            (v_key, key_t, kv_heads, True),
            (v_value, value_t, kv_heads, False),
        ):
            projected = jnp.transpose(nn(source, ref[l])) if ref is v_query else nt(ref[l], source)
            for h in range(count):
                values = projected[h * HD : (h + 1) * HD]
                values = turned(values, 1.0) if rope else values
                dst[l, h * HD : (h + 1) * HD, :] = values.astype(low)
        for h in range(heads):
            scores = scores_t(l, h)
            row_max = jnp.max(scores, axis=0, keepdims=True)
            exponent = jnp.exp(scores - row_max)
            row_total = jnp.sum(exponent, axis=0, keepdims=True)
            probabilities = (exponent / row_total).astype(low)
            logsum[l, h : h + 1, :] = row_max + jnp.log(row_total)
            mixed = nn(head(value_t, l, h // share), probabilities)
            mixed_t[l, h * HD : (h + 1) * HD, :] = mixed.astype(low).astype(full)
        mixed = jnp.transpose(mixed_t[l])
        mixed_out[l] = mixed
        left_low[:, : heads * HD] = mixed.astype(low)

    def attention_back(l):
        grad_mixed_t = jnp.transpose(nt(normed_low[...], v_output[l]).astype(low).astype(full))
        for g in range(kv_heads):
            grad_value = jnp.zeros((HD, length), full)
            grad_key = jnp.zeros((HD, length), full)
            for h in range(g * share, (g + 1) * share):
                grad_mixed = grad_mixed_t[h * HD : (h + 1) * HD]
                grad_mixed_low = grad_mixed.astype(low)
                again = jnp.exp(scores_t(l, h) - logsum[l, h : h + 1, :])
                grad_value += nt(grad_mixed_low, again.astype(low))
                grad_probs = tn(head(value_t, l, g), grad_mixed_low)
                row_dot = jnp.sum(grad_mixed * head(mixed_t, l, h), axis=0, keepdims=True)
                grad_scores = (again * (grad_probs - row_dot) * scale).astype(low)
                grad_query = nn(head(key_t, l, g), grad_scores)
                grad_key += nt(head(query_t, l, h), grad_scores)
                wide[h * HD : (h + 1) * HD, :] = turned(grad_query, -1.0).astype(low).astype(full)
            at = (heads + g) * HD
            wide[at : at + HD, :] = turned(grad_key, -1.0).astype(low).astype(full)
            at = (heads + kv_heads + g) * HD
            wide[at : at + HD, :] = grad_value.astype(low).astype(full)
        rows = jnp.transpose(wide[...])
        qkv_out[l] = rows
        left_low[:, : rows.shape[1]] = rows.astype(low)

    step = hidden_units // 2
    nothing = lambda: None

    def turn_normed(l):
        turn_over(slices_out.at[l], normed_two_out.at[l])
        send_slices("normed", l)

    def turn_grad_att(l):
        settle_slices("normed", LAYERS - 1 - l)
        turn_over(slices_out.at[LAYERS - 1 - l], part_wide)
        send_slices("grad_att", l)

    def attention_layer(l, meanwhile):
        normalize(stream.at[2 * l], attn_gain, l, normed_low, normed_two_out.at[l])
        attend(l)
        send_own("mixed", l)
        loads[l, 3].wait()
        tensor_sum(
            2 * l,
            lambda at: nn(left_low[:, : heads * HD], v_output[l, :, at]),
            stream.at[2 * l],
            stream.at[2 * l + 1],
            steps((turn_normed, l), (meanwhile,)),
        )

    def mlp_layer(l, meanwhile):
        normalize(stream.at[2 * l + 1], mlp_gain, l, normed_low, normed_two_out.at[l])
        send_own("normed_two", l)
        loads[l, 4].wait()
        loads[l, 5].wait()

        def units(i):
            at = columns(i * TILE, TILE)
            source = normed_low[...]
            gate = nn(source, v_gate[l, :, at])
            up = nn(source, v_up[l, :, at])
            gate_pre[l, :, at] = gate
            up_pre[l, :, at] = up
            left_low[:, at] = (gate * jax.nn.sigmoid(gate) * up).astype(low)

        each(hidden_units // TILE, units)
        loads[l, 6].wait()
        tensor_sum(
            2 * l + 1,
            lambda at: nn(left_low[...], v_down[l, :, at]),
            stream.at[2 * l + 1],
            stream.at[2 * l + 2],
            meanwhile,
        )

    def mlp_back(l, meanwhile):
        def units(i):
            at = columns(i * TILE, TILE)
            grad_act = nt(normed_low[...], v_down[l, at, :])
            left, right, _ = mlp_grads(gate_pre[l, :, at], up_pre[l, :, at], grad_act)
            left_low[:, at] = left
            right_low[:, at] = right

        each(hidden_units // TILE, units)
        j = 2 * LAYERS + 2 * (LAYERS - 1 - l)
        tensor_sum(
            j,
            lambda at: nt(left_low[...], v_gate[l, at, :]) + nt(right_low[...], v_up[l, at, :]),
            None,
            grads.at[j % 2],
            meanwhile,
        )
        norm_backward(
            grads.at[j % 2],
            stream.at[2 * l + 1],
            mlp_gain,
            l,
            LAYERS + l,
            upstream,
            upstream,
            normed_low,
            part_wide,
        )

    part_wide = grads.at[2]

    def attention_layer_back(l, meanwhile):
        attention_back(l)
        send_own("query", l)
        if l == 0:
            send_own("keyval", l)
        j = 2 * LAYERS + 2 * (LAYERS - 1 - l) + 1
        q_end, k_end = heads * HD, (heads + kv_heads) * HD
        v_end = (heads + 2 * kv_heads) * HD
        tensor_sum(
            j,
            lambda at: nt(left_low[:, :q_end], v_query[l, at, :])
            + nn(left_low[:, q_end:k_end], v_key[l, :, at])
            + nn(left_low[:, k_end:v_end], v_value[l, :, at]),
            None,
            grads.at[j % 2],
            steps((turn_grad_att, l), (meanwhile,)),
        )
        last = l == 0
        norm_backward(
            grads.at[j % 2],
            stream.at[2 * l],
            attn_gain,
            l,
            l,
            upstream,
            upstream,
            None if last else normed_low,
            None if last else g_out.at[l - 1],
        )

    window = cut_a.shape[0]
    start = jnp.minimum(dp * piece // 128 * 128, width - window)
    offset = pl.multiple_of(dp * piece - start, 8)

    def stream_tokens(first, count, copies, body):
        def go(i, slot):
            for c in copies(i, slot):
                c.start()

        go(first, 0)

        def step(i):
            slot = lax.rem(i, 2)
            for c in copies(first + i, slot):
                c.wait()

            @pl.when(i + 1 < count)
            def _():
                go(first + i + 1, 1 - slot)

            body(slot)

        each(count, step)

    def mlp_gradients(l, share=0, shares=1):
        def copies(i, slot):
            rows = pl.ds(pl.multiple_of(i * TOKENS, 8), TOKENS)
            return (
                pltpu.make_async_copy(
                    normed_two_all.at[l, rows], token_a.at[slot], fetch.at[0, slot]
                ),
                pltpu.make_async_copy(g_all.at[l, rows], token_b.at[slot], fetch.at[1, slot]),
            )

        if share == 0:
            sum_g[...] = jnp.zeros_like(sum_g)
            sum_u[...] = jnp.zeros_like(sum_u)
            sum_d[...] = jnp.zeros_like(sum_d)

        def body(slot):
            low_a[...] = token_a[slot].astype(low)
            low_b[...] = token_b[slot].astype(low)
            cut_a[...] = jnp.transpose(token_a[slot, :, columns(start, window)]).astype(low)
            cut_b[...] = jnp.transpose(token_b[slot, :, columns(start, window)]).astype(low)

            def units(i):
                at = columns(i * UNITS, UNITS)
                gate = nn(low_a[...], v_gate[l, :, at])
                up = nn(low_a[...], v_up[l, :, at])
                grad_act = nt(low_b[...], v_down[l, at, :])
                left, right, activated = mlp_grads(gate, up, grad_act)
                sum_g[:, at] += nn(cut_a[...], left)
                sum_u[:, at] += nn(cut_a[...], right)
                sum_d[:, at] += nn(cut_b[...], activated)

            each(hidden_units // UNITS, units)

        count = n * length // TOKENS // shares
        stream_tokens(share * count, count, copies, body)
        if share < shares - 1:
            return
        outs = [
            pltpu.make_async_copy(src.at[pl.ds(offset, piece)], dst.at[l], edge.at[4 + i])
            for i, (src, dst) in enumerate(((sum_g, grad_g), (sum_u, grad_u), (sum_d, grad_d)))
        ]
        for c in outs:
            c.start()
        for c in outs:
            c.wait()

    def attention_gradients(l):
        blocks = TOKENS // length

        def copies(i, slot):
            rows = pl.ds(pl.multiple_of(i * TOKENS, 8), TOKENS)
            return (
                pltpu.make_async_copy(
                    query_all.at[l, rows],
                    state_qkv.at[slot, :, spans["query"]],
                    fetch.at[2, slot],
                ),
                pltpu.make_async_copy(
                    keyval_all.at[l, rows],
                    state_qkv.at[slot, :, spans["keyval"]],
                    fetch.at[4 + 2 * blocks, slot],
                ),
                pltpu.make_async_copy(
                    mixed_all.at[l, rows], state_mixed.at[slot], fetch.at[3, slot]
                ),
            ) + tuple(
                pltpu.make_async_copy(
                    src.at[l, i * blocks + b],
                    dst.at[slot, :, pl.ds(b * length, length)],
                    fetch.at[at + b, slot],
                )
                for src, dst, at in ((normed_all, state_a, 4), (grad_att_all, state_b, 4 + blocks))
                for b in range(blocks)
            )

        for ref in (sum_q, sum_k, sum_v, sum_o):
            ref[...] = jnp.zeros_like(ref)
        q_end, k_end = heads * HD, (heads + kv_heads) * HD

        def body(slot):
            normed = state_a[slot].astype(low)
            qkv = state_qkv[slot].astype(low)
            sum_q[...] += nn(normed, qkv[:, :q_end])
            sum_k[...] += nn(normed, qkv[:, q_end:k_end])
            sum_v[...] += nn(normed, qkv[:, k_end:])
            sum_o[...] += nn(state_b[slot].astype(low), state_mixed[slot].astype(low))

        stream_tokens(0, n * length // TOKENS, copies, body)
        outs = [
            pltpu.make_async_copy(src, dst.at[l], edge.at[7 + i])
            for i, (src, dst) in enumerate(
                ((sum_q, grad_q), (sum_k, grad_k), (sum_v, grad_v), (sum_o, grad_o))
            )
        ]
        for c in outs:
            c.start()
        for c in outs:
            c.wait()

    for c in arriving:
        c.wait()
    g_out[LAYERS - 1] = upstream[...].astype(low).astype(full)
    send_own("g", LAYERS - 1)
    gain_rows[...] = jnp.zeros_like(gain_rows)

    attention_layer(
        0,
        steps(
            (pass_part, "g", 1, 0, 3),
            (pass_part, "g", 1, 1, 3),
        ),
    )
    mlp_layer(
        0,
        steps(
            (pass_part, "g", 1, 2, 3),
            (pass_part, "mixed", 0, 0, 3),
            (pass_part, "mixed", 0, 1, 3),
            (take_slices, "normed", 0),
        ),
    )
    attention_layer(
        1,
        steps(
            (pass_part, "mixed", 0, 2, 3),
            (take_across, "g", 1),
            (share_y, "g", 1, 0, 3),
            (pass_part, "normed_two", 0, 0, 3),
            (pass_part, "normed_two", 0, 1, 3),
        ),
    )
    mlp_layer(
        1,
        steps(
            (pass_part, "normed_two", 0, 2, 3),
            (take_across, "mixed", 0),
            (share_y, "g", 1, 1, 3),
            (take_slices, "normed", 1),
            (pass_part, "mixed", 1, 0, 3),
            (pass_part, "mixed", 1, 1, 3),
        ),
    )
    going = [pltpu.make_async_copy(stream.at[2 * LAYERS], hidden_out, edge.at[2])]
    going[0].start()
    normed_low[...] = g_out[LAYERS - 1].astype(low)
    mlp_back(
        1,
        steps(
            (pass_part, "mixed", 1, 2, 3),
            (take_across, "normed_two", 0),
            (share_y, "g", 1, 2, 3),
            (pass_part, "normed_two", 1, 0, 3),
            (pass_part, "normed_two", 1, 1, 3),
        ),
    )
    attention_layer_back(
        1,
        steps(
            (pass_part, "normed_two", 1, 2, 3),
            (take_across, "mixed", 1),
            (share_y, "normed_two", 0, 0, 3),
            (take_y, "g", 1),
            (take_slices_y, "normed", 0),
        ),
    )
    send_own("g", 0)
    send_own("keyval", 1)
    mlp_back(
        0,
        steps(
            (take_slices, "grad_att", 1),
            (pass_part, "query", 1, 0, 3),
            (pass_part, "query", 1, 1, 3),
            (take_across, "normed_two", 1),
            (share_y, "normed_two", 0, 1, 3),
        ),
    )
    attention_layer_back(
        0,
        steps(
            (pass_part, "query", 1, 2, 3),
            (pass_on, "g", 0),
            (share_own, "g", 0),
            (share_y, "normed_two", 0, 2, 3),
            (complete, "normed_two", 1),
            (complete, "g", 1),
            (mlp_gradients, 1, 0, 4),
        ),
    )
    going.append(pltpu.make_async_copy(upstream, grad_input, edge.at[3]))
    going[1].start()
    cut(gains_out, 0, gain_rows)
    send_slices("gains", 0)
    for call, *what in (
        (pass_on, "keyval", 1),
        (take_across, "g", 0),
        (share_across, "g", 0),
        (take_slices_y, "normed", 1),
        (take_slices_y, "grad_att", 1),
        (take_y, "normed_two", 0),
        (take_across, "query", 1),
        (mlp_gradients, 1, 1, 4),
        (take_slices, "grad_att", 0),
        (pass_part, "query", 0, 0, 3),
        (mlp_gradients, 1, 2, 4),
        (pass_part, "query", 0, 1, 3),
        (pass_part, "query", 0, 2, 3),
        (mlp_gradients, 1, 3, 4),
        (pass_part, "keyval", 0, 0, 3),
        (take_across, "keyval", 1),
        (take_y, "g", 0),
        (pass_part, "keyval", 0, 1, 3),
        (complete, "normed_two", 0),
        (complete, "g", 0),
        (mlp_gradients, 0, 0, 4),
        (pass_part, "keyval", 0, 2, 3),
        (take_across, "query", 0),
        (mlp_gradients, 0, 1, 4),
        (mlp_gradients, 0, 2, 4),
        (mlp_gradients, 0, 3, 4),
        (complete, "query", 1),
        (complete, "keyval", 1),
        (complete, "mixed", 1),
        (complete, "normed", 1),
        (complete, "grad_att", 1),
        (attention_gradients, 1),
        (take_across, "keyval", 0),
        (take_slices_y, "grad_att", 0),
        (take_slices, "gains", 0),
        (complete, "gains", 0),
        (complete, "query", 0),
        (complete, "keyval", 0),
        (complete, "mixed", 0),
        (complete, "normed", 0),
        (complete, "grad_att", 0),
        (attention_gradients, 0),
    ):
        call(*what)
    assert not missing
    for c in unsent:
        c.wait_send()
    for condition, make in conditional:

        @pl.when(condition)
        def _():
            make().wait_send()

    for key in list(leaving):
        settle_slices(*key)
    for c in going:
        c.wait()


def layers(n, hidden_in, cotangent, cosine, sine, allowed, attn_gain, mlp_gain, weights):
    length, width = hidden_in.shape
    w_query, w_key, w_value, w_output, w_gate, w_up, w_down = weights
    q_width, kv_width, hidden_units = w_query.shape[2], w_key.shape[1], w_gate.shape[2]
    qkv_width = q_width + 2 * kv_width
    piece = width // n
    f32 = lambda *shape: jax.ShapeDtypeStruct(shape, full)
    out_shape = [
        f32(length, width),
        f32(length, width),
        f32(LAYERS, piece, q_width),
        f32(LAYERS, piece, kv_width),
        f32(LAYERS, piece, kv_width),
        f32(LAYERS, piece, q_width),
        f32(LAYERS, piece, hidden_units),
        f32(LAYERS, piece, hidden_units),
        f32(LAYERS, piece, hidden_units),
        f32(LAYERS, n * length, q_width),
        f32(LAYERS, n * length, q_width),
        f32(LAYERS, n * length, 2 * kv_width),
        f32(LAYERS, n * length, width),
        f32(LAYERS, n * length, width),
        f32(LAYERS, n, piece, length),
        f32(LAYERS, n, piece, length),
        f32(1, n, 8, piece),
    ]
    vmem = pl.BlockSpec(memory_space=pltpu.VMEM)
    anywhere = pl.BlockSpec(memory_space=pl.ANY)
    dma = pltpu.SemaphoreType.DMA
    keep = lambda dtype, *shape: pltpu.VMEM(shape, dtype)
    sums = 4 * LAYERS
    chunks = width // 2 // TILE
    window = pl.cdiv(piece + 128 - math.gcd(piece, 128), 128) * 128
    return pl.pallas_call(
        functools.partial(layers_kernel, n),
        out_shape=out_shape,
        in_specs=[anywhere] * 2 + [vmem] * 5 + [anywhere] * 7,
        out_specs=[anywhere] * 17,
        scratch_shapes=[keep(low, *w.shape) for w in weights]
        + [
            keep(full, 2 * LAYERS + 1, length, width),
            keep(full, 3, length, width),
            keep(full, length, width),
            keep(low, length, width),
            keep(low, length, hidden_units),
            keep(low, length, hidden_units),
            keep(full, LAYERS, length, hidden_units),
            keep(full, LAYERS, length, hidden_units),
            keep(low, LAYERS, q_width, length),
            keep(low, LAYERS, kv_width, length),
            keep(low, LAYERS, kv_width, length),
            keep(full, LAYERS, q_width, length),
            keep(full, LAYERS, 8, length),
            keep(full, LAYERS, length, q_width),
            keep(full, LAYERS, length, qkv_width),
            keep(full, LAYERS, length, width),
            keep(full, LAYERS, length, width),
            keep(full, LAYERS, width, length),
            keep(full, 1, n, 8, piece),
            keep(full, 8, width),
            keep(full, qkv_width, length),
            keep(full, length, width // 2),
            keep(full, 2, length, width // 2),
            keep(full, length, width // 2),
            keep(full, 2, length, width // 2),
            keep(full, 2, TOKENS, width),
            keep(full, 2, TOKENS, width),
            keep(low, TOKENS, width),
            keep(low, TOKENS, width),
            keep(low, window, TOKENS),
            keep(low, window, TOKENS),
            keep(full, window, hidden_units),
            keep(full, window, hidden_units),
            keep(full, window, hidden_units),
            keep(full, 2, TOKENS, qkv_width),
            keep(full, 2, TOKENS, q_width),
            keep(full, 2, piece, TOKENS),
            keep(full, 2, piece, TOKENS),
            keep(full, piece, q_width),
            keep(full, piece, kv_width),
            keep(full, piece, kv_width),
            keep(full, piece, q_width),
            dma((LAYERS, 7)),
            dma((sums, 3, chunks)),
            dma((sums, 3, chunks)),
            dma((5 * LAYERS, n // 2)),
            dma((5 * LAYERS,)),
            dma((5 * LAYERS, n // 2)),
            dma((5 * LAYERS, n // 2)),
            dma((5 * LAYERS, n // 2)),
            dma((2 * LAYERS, n)),
            dma((2 * LAYERS, n)),
            dma((3 * LAYERS, n)),
            dma((3 * LAYERS, n)),
            dma((2 * LAYERS, n)),
            dma((2 * LAYERS, n)),
            dma((2 * LAYERS, n)),
            dma((2 * LAYERS, n)),
            dma((2 * LAYERS, n)),
            dma((2 * LAYERS, n)),
            dma((2 * LAYERS, n)),
            dma((2 * LAYERS, n)),
            dma((2 * LAYERS, n)),
            dma((2 * LAYERS, n)),
            dma((8 * LAYERS,)),
            dma((11,)),
            dma((5 + 2 * (TOKENS // length), 2)),
        ],
        compiler_params=pltpu.CompilerParams(
            collective_id=0, has_side_effects=True, vmem_limit_bytes=66_000_000
        ),
        name="layers",
    )(hidden_in, cotangent, cosine, sine, allowed, attn_gain, mlp_gain, *weights)


def shards(
    hidden_in,
    cotangent,
    segment_ids,
    positions,
    w_query,
    w_key,
    w_value,
    w_output,
    w_gate,
    w_up,
    w_down,
    attn_gain,
    mlp_gain,
):
    n = lax.axis_size("dp")
    length = hidden_in.shape[0]
    weights = (
        w_query,
        jnp.swapaxes(w_key, 1, 2),
        jnp.swapaxes(w_value, 1, 2),
        w_output,
        w_gate,
        w_up,
        w_down,
    )
    half_dim = HD // 2
    frequencies = rope_base ** (-(jnp.arange(half_dim).astype(jnp.float32) * 2.0 / HD))
    angles = frequencies[:, None] * positions[0].astype(jnp.float32)[None, :]
    segments = segment_ids[0]
    token_order = jnp.arange(length)
    allowed = (segments[:, None] == segments[None, :]) & (
        token_order[:, None] <= token_order[None, :]
    )
    outs = layers(
        n,
        hidden_in,
        cotangent,
        jnp.cos(angles),
        jnp.sin(angles),
        allowed.astype(jnp.float32),
        attn_gain,
        mlp_gain,
        weights,
    )
    hidden, grad_input, grad_q, grad_k, grad_v, grad_o, grad_g, grad_u, grad_d = outs[:9]
    gain_sums = jnp.sum(outs[-1][0], axis=0)
    return (
        hidden,
        grad_input,
        grad_q,
        grad_k,
        grad_v,
        jnp.swapaxes(grad_o, 1, 2),
        grad_g,
        grad_u,
        jnp.swapaxes(grad_d, 1, 2),
        gain_sums[:LAYERS],
        gain_sums[LAYERS : 2 * LAYERS],
    )


def solution(mesh):
    return jax.shard_map(
        shards,
        mesh=mesh,
        in_specs=(
            P("dp", None),
            P("dp", None),
            P("dp", None),
            P("dp", None),
            P(None, None, "tensor"),
            P(None, None, "tensor"),
            P(None, None, "tensor"),
            P(None, "tensor", None),
            P(None, None, "tensor"),
            P(None, None, "tensor"),
            P(None, "tensor", None),
            P(),
            P(),
        ),
        out_specs=(
            P("dp", None),
            P("dp", None),
            P(None, "dp", "tensor"),
            P(None, "dp", "tensor"),
            P(None, "dp", "tensor"),
            P(None, "tensor", "dp"),
            P(None, "dp", "tensor"),
            P(None, "dp", "tensor"),
            P(None, "tensor", "dp"),
            P(None, "dp"),
            P(None, "dp"),
        ),
        check_vma=False,
    )
```
